32 devices in a mesh: row: 8 (over z, y), col: 4 (over x, core).
Axes of the slice: x: 2, y: 2, z: 4, core: 2. Of those that a mesh axis runs over, the one named last changes fastest.
Arguments:
- right_side: float32 [3, 64, 512], P(None, 'row', 'col'), may hold values from -6 to 6
- viscosity: float32 [64, 512], P('row', 'col'), may hold values from 0.1 to 3
- free_mask: int32 [3, 64, 512], P(None, 'row', 'col'), may hold values 0 or 1
- coarse_basis: float32 [64, 3, 64, 512], P(None, None, 'row', 'col'), may hold values from -6 to 6
- gram_inverse: float32 [64, 64], P('col'), may hold values from -3 to 6, as said below
Outputs:
- solution: float32 [3, 64, 512], P(None, 'row', 'col')
- residual: float32 [3, 64, 512], P(None, 'row', 'col')
The draws below stay inside these ranges and needn't reach their ends.
Inputs may be any that keep to these rules, and one draw needn't show every extreme that they name: `free_mask`: 1 marks a free velocity unknown, 0 one whose value is prescribed. `gram_inverse`: symmetric positive definite.
All inputs are finite; a program needn't handle non-finite values. No bound on the sum of `free_mask` on one device may be relied on, other than what follows from the above.
Results may differ from the reference program's by a relative error of at most 0.0003.
Values sent between devices are 32-bit elements; how exact they have to be, the bound alone decides.
No kernel may reach another device: no remote copies, remote signals or barrier semaphores. Data moves between devices by JAX's collectives and lax.ppermute only.
A program may use at most 64 MiB of HBM per device.

```python
import math
import jax
import jax.numpy as jnp
from jax import lax

COMP = 3
BASIS = 64
ITERS = 2
NA = 64
NB = 512


def draw_gram_inverse(key, part):
    base_key = jax.random.fold_in(key, 7)
    first_key, second_key = jax.random.split(base_key)
    factor = jax.random.uniform(first_key, (BASIS, BASIS), jnp.float32, -1.0, 1.0)
    square = jnp.dot(factor, factor.T, precision=lax.Precision.HIGHEST) * (3.0 / BASIS)
    square = 0.5 * (square + square.T)
    diagonal = jax.random.uniform(second_key, (BASIS,), jnp.float32, 1.0, 3.0)
    return (square + jnp.diag(diagonal)).astype(jnp.float32)


def set_ends(values, stream_key, smallest, largest):
    extent = values.shape
    spot = [jax.random.randint(jax.random.fold_in(stream_key, axis), (), 0, extent[axis]) for axis in range(len(extent))]
    values = values.at[tuple(spot)].set(smallest)
    longest = extent.index(max(extent))
    spot[longest] = (spot[longest] + 1) % extent[longest]
    return values.at[tuple(spot)].set(largest)


def steps_of(own_key, dims, shards, smallest, high):
    loudness = 1.0
    for dim, parts in shards:
        steps = jax.random.uniform(jax.random.fold_in(jax.random.fold_in(own_key, 6), dim), (parts,), jnp.float32, smallest / len(shards), high / len(shards))
        loudness = loudness * jnp.repeat(jnp.exp(steps), dims[dim] // parts).reshape((-1,) + (1,) * (len(dims) - 1 - dim))
    return loudness


def scatter_about(key, dims, width, most, cuts=(), kind=jnp.bfloat16):
    drawn = jax.random.normal(key, dims, jnp.float32) * width
    if len(cuts) > 0:
        drawn = steps_of(key, dims, cuts, -0.22, 0.18) * drawn
    return jnp.clip(drawn, min=-most, max=most).astype(kind)


def setup_inputs(seed: int = 0) -> dict:
    arg_keys = jax.random.split(jax.random.key(seed), 6)
    right_side = scatter_about(arg_keys[0], (COMP, NA, NB), 1.0, 6.0, ((1, 8), (2, 4)), jnp.float32)
    viscosity = jnp.clip(jnp.exp(math.log(3.0) - 3.4011974 * jax.random.uniform(arg_keys[1], (NA, NB), jnp.float32) ** steps_of(arg_keys[1], (NA, NB), ((0, 8), (1, 4)), -0.2, 0.2)), 0.1, 3.0)
    free_mask = set_ends((jax.random.randint(arg_keys[2], (COMP, NA, NB), 0, 8) < 7).astype(jnp.int32), jax.random.fold_in(arg_keys[2], 1), 0, 1)
    coarse_basis = scatter_about(arg_keys[3], (BASIS, COMP, NA, NB), 1.0, 6.0, ((2, 8), (3, 4)), jnp.float32)
    gram_inverse = draw_gram_inverse(jax.random.fold_in(arg_keys[5], 71), 0)
    return dict(right_side=right_side, viscosity=viscosity, free_mask=free_mask, coarse_basis=coarse_basis, gram_inverse=gram_inverse)


def face_terms(viscosity):
    padded = jnp.pad(viscosity, ((1, 1), (1, 1)))
    face_north = 0.5 * (viscosity + padded[2:, 1:-1])
    face_south = 0.5 * (viscosity + padded[:-2, 1:-1])
    face_east = 0.5 * (viscosity + padded[1:-1, 2:])
    face_west = 0.5 * (viscosity + padded[1:-1, :-2])
    diagonal = 1.0 + face_north + face_south + face_east + face_west
    return (face_north, face_south, face_east, face_west, diagonal)

def operate(vector, unfixed, faces):
    face_north, face_south, face_east, face_west, diagonal = faces
    masked = unfixed * vector
    padded = jnp.pad(masked, ((0, 0), (1, 1), (1, 1)))
    stencil = diagonal * masked - (face_north * padded[:, 2:, 1:-1] + face_south * padded[:, :-2, 1:-1] + face_east * padded[:, 1:-1, 2:] + face_west * padded[:, 1:-1, :-2])
    return unfixed * stencil + (1.0 - unfixed) * vector

def reference(right_side, viscosity, free_mask, coarse_basis, gram_inverse):
    high = lax.Precision.HIGHEST
    coarse_scale = 1.0 / (32.0 * math.sqrt(float(COMP * NA * NB * BASIS)))
    faces = face_terms(viscosity)
    unfixed = free_mask.astype(jnp.float32)
    jacobi = unfixed / faces[4] + (1.0 - unfixed)
    basis_rows = coarse_basis.reshape(BASIS, -1)

    def precondition(residual):
        coarse_dot = jnp.dot(basis_rows, residual.reshape(-1), precision=high)
        weighted_sq = jnp.sum(jacobi * residual * residual)
        coeffs = jnp.dot(gram_inverse, coarse_dot, precision=high) * coarse_scale
        smoothed = jacobi * residual + jnp.dot(coeffs, basis_rows, precision=high).reshape(residual.shape)
        return (smoothed, weighted_sq + jnp.dot(coarse_dot, coeffs, precision=high))
    solution = jnp.zeros_like(right_side)
    residual = right_side
    direction, energy = precondition(residual)
    for iteration in range(ITERS):
        applied = operate(direction, unfixed, faces)
        step_len = energy / jnp.sum(direction * applied)
        solution = solution + step_len * direction
        residual = residual - step_len * applied
        if iteration + 1 < ITERS:
            smoothed, energy_new = precondition(residual)
            direction = smoothed + energy_new / energy * direction
            energy = energy_new
    return (solution, residual)
```

```python
import math

import jax
import jax.numpy as jnp
from jax import lax
from jax.sharding import PartitionSpec as P

ITERS = 2


def padded_2(shard, sides, width):
    for axis, dim in sides:
        count, length = (lax.axis_size(axis), shard.shape[dim])
        up = [(i, (i + 1) % count) for i in range(count - 1)]
        down = [(j, i) for i, j in up]
        last = lax.slice_in_dim(shard, length - width, length, axis=dim)
        leading = lax.slice_in_dim(shard, 0, width, axis=dim)
        before = lax.ppermute(last, axis, up)
        after = lax.ppermute(leading, axis, down)
        shard = jnp.concatenate([before, shard, after], axis=dim)
    return shard


def share(rows):
    return lax.all_to_all(rows, ("row", "col"), 0, 0, tiled=True)


def sum_over(values):
    count = lax.axis_size("row") * lax.axis_size("col")
    return jnp.sum(share(jnp.broadcast_to(values, (count,) + values.shape)), axis=0)


def on_device(right_side, viscosity, free_mask, coarse_basis, gram_inverse):
    high = lax.Precision.HIGHEST
    components, patch_rows, patch_cols = right_side.shape
    columns = coarse_basis.shape[0]
    unknowns = (
        components * patch_rows * patch_cols * lax.axis_size("row") * lax.axis_size("col") * columns
    )
    coarse_scale = 1.0 / (32.0 * math.sqrt(float(unknowns)))
    viscosity_pad = padded_2(viscosity, (("row", 0), ("col", 1)), 1)
    face_north = 0.5 * (viscosity + viscosity_pad[2:, 1:-1])
    face_south = 0.5 * (viscosity + viscosity_pad[:-2, 1:-1])
    face_east = 0.5 * (viscosity + viscosity_pad[1:-1, 2:])
    face_west = 0.5 * (viscosity + viscosity_pad[1:-1, :-2])
    diagonal = 1.0 + face_north + face_south + face_east + face_west
    unfixed = free_mask.astype(jnp.float32)
    jacobi = unfixed / diagonal + (1.0 - unfixed)
    basis_rows = coarse_basis.reshape(columns, -1)

    def solve_coarse(coarse_dot):
        return jnp.dot(gram, coarse_dot, precision=high) * coarse_scale

    def precondition(residual, coarse_dot, weighted_sq):
        coeffs = solve_coarse(coarse_dot)
        smoothed = jacobi * residual + jnp.dot(coeffs, basis_rows, precision=high).reshape(
            residual.shape
        )
        return (smoothed, weighted_sq + jnp.dot(coarse_dot, coeffs, precision=high))

    solution = jnp.zeros_like(right_side)
    residual = right_side
    rows, cols = (lax.axis_size("row"), lax.axis_size("col"))
    block = gram_inverse.size
    piece = -(-block // rows)
    gram_flat = jnp.pad(gram_inverse.reshape(-1), (0, piece * rows - block))
    own_piece = lax.dynamic_slice_in_dim(gram_flat, lax.axis_index("row") * piece, piece)
    sent = jnp.concatenate(
        [
            jnp.dot(basis_rows, residual.reshape(-1), precision=high),
            jnp.sum(jacobi * residual * residual)[None],
            own_piece,
        ]
    )
    got = share(jnp.broadcast_to(sent, (rows * cols,) + sent.shape))
    sums = jnp.sum(got[:, : columns + 1], axis=0)
    coarse_dot, weighted_sq = (sums[:columns], sums[columns])
    gram = got[:, columns + 1 :].reshape(rows, cols, piece).transpose(1, 0, 2)
    gram = gram.reshape(cols, rows * piece)[:, :block].reshape(columns, columns)
    direction, energy = precondition(residual, coarse_dot, weighted_sq)
    for iteration in range(ITERS):
        masked = unfixed * direction
        padded = padded_2(masked, (("row", 1), ("col", 2)), 1)
        stencil = diagonal * masked - (
            face_north * padded[:, 2:, 1:-1]
            + face_south * padded[:, :-2, 1:-1]
            + face_east * padded[:, 1:-1, 2:]
            + face_west * padded[:, 1:-1, :-2]
        )
        applied = unfixed * stencil + (1.0 - unfixed) * direction
        if iteration + 1 < ITERS:
            sums = sum_over(
                jnp.concatenate(
                    [
                        jnp.dot(basis_rows, applied.reshape(-1), precision=high),
                        jnp.sum(direction * applied)[None],
                        jnp.sum(jacobi * residual * applied)[None],
                        jnp.sum(jacobi * applied * applied)[None],
                    ]
                )
            )
            image_coarse = sums[:columns]
            curve_sum, cross_term, image_sq = (sums[columns], sums[columns + 1], sums[columns + 2])
            step_len = energy / curve_sum
            solution = step_len * direction
            residual = residual - step_len * applied
            coarse_dot = coarse_dot - step_len * image_coarse
            weighted_sq = weighted_sq - 2.0 * step_len * cross_term + step_len * step_len * image_sq
            smoothed, energy_new = precondition(residual, coarse_dot, weighted_sq)
            direction = smoothed + energy_new / energy * direction
            energy = energy_new
        else:
            curve_sum = sum_over(jnp.sum(direction * applied)[None])[0]
            step_len = energy / curve_sum
            solution = solution + step_len * direction
            residual = residual - step_len * applied
    return (solution, residual)


def solution(mesh):
    in_specs = (
        P(None, "row", "col"),
        P("row", "col"),
        P(None, "row", "col"),
        P(None, None, "row", "col"),
        P("col", None),
    )
    out_specs = (P(None, "row", "col"), P(None, "row", "col"))
    return jax.shard_map(
        on_device, mesh=mesh, in_specs=in_specs, out_specs=out_specs, check_vma=False
    )
```

```python
import functools
import math

import jax
import jax.numpy as jnp
from jax import lax
from jax.experimental import pallas as pl
from jax.experimental.pallas import tpu as pltpu
from jax.sharding import PartitionSpec as P

F32 = jnp.float32
VMEM = pl.BlockSpec(memory_space=pltpu.VMEM)
DOTS, EAST, WEST = 64, 72, 96


def iota(shape, dim):
    return lax.broadcasted_iota(jnp.int32, shape, dim)


def pick(flag, yes, no):
    return jnp.where(jnp.full(yes.shape, flag, jnp.int32) == 1, yes, no)


def to_row(column, first=0):
    shape = (column.shape[0], 128)
    spread = jnp.where(iota(shape, 1) == iota(shape, 0) + first, column, 0.0)
    return jnp.sum(spread, axis=0, keepdims=True)


def to_column(row, count, first=0):
    shape = (count, 128)
    spread = jnp.where(iota(shape, 1) == iota(shape, 0) + first, row, 0.0)
    return jnp.sum(spread, axis=1, keepdims=True)


def total(values):
    return jnp.sum(jnp.sum(values, axis=0, keepdims=True), axis=1, keepdims=True)


def shifts(tile, north, south, east, west):
    rows, cols = tile.shape
    sub, lane = (iota(tile.shape, 0), iota(tile.shape, 1))
    return (
        jnp.where(sub == rows - 1, north, pltpu.roll(tile, rows - 1, 0)),
        jnp.where(sub == 0, south, pltpu.roll(tile, 1, 0)),
        jnp.where(lane == cols - 1, east, pltpu.roll(tile, cols - 1, 1)),
        jnp.where(lane == 0, west, pltpu.roll(tile, 1, 1)),
    )


def project(basis_ref, field, acc_ref, columns, comps, rows):
    for k in range(columns):
        base = k * comps * rows
        acc = basis_ref[base : base + rows, :] * field[0]
        for c in range(1, comps):
            acc = acc + basis_ref[base + c * rows : base + (c + 1) * rows, :] * field[c]
        acc_ref[k * rows : (k + 1) * rows, :] = acc
    sums = acc_ref[pl.ds(0, columns, stride=rows), :]
    for s in range(1, rows):
        sums = sums + acc_ref[pl.ds(s, columns, stride=rows), :]
    return jnp.sum(sums, axis=1, keepdims=True)


def combine(basis_ref, wide_ref, columns, comps, rows):
    out = [[None, None] for _ in range(comps)]
    for k in range(columns):
        weight = jnp.broadcast_to(wide_ref[k : k + 1, :], (rows, 128))
        for c in range(comps):
            base = (k * comps + c) * rows
            term = weight * basis_ref[base : base + rows, :]
            old = out[c][k % 2]
            out[c][k % 2] = term if old is None else old + term
    return [a + b for a, b in out]


def pack_kernel(sizes, basis_ref, rhs_ref, mask_ref, visc_ref, gram_ref,
                send_ref, rowa_ref, rowb_ref, cola_ref, colb_ref, acc_ref):
    columns, comps, rows, cols = sizes
    even_row = 1 - lax.rem(lax.axis_index("row"), 2)
    even_col = 1 - lax.rem(lax.axis_index("col"), 2)
    rhs = [rhs_ref[c * rows : (c + 1) * rows, :] for c in range(comps)]
    mask = [mask_ref[c * rows : (c + 1) * rows, :].astype(F32) for c in range(comps)]
    visc = visc_ref[...]
    lane = iota((rows, cols), 1)
    top, low = rows - 1, cols - 1

    for c in range(comps):
        north = basis_ref[pl.ds(c * rows + top, columns, stride=comps * rows), :]
        south = basis_ref[pl.ds(c * rows, columns, stride=comps * rows), :]
        north = north * mask[c][top : top + 1, :]
        south = south * mask[c][0:1, :]
        rowa_ref[c * columns : (c + 1) * columns, :] = pick(even_row, north, south)
        rowb_ref[c * columns : (c + 1) * columns, :] = pick(even_row, south, north)
    north = [mask[c][top : top + 1, :] * rhs[c][top : top + 1, :] for c in range(comps)]
    south = [mask[c][0:1, :] * rhs[c][0:1, :] for c in range(comps)]
    north += [visc[top : top + 1, :], visc[top - 1 : top, :]]
    south += [visc[0:1, :], visc[1:2, :]]
    for i in range(comps + 2):
        at = comps * columns + i
        rowa_ref[at : at + 1, :] = pick(even_row, north[i], south[i])
        rowb_ref[at : at + 1, :] = pick(even_row, south[i], north[i])
    rest = comps * columns + comps + 2
    blank = jnp.zeros((rowa_ref.shape[0] - rest, cols), F32)
    rowa_ref[rest:, :] = blank
    rowb_ref[rest:, :] = blank

    for c in range(comps):
        east, west = (jnp.zeros((rows, cols), F32), jnp.zeros((rows, cols), F32))
        for k in range(columns):
            base = (k * comps + c) * rows
            tile = basis_ref[base : base + rows, :]
            east = jnp.where(lane == k, pltpu.roll(tile, (k - low) % cols, 1), east)
            west = jnp.where(lane == k, tile if k == 0 else pltpu.roll(tile, k, 1), west)
        east = jnp.where(lane == columns, rhs[c][:, low : low + 1], east)
        west = jnp.where(lane == columns, rhs[c][:, 0:1], west)
        east = east * mask[c][:, low : low + 1]
        west = west * mask[c][:, 0:1]
        cola_ref[c * rows : (c + 1) * rows, :] = pick(even_col, east, west)
        colb_ref[c * rows : (c + 1) * rows, :] = pick(even_col, west, east)
    east = jnp.where(lane == 0, visc[:, low : low + 1], visc[:, low - 1 : low])
    west = jnp.where(lane == 0, visc[:, 0:1], visc[:, 1:2])
    cola_ref[comps * rows :, :] = pick(even_col, east, west)
    colb_ref[comps * rows :, :] = pick(even_col, west, east)

    row = to_row(project(basis_ref, rhs, acc_ref, columns, comps, rows))
    lanes = iota((1, cols), 1)
    corners = [visc[i : i + 1, j : j + 1] for i in (0, top) for j in (0, low)]
    for i, corner in enumerate(corners):
        row = jnp.where(lanes == columns + i, corner, row)
    both = jnp.concatenate([row, gram_ref[...]], axis=0)
    send_ref[...] = jnp.broadcast_to(both[None], send_ref.shape)


def first_kernel(sizes, whole_rows, got_ref, *refs):
    columns, comps, rows, cols, scale = sizes
    if whole_rows:
        gram_in_ref = None
    else:
        gram_in_ref, *refs = refs
    (basis_ref, rhs_ref, mask_ref, visc_ref, rowa_ref, rowb_ref, cola_ref, colb_ref,
     send_ref, state_ref, face_ref, edge_ref, side_ref, small_ref, gram_ref,
     acc_ref, wide_ref) = refs
    at_row, at_col = (lax.axis_index("row"), lax.axis_index("col"))
    row_count, col_count = (lax.axis_size("row"), lax.axis_size("col"))
    even_row, even_col = (1 - lax.rem(at_row, 2), 1 - lax.rem(at_col, 2))
    me = at_row * col_count + at_col
    top, low = rows - 1, cols - 1
    rhs = [rhs_ref[c * rows : (c + 1) * rows, :] for c in range(comps)]
    mask = [mask_ref[c * rows : (c + 1) * rows, :].astype(F32) for c in range(comps)]
    visc = visc_ref[...]
    sub, lane = (iota((rows, cols), 0), iota((rows, cols), 1))
    lanes = iota((1, cols), 1)

    if whole_rows:
        per = cols // columns
        for r in range(row_count):
            for c in range(col_count):
                piece = got_ref[r * col_count + c, 1:2, :]
                for t in range(per):
                    at = (c * row_count + r) * per + t
                    moved = pltpu.roll(piece, cols - t * columns, 1) if t else piece
                    gram_ref[at : at + 1, :] = moved
    else:
        gram_ref[:, :columns] = gram_in_ref[...]
    sums = jnp.sum(got_ref[...], axis=0)[0:1, :]
    dots = jnp.where(lanes < columns, sums, 0.0)
    gram = jnp.where(iota((columns, cols), 1) < columns, gram_ref[...], 0.0)
    coeffs = jnp.sum(gram * dots, axis=1, keepdims=True) * scale
    wide = jnp.broadcast_to(coeffs, (columns, cols))
    wide_ref[...] = wide
    coeff_row = to_row(coeffs)

    extra = comps * columns
    tail_a, tail_b = (rowa_ref[extra:, :], rowb_ref[extra:, :])
    north_tail, south_tail = (pick(even_row, tail_a, tail_b), pick(even_row, tail_b, tail_a))
    side_a, side_b = (cola_ref[...], colb_ref[...])
    east_side, west_side = (pick(even_col, side_a, side_b), pick(even_col, side_b, side_a))
    v_north, v_south = (north_tail[comps : comps + 1, :], south_tail[comps : comps + 1, :])
    v_north2, v_south2 = (north_tail[comps + 1 : comps + 2, :], south_tail[comps + 1 : comps + 2, :])
    v_east, v_west = (east_side[comps * rows :, 0:1], west_side[comps * rows :, 0:1])
    v_east2, v_west2 = (east_side[comps * rows :, 1:2], west_side[comps * rows :, 1:2])
    faces = [0.5 * (visc + v) for v in shifts(visc, v_north, v_south, v_east, v_west)]
    diagonal = 1.0 + faces[0] + faces[1] + faces[2] + faces[3]
    face_ref[...] = jnp.concatenate(faces + [diagonal], axis=0)
    jacobi = [m / diagonal + (1.0 - m) for m in mask]

    def corner(step_row, step_col, which):
        r, c = (at_row + step_row, at_col + step_col)
        inside = (r >= 0) & (r < row_count) & (c >= 0) & (c < col_count)
        place = jnp.where(inside, r * col_count + c, me)
        value = got_ref[place, 0:1, :]
        value = jnp.sum(jnp.where(lanes == columns + which, value, 0.0), axis=1, keepdims=True)
        return value * jnp.where(inside, 1.0, 0.0)

    north_west, north_east = (corner(1, -1, 1), corner(1, 1, 0))
    south_west, south_east = (corner(-1, -1, 3), corner(-1, 1, 2))

    def row_inverse(own, inner, outer, west, east):
        right = jnp.where(lanes == low, east, pltpu.roll(own, low, 1))
        left = jnp.where(lanes == 0, west, pltpu.roll(own, 1, 1))
        return 1.0 / (1.0 + 0.5 * (4.0 * own + inner + outer + left + right))

    def side_inverse(own, inner, outer, south, north):
        own = jnp.broadcast_to(own, (rows, cols))
        up = jnp.where(sub == top, north, pltpu.roll(own, top, 0))
        down = jnp.where(sub == 0, south, pltpu.roll(own, 1, 0))
        return 1.0 / (1.0 + 0.5 * (4.0 * own + inner + outer + up + down))

    inv_north = row_inverse(v_north, visc[top : top + 1, :], v_north2, north_west, north_east)
    inv_south = row_inverse(v_south, visc[0:1, :], v_south2, south_west, south_east)
    inv_east = side_inverse(v_east, visc[:, low : low + 1], v_east2, south_east, north_east)
    inv_west = side_inverse(v_west, visc[:, 0:1], v_west2, south_west, north_west)

    corr = combine(basis_ref, wide_ref, columns, comps, rows)
    image, scaled, smooth, point = ([], [], [], [])
    for c in range(comps):
        span = slice(c * columns, (c + 1) * columns)
        sum_a = jnp.sum(wide * rowa_ref[span, :], axis=0, keepdims=True)
        sum_b = jnp.sum(wide * rowb_ref[span, :], axis=0, keepdims=True)
        u_north = inv_north * north_tail[c : c + 1, :]
        u_south = inv_south * south_tail[c : c + 1, :]
        p_north = u_north + pick(even_row, sum_a, sum_b)
        p_south = u_south + pick(even_row, sum_b, sum_a)
        here = slice(c * rows, (c + 1) * rows)
        east, west = (east_side[here, :], west_side[here, :])
        u_east = inv_east * east[:, columns : columns + 1]
        u_west = inv_west * west[:, columns : columns + 1]
        p_east = u_east + jnp.sum(coeff_row * east, axis=1, keepdims=True)
        p_west = u_west + jnp.sum(coeff_row * west, axis=1, keepdims=True)
        u = jacobi[c] * rhs[c]
        p = u + corr[c]
        masked = mask[c] * p
        near = shifts(masked, p_north, p_south, p_east, p_west)
        stencil = diagonal * masked - (
            faces[0] * near[0] + faces[1] * near[1] + faces[2] * near[2] + faces[3] * near[3]
        )
        q = mask[c] * stencil + (1.0 - mask[c]) * p
        smooth.append(u)
        point.append(p)
        image.append(q)
        scaled.append(jacobi[c] * q)
        for i, value in enumerate((u_north, u_south, p_north, p_south)):
            edge_ref[i * 8 + c : i * 8 + c + 1, :] = value
        for i, value in enumerate((u_east, u_west, p_east, p_west)):
            side_ref[(i * comps + c) * rows : (i * comps + c + 1) * rows, :] = value
    state_ref[...] = jnp.concatenate(smooth + point + image + scaled, axis=0)

    row = to_row(project(basis_ref, image, acc_ref, columns, comps, rows))
    pairs = ((point, image), (smooth, image), (image, scaled), (rhs, smooth))
    for i, (left, right) in enumerate(pairs):
        value = left[0] * right[0]
        for c in range(1, comps):
            value = value + left[c] * right[c]
        row = jnp.where(lanes == DOTS + i, total(value), row)
    masked = [mask[c] * scaled[c] for c in range(comps)]
    east = jnp.concatenate([m[:, low : low + 1] for m in masked], axis=0)
    west = jnp.concatenate([m[:, 0:1] for m in masked], axis=0)
    row = row + to_row(east, EAST) + to_row(west, WEST)
    message = jnp.concatenate([row] + [m[top : top + 1, :] for m in masked], axis=0)
    send_ref[...] = jnp.broadcast_to(message[None], send_ref.shape)
    message = jnp.concatenate([row] + [m[0:1, :] for m in masked], axis=0)
    send_ref[jnp.where(at_row > 0, me - col_count, me)] = message
    small_ref[...] = jnp.concatenate([dots, coeff_row, jnp.zeros((6, cols), F32)], axis=0)


def second_kernel(sizes, got_ref, basis_ref, rhs_ref, mask_ref, rowa_ref, rowb_ref, cola_ref,
                  colb_ref, state_ref, face_ref, edge_ref, side_ref, small_ref, gram_ref,
                  send_ref, out_ref, last_ref, wide_ref):
    columns, comps, rows, cols, scale = sizes
    at_row, at_col = (lax.axis_index("row"), lax.axis_index("col"))
    row_count, col_count = (lax.axis_size("row"), lax.axis_size("col"))
    even_row, even_col = (1 - lax.rem(at_row, 2), 1 - lax.rem(at_col, 2))
    me = at_row * col_count + at_col
    lanes = iota((1, cols), 1)
    mask = [mask_ref[c * rows : (c + 1) * rows, :].astype(F32) for c in range(comps)]

    sums = jnp.sum(got_ref[...], axis=0)[0:1, :]
    image_dots = jnp.where(lanes < columns, sums, 0.0)
    curve, cross, image_sq, rhs_sq = [
        jnp.sum(jnp.where(lanes == DOTS + i, sums, 0.0), axis=1, keepdims=True) for i in range(4)
    ]
    dots, coeff_row = (small_ref[0:1, :], small_ref[1:2, :])
    energy = rhs_sq + jnp.sum(dots * coeff_row, axis=1, keepdims=True)
    step = energy / curve
    gram = jnp.where(iota((columns, cols), 1) < columns, gram_ref[...], 0.0)
    dots = dots - step * image_dots
    coeffs = jnp.sum(gram * dots, axis=1, keepdims=True) * scale
    wide = jnp.broadcast_to(coeffs, (columns, cols))
    wide_ref[...] = wide
    coeff_row = to_row(coeffs)
    energy_new = rhs_sq - 2.0 * step * cross + step * step * image_sq
    energy_new = energy_new + jnp.sum(dots * coeff_row, axis=1, keepdims=True)
    ratio = energy_new / energy

    def beside(step_row, step_col):
        r, c = (at_row + step_row, at_col + step_col)
        inside = (r >= 0) & (r < row_count) & (c >= 0) & (c < col_count)
        message = got_ref[jnp.where(inside, r * col_count + c, me)]
        return message * jnp.where(inside, 1.0, 0.0)

    q_north, q_south = (beside(1, 0), beside(-1, 0))
    q_east = to_column(beside(0, 1)[0:1, :], comps * rows, WEST)
    q_west = to_column(beside(0, -1)[0:1, :], comps * rows, EAST)

    side_a, side_b = (cola_ref[...], colb_ref[...])
    east_side, west_side = (pick(even_col, side_a, side_b), pick(even_col, side_b, side_a))
    faces = [face_ref[i * rows : (i + 1) * rows, :] for i in range(4)]
    diagonal = face_ref[4 * rows : 5 * rows, :]
    corr = combine(basis_ref, wide_ref, columns, comps, rows)
    curve_part = jnp.zeros((rows, cols), F32)
    first, second, third, fourth = ([], [], [], [])
    for c in range(comps):
        span = slice(c * columns, (c + 1) * columns)
        here = slice(c * rows, (c + 1) * rows)
        sum_a = jnp.sum(wide * rowa_ref[span, :], axis=0, keepdims=True)
        sum_b = jnp.sum(wide * rowb_ref[span, :], axis=0, keepdims=True)
        old = [edge_ref[i * 8 + c : i * 8 + c + 1, :] for i in range(4)]
        p_north = old[0] - step * q_north[1 + c : 2 + c, :] + pick(even_row, sum_a, sum_b)
        p_south = old[1] - step * q_south[1 + c : 2 + c, :] + pick(even_row, sum_b, sum_a)
        p_north, p_south = (p_north + ratio * old[2], p_south + ratio * old[3])
        old = [side_ref[(i * comps + c) * rows : (i * comps + c + 1) * rows, :] for i in range(4)]
        p_east = old[0] - step * q_east[here] + ratio * old[2]
        p_west = old[1] - step * q_west[here] + ratio * old[3]
        p_east = p_east + jnp.sum(coeff_row * east_side[here, :], axis=1, keepdims=True)
        p_west = p_west + jnp.sum(coeff_row * west_side[here, :], axis=1, keepdims=True)
        u, p, q, jq = [
            state_ref[(i * comps + c) * rows : (i * comps + c + 1) * rows, :] for i in range(4)
        ]
        new = u - step * jq + corr[c] + ratio * p
        masked = mask[c] * new
        near = shifts(masked, p_north, p_south, p_east, p_west)
        stencil = diagonal * masked - (
            faces[0] * near[0] + faces[1] * near[1] + faces[2] * near[2] + faces[3] * near[3]
        )
        applied = mask[c] * stencil + (1.0 - mask[c]) * new
        curve_part = curve_part + new * applied
        first.append(step * p)
        second.append(new)
        third.append(rhs_ref[here, :] - step * q)
        fourth.append(applied)
    out_ref[...] = jnp.concatenate(first + second + third + fourth, axis=0)
    last_ref[...] = jnp.broadcast_to(energy_new, last_ref.shape)
    send_ref[...] = jnp.broadcast_to(total(curve_part)[None], send_ref.shape)


def last_kernel(count, got_ref, in_ref, last_ref, solution_ref, residual_ref):
    step = last_ref[0:1, :] / jnp.sum(got_ref[...], axis=0)
    solution_ref[...] = in_ref[:count, :] + step * in_ref[count : 2 * count, :]
    residual_ref[...] = in_ref[2 * count : 3 * count, :] - step * in_ref[3 * count :, :]


def on_device(right_side, viscosity, free_mask, coarse_basis, gram_inverse):
    comps, rows, cols = right_side.shape
    columns = coarse_basis.shape[0]
    row_count, col_count = (lax.axis_size("row"), lax.axis_size("col"))
    devices = row_count * col_count
    scale = 1.0 / (32.0 * math.sqrt(float(comps * rows * cols * devices * columns)))
    sizes = (columns, comps, rows, cols)

    def call(kernel, outs, scratch, *args):
        return pl.pallas_call(
            kernel,
            out_shape=[jax.ShapeDtypeStruct(s, F32) for s in outs],
            in_specs=[VMEM] * len(args),
            out_specs=[VMEM] * len(outs),
            scratch_shapes=[pltpu.VMEM(s, F32) for s in scratch],
            compiler_params=pltpu.CompilerParams(vmem_limit_bytes=16 * 1024 * 1024),
        )(*args)

    def share(message):
        return lax.all_to_all(message, ("row", "col"), 0, 0, tiled=True)

    def swap(packet, axis, first):
        pairs = [(i, i + 1) for i in range(first, lax.axis_size(axis) - 1, 2)]
        return lax.ppermute(packet, axis, pairs + [(j, i) for i, j in pairs])

    basis = coarse_basis.reshape(columns * comps * rows, cols)
    rhs = right_side.reshape(comps * rows, cols)
    mask = free_mask.reshape(comps * rows, cols)

    block = gram_inverse.size
    piece = -(-block // row_count)
    flat = jnp.pad(gram_inverse.reshape(-1), (0, piece * row_count - block))
    own = lax.dynamic_slice_in_dim(flat, lax.axis_index("row") * piece, piece)
    own = jnp.pad(own, (0, cols - piece)).reshape(1, cols)

    tall = -(-(comps * columns + comps + 2) // 8) * 8
    wide = (comps + 1) * rows
    field = comps * rows
    send, row_a, row_b, col_a, col_b = call(
        functools.partial(pack_kernel, sizes),
        [(devices, 2, cols), (tall, cols), (tall, cols), (wide, cols), (wide, cols)],
        [(columns * rows, cols)],
        basis, rhs, mask, viscosity, own,
    )
    halos = (swap(row_a, "row", 0), swap(row_b, "row", 1), swap(col_a, "col", 0), swap(col_b, "col", 1))
    got = share(send)
    whole_rows = piece == cols and cols % columns == 0 and block == piece * row_count
    gram = ()
    if not whole_rows:
        gram = got[:, 1, :piece].reshape(row_count, col_count, piece).transpose(1, 0, 2)
        gram = gram.reshape(col_count, row_count * piece)[:, :block].reshape(columns, columns)
        gram = (gram,)
    sizes = sizes + (scale,)
    send, *state = call(
        functools.partial(first_kernel, sizes, whole_rows),
        [(devices, 1 + comps, cols), (4 * field, cols), (5 * rows, cols), (32, cols),
         (4 * field, cols), (8, cols), (columns, cols)],
        [(columns * rows, cols), (columns, cols)],
        got, *gram, basis, rhs, mask, viscosity, *halos,
    )
    send, fields, last = call(
        functools.partial(second_kernel, sizes),
        [(devices, 1, cols), (4 * field, cols), (8, cols)],
        [(columns, cols)],
        share(send), basis, rhs, mask, *halos, *state,
    )
    solution, residual = call(
        functools.partial(last_kernel, field),
        [(field, cols), (field, cols)],
        [],
        share(send), fields, last,
    )
    return (solution.reshape(right_side.shape), residual.reshape(right_side.shape))


def solution(mesh):
    in_specs = (
        P(None, "row", "col"),
        P("row", "col"),
        P(None, "row", "col"),
        P(None, None, "row", "col"),
        P("col", None),
    )
    out_specs = (P(None, "row", "col"), P(None, "row", "col"))
    return jax.shard_map(
        on_device, mesh=mesh, in_specs=in_specs, out_specs=out_specs, check_vma=False
    )
```

```python
import functools
import math

import jax
import jax.numpy as jnp
from jax import lax
from jax.experimental import pallas as pl
from jax.experimental.pallas import tpu as pltpu
from jax.sharding import PartitionSpec as P

F32 = jnp.float32
VMEM = pl.BlockSpec(memory_space=pltpu.VMEM)
DOTS, EAST, WEST = 64, 72, 96


def flags():
    at_row, at_col = (lax.axis_index("row"), lax.axis_index("col"))
    tests = (
        at_row < lax.axis_size("row") - 1,
        at_row > 0,
        at_col < lax.axis_size("col") - 1,
        at_col > 0,
    )
    return [jnp.where(test, 1.0, 0.0) for test in tests]


def iota(shape, dim):
    return lax.broadcasted_iota(jnp.int32, shape, dim)


def pick(flag, yes, no):
    return jnp.where(jnp.full(yes.shape, flag, jnp.int32) == 1, yes, no)


def to_row(column, first=0):
    shape = (column.shape[0], 128)
    spread = jnp.where(iota(shape, 1) == iota(shape, 0) + first, column, 0.0)
    return jnp.sum(spread, axis=0, keepdims=True)


def to_column(row, count, first=0):
    shape = (count, 128)
    spread = jnp.where(iota(shape, 1) == iota(shape, 0) + first, row, 0.0)
    return jnp.sum(spread, axis=1, keepdims=True)


def total(values):
    return jnp.sum(jnp.sum(values, axis=0, keepdims=True), axis=1, keepdims=True)


def shifts(tile, north, south, east, west):
    rows, cols = tile.shape
    sub, lane = (iota(tile.shape, 0), iota(tile.shape, 1))
    return (
        jnp.where(sub == rows - 1, north, pltpu.roll(tile, rows - 1, 0)),
        jnp.where(sub == 0, south, pltpu.roll(tile, 1, 0)),
        jnp.where(lane == cols - 1, east, pltpu.roll(tile, cols - 1, 1)),
        jnp.where(lane == 0, west, pltpu.roll(tile, 1, 1)),
    )


def project(basis_ref, field, acc_ref, columns, comps, rows):
    for k in range(columns):
        base = k * comps * rows
        acc = basis_ref[base : base + rows, :] * field[0]
        for c in range(1, comps):
            acc = acc + basis_ref[base + c * rows : base + (c + 1) * rows, :] * field[c]
        acc_ref[k * rows : (k + 1) * rows, :] = acc
    sums = acc_ref[pl.ds(0, columns, stride=rows), :]
    for s in range(1, rows):
        sums = sums + acc_ref[pl.ds(s, columns, stride=rows), :]
    return jnp.sum(sums, axis=1, keepdims=True)


def combine(basis_ref, wide_ref, columns, comps, rows):
    out = [[None, None] for _ in range(comps)]
    for k in range(columns):
        weight = jnp.broadcast_to(wide_ref[k : k + 1, :], (rows, 128))
        for c in range(comps):
            base = (k * comps + c) * rows
            term = weight * basis_ref[base : base + rows, :]
            old = out[c][k % 2]
            out[c][k % 2] = term if old is None else old + term
    return [a + b for a, b in out]


def pack_kernel(sizes, basis_ref, rhs_ref, mask_ref, visc_ref, gram_ref,
                send_ref, rowa_ref, rowb_ref, cola_ref, colb_ref, acc_ref):
    columns, comps, rows, cols = sizes
    even_row = 1 - lax.rem(lax.axis_index("row"), 2)
    even_col = 1 - lax.rem(lax.axis_index("col"), 2)
    rhs = [rhs_ref[c * rows : (c + 1) * rows, :] for c in range(comps)]
    mask = [mask_ref[c * rows : (c + 1) * rows, :].astype(F32) for c in range(comps)]
    visc = visc_ref[...]
    lane = iota((rows, cols), 1)
    top, low = rows - 1, cols - 1

    for c in range(comps):
        north = basis_ref[pl.ds(c * rows + top, columns, stride=comps * rows), :]
        south = basis_ref[pl.ds(c * rows, columns, stride=comps * rows), :]
        north = north * mask[c][top : top + 1, :]
        south = south * mask[c][0:1, :]
        rowa_ref[c * columns : (c + 1) * columns, :] = pick(even_row, north, south)
        rowb_ref[c * columns : (c + 1) * columns, :] = pick(even_row, south, north)
    north = [mask[c][top : top + 1, :] * rhs[c][top : top + 1, :] for c in range(comps)]
    south = [mask[c][0:1, :] * rhs[c][0:1, :] for c in range(comps)]
    north += [visc[top : top + 1, :], visc[top - 1 : top, :]]
    south += [visc[0:1, :], visc[1:2, :]]
    for i in range(comps + 2):
        at = comps * columns + i
        rowa_ref[at : at + 1, :] = pick(even_row, north[i], south[i])
        rowb_ref[at : at + 1, :] = pick(even_row, south[i], north[i])
    rest = comps * columns + comps + 2
    blank = jnp.zeros((rowa_ref.shape[0] - rest, cols), F32)
    rowa_ref[rest:, :] = blank
    rowb_ref[rest:, :] = blank

    for c in range(comps):
        east, west = (jnp.zeros((rows, cols), F32), jnp.zeros((rows, cols), F32))
        for k in range(columns):
            base = (k * comps + c) * rows
            tile = basis_ref[base : base + rows, :]
            east = jnp.where(lane == k, pltpu.roll(tile, (k - low) % cols, 1), east)
            west = jnp.where(lane == k, tile if k == 0 else pltpu.roll(tile, k, 1), west)
        east = jnp.where(lane == columns, rhs[c][:, low : low + 1], east)
        west = jnp.where(lane == columns, rhs[c][:, 0:1], west)
        east = east * mask[c][:, low : low + 1]
        west = west * mask[c][:, 0:1]
        cola_ref[c * rows : (c + 1) * rows, :] = pick(even_col, east, west)
        colb_ref[c * rows : (c + 1) * rows, :] = pick(even_col, west, east)
    east = jnp.where(lane == 0, visc[:, low : low + 1], visc[:, low - 1 : low])
    west = jnp.where(lane == 0, visc[:, 0:1], visc[:, 1:2])
    cola_ref[comps * rows :, :] = pick(even_col, east, west)
    colb_ref[comps * rows :, :] = pick(even_col, west, east)

    row = to_row(project(basis_ref, rhs, acc_ref, columns, comps, rows))
    lanes = iota((1, cols), 1)
    corners = [visc[i : i + 1, j : j + 1] for i in (0, top) for j in (0, low)]
    for i, corner in enumerate(corners):
        row = jnp.where(lanes == columns + i, corner, row)
    both = jnp.concatenate([row, gram_ref[...]], axis=0)
    send_ref[...] = jnp.broadcast_to(both[None], send_ref.shape)


def first_kernel(sizes, whole_rows, got_ref, *refs):
    columns, comps, rows, cols, scale = sizes
    if whole_rows:
        gram_in_ref = None
    else:
        gram_in_ref, *refs = refs
    (basis_ref, rhs_ref, mask_ref, visc_ref, rowa_ref, rowb_ref, cola_ref, colb_ref,
     send_ref, state_ref, face_ref, edge_ref, side_ref, small_ref, gram_ref,
     acc_ref, wide_ref) = refs
    at_row, at_col = (lax.axis_index("row"), lax.axis_index("col"))
    row_count, col_count = (lax.axis_size("row"), lax.axis_size("col"))
    even_row, even_col = (1 - lax.rem(at_row, 2), 1 - lax.rem(at_col, 2))
    me = at_row * col_count + at_col
    top, low = rows - 1, cols - 1
    rhs = [rhs_ref[c * rows : (c + 1) * rows, :] for c in range(comps)]
    mask = [mask_ref[c * rows : (c + 1) * rows, :].astype(F32) for c in range(comps)]
    visc = visc_ref[...]
    sub, lane = (iota((rows, cols), 0), iota((rows, cols), 1))
    lanes = iota((1, cols), 1)

    if whole_rows:
        per = cols // columns
        for r in range(row_count):
            for c in range(col_count):
                piece = got_ref[r * col_count + c, 1:2, :]
                for t in range(per):
                    at = (c * row_count + r) * per + t
                    moved = pltpu.roll(piece, cols - t * columns, 1) if t else piece
                    gram_ref[at : at + 1, :] = moved
    else:
        gram_ref[:, :columns] = gram_in_ref[...]
    sums = jnp.sum(got_ref[...], axis=0)[0:1, :]
    dots = jnp.where(lanes < columns, sums, 0.0)
    gram = jnp.where(iota((columns, cols), 1) < columns, gram_ref[...], 0.0)
    coeffs = jnp.sum(gram * dots, axis=1, keepdims=True) * scale
    wide = jnp.broadcast_to(coeffs, (columns, cols))
    wide_ref[...] = wide
    coeff_row = to_row(coeffs)

    extra = comps * columns
    tail_a, tail_b = (rowa_ref[extra:, :], rowb_ref[extra:, :])
    has_north, has_south, has_east, has_west = flags()
    north_tail = pick(even_row, tail_a, tail_b) * has_north
    south_tail = pick(even_row, tail_b, tail_a) * has_south
    side_a, side_b = (cola_ref[...], colb_ref[...])
    east_side = pick(even_col, side_a, side_b) * has_east
    west_side = pick(even_col, side_b, side_a) * has_west
    v_north, v_south = (north_tail[comps : comps + 1, :], south_tail[comps : comps + 1, :])
    v_north2, v_south2 = (north_tail[comps + 1 : comps + 2, :], south_tail[comps + 1 : comps + 2, :])
    v_east, v_west = (east_side[comps * rows :, 0:1], west_side[comps * rows :, 0:1])
    v_east2, v_west2 = (east_side[comps * rows :, 1:2], west_side[comps * rows :, 1:2])
    faces = [0.5 * (visc + v) for v in shifts(visc, v_north, v_south, v_east, v_west)]
    diagonal = 1.0 + faces[0] + faces[1] + faces[2] + faces[3]
    face_ref[...] = jnp.concatenate(faces + [diagonal], axis=0)
    jacobi = [m / diagonal + (1.0 - m) for m in mask]

    def corner(step_row, step_col, which):
        r, c = (at_row + step_row, at_col + step_col)
        inside = (r >= 0) & (r < row_count) & (c >= 0) & (c < col_count)
        place = jnp.where(inside, r * col_count + c, me)
        value = got_ref[place, 0:1, :]
        value = jnp.sum(jnp.where(lanes == columns + which, value, 0.0), axis=1, keepdims=True)
        return value * jnp.where(inside, 1.0, 0.0)

    north_west, north_east = (corner(1, -1, 1), corner(1, 1, 0))
    south_west, south_east = (corner(-1, -1, 3), corner(-1, 1, 2))

    def row_inverse(own, inner, outer, west, east):
        right = jnp.where(lanes == low, east, pltpu.roll(own, low, 1))
        left = jnp.where(lanes == 0, west, pltpu.roll(own, 1, 1))
        return 1.0 / (1.0 + 0.5 * (4.0 * own + inner + outer + left + right))

    def side_inverse(own, inner, outer, south, north):
        own = jnp.broadcast_to(own, (rows, cols))
        up = jnp.where(sub == top, north, pltpu.roll(own, top, 0))
        down = jnp.where(sub == 0, south, pltpu.roll(own, 1, 0))
        return 1.0 / (1.0 + 0.5 * (4.0 * own + inner + outer + up + down))

    inv_north = row_inverse(v_north, visc[top : top + 1, :], v_north2, north_west, north_east)
    inv_south = row_inverse(v_south, visc[0:1, :], v_south2, south_west, south_east)
    inv_east = side_inverse(v_east, visc[:, low : low + 1], v_east2, south_east, north_east)
    inv_west = side_inverse(v_west, visc[:, 0:1], v_west2, south_west, north_west)

    corr = combine(basis_ref, wide_ref, columns, comps, rows)
    image, scaled, smooth, point = ([], [], [], [])
    for c in range(comps):
        span = slice(c * columns, (c + 1) * columns)
        sum_a = jnp.sum(wide * rowa_ref[span, :], axis=0, keepdims=True)
        sum_b = jnp.sum(wide * rowb_ref[span, :], axis=0, keepdims=True)
        u_north = inv_north * north_tail[c : c + 1, :]
        u_south = inv_south * south_tail[c : c + 1, :]
        p_north = u_north + has_north * pick(even_row, sum_a, sum_b)
        p_south = u_south + has_south * pick(even_row, sum_b, sum_a)
        here = slice(c * rows, (c + 1) * rows)
        east, west = (east_side[here, :], west_side[here, :])
        u_east = inv_east * east[:, columns : columns + 1]
        u_west = inv_west * west[:, columns : columns + 1]
        p_east = u_east + jnp.sum(coeff_row * east, axis=1, keepdims=True)
        p_west = u_west + jnp.sum(coeff_row * west, axis=1, keepdims=True)
        u = jacobi[c] * rhs[c]
        p = u + corr[c]
        masked = mask[c] * p
        near = shifts(masked, p_north, p_south, p_east, p_west)
        stencil = diagonal * masked - (
            faces[0] * near[0] + faces[1] * near[1] + faces[2] * near[2] + faces[3] * near[3]
        )
        q = mask[c] * stencil + (1.0 - mask[c]) * p
        smooth.append(u)
        point.append(p)
        image.append(q)
        scaled.append(jacobi[c] * q)
        for i, value in enumerate((u_north, u_south, p_north, p_south)):
            edge_ref[i * 8 + c : i * 8 + c + 1, :] = value
        for i, value in enumerate((u_east, u_west, p_east, p_west)):
            side_ref[(i * comps + c) * rows : (i * comps + c + 1) * rows, :] = value
    state_ref[...] = jnp.concatenate(smooth + point + image + scaled, axis=0)

    row = to_row(project(basis_ref, image, acc_ref, columns, comps, rows))
    pairs = ((point, image), (smooth, image), (image, scaled), (rhs, smooth))
    for i, (left, right) in enumerate(pairs):
        value = left[0] * right[0]
        for c in range(1, comps):
            value = value + left[c] * right[c]
        row = jnp.where(lanes == DOTS + i, total(value), row)
    masked = [mask[c] * scaled[c] for c in range(comps)]
    east = jnp.concatenate([m[:, low : low + 1] for m in masked], axis=0)
    west = jnp.concatenate([m[:, 0:1] for m in masked], axis=0)
    row = row + to_row(east, EAST) + to_row(west, WEST)
    message = jnp.concatenate([row] + [m[top : top + 1, :] for m in masked], axis=0)
    send_ref[...] = jnp.broadcast_to(message[None], send_ref.shape)
    message = jnp.concatenate([row] + [m[0:1, :] for m in masked], axis=0)
    send_ref[jnp.where(at_row > 0, me - col_count, me)] = message
    small_ref[...] = jnp.concatenate([dots, coeff_row, jnp.zeros((6, cols), F32)], axis=0)


def second_kernel(sizes, got_ref, basis_ref, rhs_ref, mask_ref, rowa_ref, rowb_ref, cola_ref,
                  colb_ref, state_ref, face_ref, edge_ref, side_ref, small_ref, gram_ref,
                  send_ref, out_ref, last_ref, wide_ref):
    columns, comps, rows, cols, scale = sizes
    at_row, at_col = (lax.axis_index("row"), lax.axis_index("col"))
    row_count, col_count = (lax.axis_size("row"), lax.axis_size("col"))
    even_row, even_col = (1 - lax.rem(at_row, 2), 1 - lax.rem(at_col, 2))
    me = at_row * col_count + at_col
    lanes = iota((1, cols), 1)
    mask = [mask_ref[c * rows : (c + 1) * rows, :].astype(F32) for c in range(comps)]

    sums = jnp.sum(got_ref[...], axis=0)[0:1, :]
    image_dots = jnp.where(lanes < columns, sums, 0.0)
    curve, cross, image_sq, rhs_sq = [
        jnp.sum(jnp.where(lanes == DOTS + i, sums, 0.0), axis=1, keepdims=True) for i in range(4)
    ]
    dots, coeff_row = (small_ref[0:1, :], small_ref[1:2, :])
    energy = rhs_sq + jnp.sum(dots * coeff_row, axis=1, keepdims=True)
    step = energy / curve
    gram = jnp.where(iota((columns, cols), 1) < columns, gram_ref[...], 0.0)
    dots = dots - step * image_dots
    coeffs = jnp.sum(gram * dots, axis=1, keepdims=True) * scale
    wide = jnp.broadcast_to(coeffs, (columns, cols))
    wide_ref[...] = wide
    coeff_row = to_row(coeffs)
    energy_new = rhs_sq - 2.0 * step * cross + step * step * image_sq
    energy_new = energy_new + jnp.sum(dots * coeff_row, axis=1, keepdims=True)
    ratio = energy_new / energy

    def beside(step_row, step_col):
        r, c = (at_row + step_row, at_col + step_col)
        inside = (r >= 0) & (r < row_count) & (c >= 0) & (c < col_count)
        message = got_ref[jnp.where(inside, r * col_count + c, me)]
        return message * jnp.where(inside, 1.0, 0.0)

    q_north, q_south = (beside(1, 0), beside(-1, 0))
    q_east = to_column(beside(0, 1)[0:1, :], comps * rows, WEST)
    q_west = to_column(beside(0, -1)[0:1, :], comps * rows, EAST)

    side_a, side_b = (cola_ref[...], colb_ref[...])
    has_north, has_south, has_east, has_west = flags()
    east_side = pick(even_col, side_a, side_b) * has_east
    west_side = pick(even_col, side_b, side_a) * has_west
    faces = [face_ref[i * rows : (i + 1) * rows, :] for i in range(4)]
    diagonal = face_ref[4 * rows : 5 * rows, :]
    corr = combine(basis_ref, wide_ref, columns, comps, rows)
    curve_part = jnp.zeros((rows, cols), F32)
    first, second, third, fourth = ([], [], [], [])
    for c in range(comps):
        span = slice(c * columns, (c + 1) * columns)
        here = slice(c * rows, (c + 1) * rows)
        sum_a = jnp.sum(wide * rowa_ref[span, :], axis=0, keepdims=True)
        sum_b = jnp.sum(wide * rowb_ref[span, :], axis=0, keepdims=True)
        old = [edge_ref[i * 8 + c : i * 8 + c + 1, :] for i in range(4)]
        p_north = old[0] - step * q_north[1 + c : 2 + c, :] + has_north * pick(even_row, sum_a, sum_b)
        p_south = old[1] - step * q_south[1 + c : 2 + c, :] + has_south * pick(even_row, sum_b, sum_a)
        p_north, p_south = (p_north + ratio * old[2], p_south + ratio * old[3])
        old = [side_ref[(i * comps + c) * rows : (i * comps + c + 1) * rows, :] for i in range(4)]
        p_east = old[0] - step * q_east[here] + ratio * old[2]
        p_west = old[1] - step * q_west[here] + ratio * old[3]
        p_east = p_east + jnp.sum(coeff_row * east_side[here, :], axis=1, keepdims=True)
        p_west = p_west + jnp.sum(coeff_row * west_side[here, :], axis=1, keepdims=True)
        u, p, q, jq = [
            state_ref[(i * comps + c) * rows : (i * comps + c + 1) * rows, :] for i in range(4)
        ]
        new = u - step * jq + corr[c] + ratio * p
        masked = mask[c] * new
        near = shifts(masked, p_north, p_south, p_east, p_west)
        stencil = diagonal * masked - (
            faces[0] * near[0] + faces[1] * near[1] + faces[2] * near[2] + faces[3] * near[3]
        )
        applied = mask[c] * stencil + (1.0 - mask[c]) * new
        curve_part = curve_part + new * applied
        first.append(step * p)
        second.append(new)
        third.append(rhs_ref[here, :] - step * q)
        fourth.append(applied)
    out_ref[...] = jnp.concatenate(first + second + third + fourth, axis=0)
    last_ref[...] = jnp.broadcast_to(energy_new, last_ref.shape)
    send_ref[...] = jnp.broadcast_to(total(curve_part)[None], send_ref.shape)


def last_kernel(count, got_ref, in_ref, last_ref, solution_ref, residual_ref):
    step = last_ref[0:1, :] / jnp.sum(got_ref[...], axis=0)
    solution_ref[...] = in_ref[:count, :] + step * in_ref[count : 2 * count, :]
    residual_ref[...] = in_ref[2 * count : 3 * count, :] - step * in_ref[3 * count :, :]


def on_device(right_side, viscosity, free_mask, coarse_basis, gram_inverse):
    comps, rows, cols = right_side.shape
    columns = coarse_basis.shape[0]
    row_count, col_count = (lax.axis_size("row"), lax.axis_size("col"))
    devices = row_count * col_count
    scale = 1.0 / (32.0 * math.sqrt(float(comps * rows * cols * devices * columns)))
    sizes = (columns, comps, rows, cols)

    def call(kernel, outs, scratch, *args):
        return pl.pallas_call(
            kernel,
            out_shape=[jax.ShapeDtypeStruct(s, F32) for s in outs],
            in_specs=[VMEM] * len(args),
            out_specs=[VMEM] * len(outs),
            scratch_shapes=[pltpu.VMEM(s, F32) for s in scratch],
            compiler_params=pltpu.CompilerParams(vmem_limit_bytes=16 * 1024 * 1024),
        )(*args)

    def share(message):
        return lax.all_to_all(message, ("row", "col"), 0, 0, tiled=True)

    def swap(packet, axis, first):
        count = lax.axis_size(axis)
        pairs = [(i, i + 1) for i in range(first, count - 1, 2)]
        if first == 1 and count > 2 and count % 2 == 0:
            pairs.append((0, count - 1))
        return lax.ppermute(packet, axis, pairs + [(j, i) for i, j in pairs])

    basis = coarse_basis.reshape(columns * comps * rows, cols)
    rhs = right_side.reshape(comps * rows, cols)
    mask = free_mask.reshape(comps * rows, cols)

    block = gram_inverse.size
    piece = -(-block // row_count)
    flat = jnp.pad(gram_inverse.reshape(-1), (0, piece * row_count - block))
    own = lax.dynamic_slice_in_dim(flat, lax.axis_index("row") * piece, piece)
    own = jnp.pad(own, (0, cols - piece)).reshape(1, cols)

    tall = -(-(comps * columns + comps + 2) // 8) * 8
    wide = (comps + 1) * rows
    field = comps * rows
    send, row_a, row_b, col_a, col_b = call(
        functools.partial(pack_kernel, sizes),
        [(devices, 2, cols), (tall, cols), (tall, cols), (wide, cols), (wide, cols)],
        [(columns * rows, cols)],
        basis, rhs, mask, viscosity, own,
    )
    halos = (swap(row_a, "row", 0), swap(row_b, "row", 1), swap(col_a, "col", 0), swap(col_b, "col", 1))
    got = share(send)
    whole_rows = piece == cols and cols % columns == 0 and block == piece * row_count
    gram = ()
    if not whole_rows:
        gram = got[:, 1, :piece].reshape(row_count, col_count, piece).transpose(1, 0, 2)
        gram = gram.reshape(col_count, row_count * piece)[:, :block].reshape(columns, columns)
        gram = (gram,)
    sizes = sizes + (scale,)
    send, *state = call(
        functools.partial(first_kernel, sizes, whole_rows),
        [(devices, 1 + comps, cols), (4 * field, cols), (5 * rows, cols), (32, cols),
         (4 * field, cols), (8, cols), (columns, cols)],
        [(columns * rows, cols), (columns, cols)],
        got, *gram, basis, rhs, mask, viscosity, *halos,
    )
    send, fields, last = call(
        functools.partial(second_kernel, sizes),
        [(devices, 1, cols), (4 * field, cols), (8, cols)],
        [(columns, cols)],
        share(send), basis, rhs, mask, *halos, *state,
    )
    solution, residual = call(
        functools.partial(last_kernel, field),
        [(field, cols), (field, cols)],
        [],
        share(send), fields, last,
    )
    return (solution.reshape(right_side.shape), residual.reshape(right_side.shape))


def solution(mesh):
    in_specs = (
        P(None, "row", "col"),
        P("row", "col"),
        P(None, "row", "col"),
        P(None, None, "row", "col"),
        P("col", None),
    )
    out_specs = (P(None, "row", "col"), P(None, "row", "col"))
    return jax.shard_map(
        on_device, mesh=mesh, in_specs=in_specs, out_specs=out_specs, check_vma=False
    )
```

```python
import functools
import math

import jax
import jax.numpy as jnp
from jax import lax
from jax.experimental import pallas as pl
from jax.experimental.pallas import tpu as pltpu
from jax.sharding import PartitionSpec as P

F32 = jnp.float32
VMEM = pl.BlockSpec(memory_space=pltpu.VMEM)
DOTS, EAST, WEST = 64, 72, 96
EAST2, WEST2, DOTS2 = 64, 88, 112


def flags():
    at_row, at_col = (lax.axis_index("row"), lax.axis_index("col"))
    tests = (
        at_row < lax.axis_size("row") - 1,
        at_row > 0,
        at_col < lax.axis_size("col") - 1,
        at_col > 0,
    )
    return [jnp.where(test, 1.0, 0.0) for test in tests]


def iota(shape, dim):
    return lax.broadcasted_iota(jnp.int32, shape, dim)


def pick(flag, yes, no):
    return jnp.where(jnp.full(yes.shape, flag, jnp.int32) == 1, yes, no)


def to_row(column, first=0):
    shape = (column.shape[0], 128)
    spread = jnp.where(iota(shape, 1) == iota(shape, 0) + first, column, 0.0)
    return jnp.sum(spread, axis=0, keepdims=True)


def to_column(row, count, first=0):
    shape = (count, 128)
    spread = jnp.where(iota(shape, 1) == iota(shape, 0) + first, row, 0.0)
    return jnp.sum(spread, axis=1, keepdims=True)


def total(values):
    return jnp.sum(jnp.sum(values, axis=0, keepdims=True), axis=1, keepdims=True)


def shifts(tile, north, south, east, west):
    rows, cols = tile.shape
    sub, lane = (iota(tile.shape, 0), iota(tile.shape, 1))
    return (
        jnp.where(sub == rows - 1, north, pltpu.roll(tile, rows - 1, 0)),
        jnp.where(sub == 0, south, pltpu.roll(tile, 1, 0)),
        jnp.where(lane == cols - 1, east, pltpu.roll(tile, cols - 1, 1)),
        jnp.where(lane == 0, west, pltpu.roll(tile, 1, 1)),
    )


def project(basis_ref, field, acc_ref, columns, comps, rows):
    for k in range(columns):
        base = k * comps * rows
        acc = basis_ref[base : base + rows, :] * field[0]
        for c in range(1, comps):
            acc = acc + basis_ref[base + c * rows : base + (c + 1) * rows, :] * field[c]
        acc_ref[k * rows : (k + 1) * rows, :] = acc
    sums = acc_ref[pl.ds(0, columns, stride=rows), :]
    for s in range(1, rows):
        sums = sums + acc_ref[pl.ds(s, columns, stride=rows), :]
    return jnp.sum(sums, axis=1, keepdims=True)


def combine(basis_ref, wide_ref, columns, comps, rows):
    out = [[None, None] for _ in range(comps)]
    for k in range(columns):
        weight = jnp.broadcast_to(wide_ref[k : k + 1, :], (rows, 128))
        for c in range(comps):
            base = (k * comps + c) * rows
            term = weight * basis_ref[base : base + rows, :]
            old = out[c][k % 2]
            out[c][k % 2] = term if old is None else old + term
    return [a + b for a, b in out]


def pack_kernel(sizes, basis_ref, rhs_ref, mask_ref, visc_ref, gram_ref,
                send_ref, rowa_ref, rowb_ref, cola_ref, colb_ref, acc_ref):
    columns, comps, rows, cols = sizes
    packet_kernel(sizes, basis_ref, rhs_ref, mask_ref, visc_ref, rowa_ref, rowb_ref, cola_ref, colb_ref)
    rhs = [rhs_ref[c * rows : (c + 1) * rows, :] for c in range(comps)]
    visc = visc_ref[...]

    row = to_row(project(basis_ref, rhs, acc_ref, columns, comps, rows))
    lanes = iota((1, cols), 1)
    for i, corner in enumerate(corners_of(visc)):
        row = jnp.where(lanes == columns + i, corner, row)
    both = jnp.concatenate([row, gram_ref[...]], axis=0)
    send_ref[...] = jnp.broadcast_to(both[None], send_ref.shape)


def corners_of(visc):
    top, low = (visc.shape[0] - 1, visc.shape[1] - 1)
    return [visc[i : i + 1, j : j + 1] for i in (0, top) for j in (0, low)]


def packet_kernel(sizes, basis_ref, rhs_ref, mask_ref, visc_ref,
                  rowa_ref, rowb_ref, cola_ref, colb_ref):
    columns, comps, rows, cols = sizes
    even_row = 1 - lax.rem(lax.axis_index("row"), 2)
    even_col = 1 - lax.rem(lax.axis_index("col"), 2)
    rhs = [rhs_ref[c * rows : (c + 1) * rows, :] for c in range(comps)]
    mask = [mask_ref[c * rows : (c + 1) * rows, :].astype(F32) for c in range(comps)]
    visc = visc_ref[...]
    lane = iota((rows, cols), 1)
    top, low = rows - 1, cols - 1

    for c in range(comps):
        north = basis_ref[pl.ds(c * rows + top, columns, stride=comps * rows), :]
        south = basis_ref[pl.ds(c * rows, columns, stride=comps * rows), :]
        north = north * mask[c][top : top + 1, :]
        south = south * mask[c][0:1, :]
        rowa_ref[c * columns : (c + 1) * columns, :] = pick(even_row, north, south)
        rowb_ref[c * columns : (c + 1) * columns, :] = pick(even_row, south, north)
    north = [mask[c][top : top + 1, :] * rhs[c][top : top + 1, :] for c in range(comps)]
    south = [mask[c][0:1, :] * rhs[c][0:1, :] for c in range(comps)]
    north += [visc[top : top + 1, :], visc[top - 1 : top, :]]
    south += [visc[0:1, :], visc[1:2, :]]
    for i in range(comps + 2):
        at = comps * columns + i
        rowa_ref[at : at + 1, :] = pick(even_row, north[i], south[i])
        rowb_ref[at : at + 1, :] = pick(even_row, south[i], north[i])
    rest = comps * columns + comps + 2
    blank = jnp.zeros((rowa_ref.shape[0] - rest, cols), F32)
    rowa_ref[rest:, :] = blank
    rowb_ref[rest:, :] = blank

    for c in range(comps):
        east, west = (jnp.zeros((rows, cols), F32), jnp.zeros((rows, cols), F32))
        for k in range(columns):
            base = (k * comps + c) * rows
            tile = basis_ref[base : base + rows, :]
            east = jnp.where(lane == k, pltpu.roll(tile, (k - low) % cols, 1), east)
            west = jnp.where(lane == k, tile if k == 0 else pltpu.roll(tile, k, 1), west)
        east = jnp.where(lane == columns, rhs[c][:, low : low + 1], east)
        west = jnp.where(lane == columns, rhs[c][:, 0:1], west)
        east = east * mask[c][:, low : low + 1]
        west = west * mask[c][:, 0:1]
        cola_ref[c * rows : (c + 1) * rows, :] = pick(even_col, east, west)
        colb_ref[c * rows : (c + 1) * rows, :] = pick(even_col, west, east)
    east = jnp.where(lane == 0, visc[:, low : low + 1], visc[:, low - 1 : low])
    west = jnp.where(lane == 0, visc[:, 0:1], visc[:, 1:2])
    cola_ref[comps * rows :, :] = pick(even_col, east, west)
    colb_ref[comps * rows :, :] = pick(even_col, west, east)


def stencil(mask, faces, diagonal, tile, halo):
    masked = mask * tile
    near = shifts(masked, *halo)
    inner = diagonal * masked - (
        faces[0] * near[0] + faces[1] * near[1] + faces[2] * near[2] + faces[3] * near[3]
    )
    return mask * inner + (1.0 - mask) * tile


def split(values):
    high = values.astype(jnp.bfloat16)
    return jnp.concatenate([high, (values - high.astype(F32)).astype(jnp.bfloat16)], axis=0)


def gram_kernel(sizes, basis_ref, rhs_ref, mask_ref, visc_ref, gram_ref, rowa_ref, rowb_ref,
                cola_ref, colb_ref, owna_ref, ownb_ref, send_ref, acc_ref, full_ref):
    columns, comps, rows, cols = sizes
    at_row, at_col = (lax.axis_index("row"), lax.axis_index("col"))
    even_row, even_col = (1 - lax.rem(at_row, 2), 1 - lax.rem(at_col, 2))
    has_north, has_south, has_east, has_west = flags()
    top, low, half = (rows - 1, cols - 1, cols // 2)
    rhs = [rhs_ref[c * rows : (c + 1) * rows, :] for c in range(comps)]
    mask = [mask_ref[c * rows : (c + 1) * rows, :].astype(F32) for c in range(comps)]
    visc = visc_ref[...]
    lane, lanes = (iota((rows, cols), 1), iota((1, cols), 1))

    at = comps * columns + comps
    tail_a, tail_b = (rowa_ref[at : at + 1, :], rowb_ref[at : at + 1, :])
    v_north = pick(even_row, tail_a, tail_b) * has_north
    v_south = pick(even_row, tail_b, tail_a) * has_south
    side_a, side_b = (cola_ref[...], colb_ref[...])
    east_side = pick(even_col, side_a, side_b) * has_east
    west_side = pick(even_col, side_b, side_a) * has_west
    own_a, own_b = (owna_ref[...], ownb_ref[...])
    own_east, own_west = (pick(even_col, own_a, own_b), pick(even_col, own_b, own_a))
    v_east, v_west = (east_side[comps * rows :, 0:1], west_side[comps * rows :, 0:1])
    faces = [0.5 * (visc + v) for v in shifts(visc, v_north, v_south, v_east, v_west)]
    diagonal = 1.0 + faces[0] + faces[1] + faces[2] + faces[3]

    blocks = jnp.zeros((2 * columns, 2 * columns), F32)
    for c in range(comps):
        m = mask[c]
        own = m * diagonal + (1.0 - m)
        up, down = (m * faces[0], m * faces[1])
        right = jnp.where(lane == low, 0.0, m * faces[2])
        left = jnp.where(lane == 0, 0.0, m * faces[3])
        span = slice(c * columns, (c + 1) * columns)
        halo_a, halo_b = (rowa_ref[span, :], rowb_ref[span, :])
        plain = [
            basis_ref[pl.ds(c * rows + i, columns, stride=comps * rows), :] for i in range(rows)
        ]
        free = [plain[i] * m[i : i + 1, :] for i in range(rows)]
        free.append(pick(even_row, halo_a, halo_b) * has_north)
        free.append(pick(even_row, halo_b, halo_a) * has_south)
        for i in range(0, rows, 2):
            lefts, rights = ([], [])
            for j in (i, i + 1):
                here = slice(j, j + 1)
                value = own[here] * plain[j] - up[here] * free[j + 1] - down[here] * free[j - 1]
                value = value - right[here] * pltpu.roll(free[j], low, 1)
                value = value - left[here] * pltpu.roll(free[j], 1, 1)
                lefts.append(split(plain[j]))
                rights.append(split(value))
            blocks = blocks + lax.dot_general(
                jnp.concatenate(lefts, axis=1),
                jnp.concatenate(rights, axis=1),
                (((1,), (1,)), ((), ())),
                preferred_element_type=F32,
            )
    east_face = jnp.concatenate([faces[2][:, low : low + 1]] * comps, axis=0)
    west_face = jnp.concatenate([faces[3][:, 0:1]] * comps, axis=0)
    field = comps * rows
    ours = jnp.concatenate([own_east[:field] * east_face, own_west[:field] * west_face], axis=0)
    theirs = jnp.concatenate([east_side[:field], west_side[:field]], axis=0)
    edge = lax.dot_general(
        ours, theirs, (((0,), (0,)), ((), ())),
        preferred_element_type=F32, precision=lax.Precision.HIGHEST,
    )
    blocks = blocks + pltpu.roll(blocks, half, 1)
    wide_lane = iota((columns, cols), 1)
    edge = jnp.where(wide_lane < half, edge[:columns], 0.0)
    full = blocks[:columns] + blocks[columns:] - edge - pltpu.roll(edge, half, 1)
    full_ref[...] = full
    spot = jnp.where(wide_lane >= half, wide_lane - half, wide_lane) == iota((columns, cols), 0)
    spine = jnp.sum(jnp.where(spot, full, 0.0), axis=0, keepdims=True)
    count = columns // 2
    chunk = jnp.where(
        iota((count, cols), 1) < half,
        full_ref[pl.ds(0, count, stride=2), :],
        full_ref[pl.ds(1, count, stride=2), :],
    )
    dots = to_row(project(basis_ref, rhs, acc_ref, columns, comps, rows))
    corner_row = jnp.zeros((1, cols), F32)
    for i, corner in enumerate(corners_of(visc)):
        corner_row = jnp.where(lanes == i, corner, corner_row)
    head = jnp.concatenate([jnp.where(lanes < half, dots, spine), gram_ref[...]], axis=0)
    for d in range(count):
        send_ref[d] = jnp.concatenate([head, chunk[d : d + 1, :], corner_row], axis=0)


def first_kernel(sizes, whole_rows, two, got_ref, *refs):
    columns, comps, rows, cols, scale = sizes
    if whole_rows:
        gram_in_ref = None
    else:
        gram_in_ref, *refs = refs
    (basis_ref, rhs_ref, mask_ref, visc_ref, rowa_ref, rowb_ref, cola_ref, colb_ref,
     send_ref, state_ref, face_ref, edge_ref, side_ref, small_ref, gram_ref,
     acc_ref, wide_ref) = refs
    at_row, at_col = (lax.axis_index("row"), lax.axis_index("col"))
    row_count, col_count = (lax.axis_size("row"), lax.axis_size("col"))
    even_row, even_col = (1 - lax.rem(at_row, 2), 1 - lax.rem(at_col, 2))
    me = at_row * col_count + at_col
    top, low = rows - 1, cols - 1
    rhs = [rhs_ref[c * rows : (c + 1) * rows, :] for c in range(comps)]
    mask = [mask_ref[c * rows : (c + 1) * rows, :].astype(F32) for c in range(comps)]
    visc = visc_ref[...]
    sub, lane = (iota((rows, cols), 0), iota((rows, cols), 1))
    lanes = iota((1, cols), 1)

    if whole_rows:
        per = cols // columns
        for r in range(row_count):
            for c in range(col_count):
                piece = got_ref[r * col_count + c, 1:2, :]
                for t in range(per):
                    at = (c * row_count + r) * per + t
                    moved = pltpu.roll(piece, cols - t * columns, 1) if t else piece
                    gram_ref[at : at + 1, :] = moved
    else:
        gram_ref[:, :columns] = gram_in_ref[...]
    all_sums = jnp.sum(got_ref[...], axis=0)
    sums = all_sums[0:1, :]
    dots = jnp.where(lanes < columns, sums, 0.0)
    gram = jnp.where(iota((columns, cols), 1) < columns, gram_ref[...], 0.0)
    coeffs = jnp.sum(gram * dots, axis=1, keepdims=True) * scale
    wide = jnp.broadcast_to(coeffs, (columns, cols))
    wide_ref[...] = wide
    coeff_row = to_row(coeffs)

    extra = comps * columns
    tail_a, tail_b = (rowa_ref[extra:, :], rowb_ref[extra:, :])
    has_north, has_south, has_east, has_west = flags()
    north_tail = pick(even_row, tail_a, tail_b) * has_north
    south_tail = pick(even_row, tail_b, tail_a) * has_south
    side_a, side_b = (cola_ref[...], colb_ref[...])
    east_side = pick(even_col, side_a, side_b) * has_east
    west_side = pick(even_col, side_b, side_a) * has_west
    v_north, v_south = (north_tail[comps : comps + 1, :], south_tail[comps : comps + 1, :])
    v_north2, v_south2 = (north_tail[comps + 1 : comps + 2, :], south_tail[comps + 1 : comps + 2, :])
    v_east, v_west = (east_side[comps * rows :, 0:1], west_side[comps * rows :, 0:1])
    v_east2, v_west2 = (east_side[comps * rows :, 1:2], west_side[comps * rows :, 1:2])
    faces = [0.5 * (visc + v) for v in shifts(visc, v_north, v_south, v_east, v_west)]
    diagonal = 1.0 + faces[0] + faces[1] + faces[2] + faces[3]
    face_ref[...] = jnp.concatenate(faces + [diagonal], axis=0)
    jacobi = [m / diagonal + (1.0 - m) for m in mask]

    def corner(step_row, step_col, which):
        r, c = (at_row + step_row, at_col + step_col)
        inside = (r >= 0) & (r < row_count) & (c >= 0) & (c < col_count)
        place = jnp.where(inside, r * col_count + c, me)
        line, first = (3, 0) if two else (0, columns)
        value = got_ref[place, line : line + 1, :]
        value = jnp.sum(jnp.where(lanes == first + which, value, 0.0), axis=1, keepdims=True)
        return value * jnp.where(inside, 1.0, 0.0)

    north_west, north_east = (corner(1, -1, 1), corner(1, 1, 0))
    south_west, south_east = (corner(-1, -1, 3), corner(-1, 1, 2))

    def row_inverse(own, inner, outer, west, east):
        right = jnp.where(lanes == low, east, pltpu.roll(own, low, 1))
        left = jnp.where(lanes == 0, west, pltpu.roll(own, 1, 1))
        return 1.0 / (1.0 + 0.5 * (4.0 * own + inner + outer + left + right))

    def side_inverse(own, inner, outer, south, north):
        own = jnp.broadcast_to(own, (rows, cols))
        up = jnp.where(sub == top, north, pltpu.roll(own, top, 0))
        down = jnp.where(sub == 0, south, pltpu.roll(own, 1, 0))
        return 1.0 / (1.0 + 0.5 * (4.0 * own + inner + outer + up + down))

    inv_north = row_inverse(v_north, visc[top : top + 1, :], v_north2, north_west, north_east)
    inv_south = row_inverse(v_south, visc[0:1, :], v_south2, south_west, south_east)
    inv_east = side_inverse(v_east, visc[:, low : low + 1], v_east2, south_east, north_east)
    inv_west = side_inverse(v_west, visc[:, 0:1], v_west2, south_west, north_west)

    corr = combine(basis_ref, wide_ref, columns, comps, rows)
    image, scaled, smooth, point = ([], [], [], [])
    smooth_image, scaled_image = ([], [])
    none = (jnp.zeros((1, cols), F32),) * 2 + (jnp.zeros((rows, 1), F32),) * 2
    for c in range(comps):
        span = slice(c * columns, (c + 1) * columns)
        sum_a = jnp.sum(wide * rowa_ref[span, :], axis=0, keepdims=True)
        sum_b = jnp.sum(wide * rowb_ref[span, :], axis=0, keepdims=True)
        u_north = inv_north * north_tail[c : c + 1, :]
        u_south = inv_south * south_tail[c : c + 1, :]
        p_north = u_north + has_north * pick(even_row, sum_a, sum_b)
        p_south = u_south + has_south * pick(even_row, sum_b, sum_a)
        here = slice(c * rows, (c + 1) * rows)
        east, west = (east_side[here, :], west_side[here, :])
        u_east = inv_east * east[:, columns : columns + 1]
        u_west = inv_west * west[:, columns : columns + 1]
        p_east = u_east + jnp.sum(coeff_row * east, axis=1, keepdims=True)
        p_west = u_west + jnp.sum(coeff_row * west, axis=1, keepdims=True)
        u = jacobi[c] * rhs[c]
        p = u + corr[c]
        q = stencil(mask[c], faces, diagonal, p, (p_north, p_south, p_east, p_west))
        if two:
            halo = (u_north, u_south, u_east, u_west)
            smooth_image.append(stencil(mask[c], faces, diagonal, u, halo))
            scaled_image.append(stencil(mask[c], faces, diagonal, jacobi[c] * q, none))
        smooth.append(u)
        point.append(p)
        image.append(q)
        scaled.append(jacobi[c] * q)
        for i, value in enumerate((u_north, u_south, p_north, p_south)):
            edge_ref[i * 8 + c : i * 8 + c + 1, :] = value
        for i, value in enumerate((u_east, u_west, p_east, p_west)):
            side_ref[(i * comps + c) * rows : (i * comps + c + 1) * rows, :] = value
    state_ref[...] = jnp.concatenate(smooth + point + image + scaled, axis=0)

    row = to_row(project(basis_ref, image, acc_ref, columns, comps, rows))
    pairs = ((point, image), (smooth, image), (image, scaled), (rhs, smooth))
    if two:
        pairs += ((smooth, smooth_image), (scaled, smooth_image), (scaled, scaled_image))
    for i, (left, right) in enumerate(pairs):
        value = left[0] * right[0]
        for c in range(1, comps):
            value = value + left[c] * right[c]
        row = jnp.where(lanes == (DOTS2 if two else DOTS) + i, total(value), row)
    masked = [mask[c] * scaled[c] for c in range(comps)]
    if two:
        norths = [m[top : top + 1, :] * faces[0][top : top + 1, :] * has_north for m in masked]
        easts = [m[:, low : low + 1] * faces[2][:, low : low + 1] * has_east for m in masked]
        souths, wests = ([m[0:1, :] for m in masked], [m[:, 0:1] for m in masked])
        row = row + to_row(jnp.concatenate(easts, axis=0), EAST2)
        row = row + to_row(jnp.concatenate(wests, axis=0), WEST2)
        reach = project(basis_ref, scaled_image, acc_ref, columns, comps, rows)
        beyond = jnp.zeros((columns, cols), F32)
        aside = jnp.zeros((rows, cols), F32)
        for c in range(comps):
            span, here = (slice(c * columns, (c + 1) * columns), slice(c * rows, (c + 1) * rows))
            halo_a, halo_b = (rowa_ref[span, :], rowb_ref[span, :])
            low_side = souths[c] * faces[1][0:1, :] * has_south
            beyond = beyond + norths[c] * pick(even_row, halo_a, halo_b)
            beyond = beyond + low_side * pick(even_row, halo_b, halo_a)
            aside = aside + easts[c] * east_side[here, :]
            aside = aside + wests[c] * faces[3][:, 0:1] * west_side[here, :]
        reach = to_row(reach - jnp.sum(beyond, axis=1, keepdims=True))
        reach = reach - jnp.where(lanes < columns, jnp.sum(aside, axis=0, keepdims=True), 0.0)
        half = cols // 2
        ours = jnp.broadcast_to(all_sums[2:3, :], (8, cols))
        other = pltpu.roll(ours, half, 1)
        wide_lane = iota((8, cols), 1)
        for t, (first, second) in enumerate(((ours, other), (other, ours))):
            value = jnp.where(wide_lane < half, first, second)
            turn = lax.rem(half + t * (half // 2) - (2 * me + t + 1) + 2 * cols, cols)
            value = pltpu.roll(value, turn, 1)[0:1, :]
            start = half + t * (half // 2)
            reach = jnp.where((lanes >= start) & (lanes < start + half // 2), value, reach)
        message = jnp.concatenate(norths + souths + [row, reach], axis=0)
        send_ref[...] = jnp.broadcast_to(message[None], send_ref.shape)
        spine = pltpu.roll(jnp.broadcast_to(sums, (8, cols)), half, 1)[0:1, :]
        spine = jnp.where(lanes < half, spine, 0.0)
        small_ref[...] = jnp.concatenate([dots, coeff_row, spine, jnp.zeros((5, cols), F32)], axis=0)
        return
    east = jnp.concatenate([m[:, low : low + 1] for m in masked], axis=0)
    west = jnp.concatenate([m[:, 0:1] for m in masked], axis=0)
    row = row + to_row(east, EAST) + to_row(west, WEST)
    message = jnp.concatenate([row] + [m[top : top + 1, :] for m in masked], axis=0)
    send_ref[...] = jnp.broadcast_to(message[None], send_ref.shape)
    message = jnp.concatenate([row] + [m[0:1, :] for m in masked], axis=0)
    send_ref[jnp.where(at_row > 0, me - col_count, me)] = message
    small_ref[...] = jnp.concatenate([dots, coeff_row, jnp.zeros((6, cols), F32)], axis=0)


def second_kernel(sizes, got_ref, basis_ref, rhs_ref, mask_ref, rowa_ref, rowb_ref, cola_ref,
                  colb_ref, state_ref, face_ref, edge_ref, side_ref, small_ref, gram_ref,
                  send_ref, out_ref, last_ref, wide_ref):
    columns, comps, rows, cols, scale = sizes
    at_row, at_col = (lax.axis_index("row"), lax.axis_index("col"))
    row_count, col_count = (lax.axis_size("row"), lax.axis_size("col"))
    even_row, even_col = (1 - lax.rem(at_row, 2), 1 - lax.rem(at_col, 2))
    me = at_row * col_count + at_col
    lanes = iota((1, cols), 1)
    mask = [mask_ref[c * rows : (c + 1) * rows, :].astype(F32) for c in range(comps)]

    sums = jnp.sum(got_ref[...], axis=0)[0:1, :]
    image_dots = jnp.where(lanes < columns, sums, 0.0)
    curve, cross, image_sq, rhs_sq = [
        jnp.sum(jnp.where(lanes == DOTS + i, sums, 0.0), axis=1, keepdims=True) for i in range(4)
    ]
    dots, coeff_row = (small_ref[0:1, :], small_ref[1:2, :])
    energy = rhs_sq + jnp.sum(dots * coeff_row, axis=1, keepdims=True)
    step = energy / curve
    gram = jnp.where(iota((columns, cols), 1) < columns, gram_ref[...], 0.0)
    dots = dots - step * image_dots
    coeffs = jnp.sum(gram * dots, axis=1, keepdims=True) * scale
    wide = jnp.broadcast_to(coeffs, (columns, cols))
    wide_ref[...] = wide
    coeff_row = to_row(coeffs)
    energy_new = rhs_sq - 2.0 * step * cross + step * step * image_sq
    energy_new = energy_new + jnp.sum(dots * coeff_row, axis=1, keepdims=True)
    ratio = energy_new / energy

    def beside(step_row, step_col):
        r, c = (at_row + step_row, at_col + step_col)
        inside = (r >= 0) & (r < row_count) & (c >= 0) & (c < col_count)
        message = got_ref[jnp.where(inside, r * col_count + c, me)]
        return message * jnp.where(inside, 1.0, 0.0)

    q_north, q_south = (beside(1, 0), beside(-1, 0))
    q_east = to_column(beside(0, 1)[0:1, :], comps * rows, WEST)
    q_west = to_column(beside(0, -1)[0:1, :], comps * rows, EAST)

    side_a, side_b = (cola_ref[...], colb_ref[...])
    has_north, has_south, has_east, has_west = flags()
    east_side = pick(even_col, side_a, side_b) * has_east
    west_side = pick(even_col, side_b, side_a) * has_west
    faces = [face_ref[i * rows : (i + 1) * rows, :] for i in range(4)]
    diagonal = face_ref[4 * rows : 5 * rows, :]
    corr = combine(basis_ref, wide_ref, columns, comps, rows)
    curve_part = jnp.zeros((rows, cols), F32)
    first, second, third, fourth = ([], [], [], [])
    for c in range(comps):
        span = slice(c * columns, (c + 1) * columns)
        here = slice(c * rows, (c + 1) * rows)
        sum_a = jnp.sum(wide * rowa_ref[span, :], axis=0, keepdims=True)
        sum_b = jnp.sum(wide * rowb_ref[span, :], axis=0, keepdims=True)
        old = [edge_ref[i * 8 + c : i * 8 + c + 1, :] for i in range(4)]
        p_north = old[0] - step * q_north[1 + c : 2 + c, :] + has_north * pick(even_row, sum_a, sum_b)
        p_south = old[1] - step * q_south[1 + c : 2 + c, :] + has_south * pick(even_row, sum_b, sum_a)
        p_north, p_south = (p_north + ratio * old[2], p_south + ratio * old[3])
        old = [side_ref[(i * comps + c) * rows : (i * comps + c + 1) * rows, :] for i in range(4)]
        p_east = old[0] - step * q_east[here] + ratio * old[2]
        p_west = old[1] - step * q_west[here] + ratio * old[3]
        p_east = p_east + jnp.sum(coeff_row * east_side[here, :], axis=1, keepdims=True)
        p_west = p_west + jnp.sum(coeff_row * west_side[here, :], axis=1, keepdims=True)
        u, p, q, jq = [
            state_ref[(i * comps + c) * rows : (i * comps + c + 1) * rows, :] for i in range(4)
        ]
        new = u - step * jq + corr[c] + ratio * p
        masked = mask[c] * new
        near = shifts(masked, p_north, p_south, p_east, p_west)
        stencil = diagonal * masked - (
            faces[0] * near[0] + faces[1] * near[1] + faces[2] * near[2] + faces[3] * near[3]
        )
        applied = mask[c] * stencil + (1.0 - mask[c]) * new
        curve_part = curve_part + new * applied
        first.append(step * p)
        second.append(new)
        third.append(rhs_ref[here, :] - step * q)
        fourth.append(applied)
    out_ref[...] = jnp.concatenate(first + second + third + fourth, axis=0)
    last_ref[...] = jnp.broadcast_to(energy_new, last_ref.shape)
    send_ref[...] = jnp.broadcast_to(total(curve_part)[None], send_ref.shape)


def close_kernel(sizes, got_ref, basis_ref, rhs_ref, mask_ref, rowa_ref, rowb_ref, cola_ref,
                 colb_ref, state_ref, face_ref, edge_ref, side_ref, small_ref, gram_ref,
                 solution_ref, residual_ref, wide_ref):
    columns, comps, rows, cols, scale = sizes
    at_row, at_col = (lax.axis_index("row"), lax.axis_index("col"))
    row_count, col_count = (lax.axis_size("row"), lax.axis_size("col"))
    devices = row_count * col_count
    even_row, even_col = (1 - lax.rem(at_row, 2), 1 - lax.rem(at_col, 2))
    has_north, has_south, has_east, has_west = flags()
    me = at_row * col_count + at_col
    half, quarter = (cols // 2, cols // 4)
    lanes = iota((1, cols), 1)
    mask = [mask_ref[c * rows : (c + 1) * rows, :].astype(F32) for c in range(comps)]

    def along(left, right):
        return jnp.sum(left * right, axis=1, keepdims=True)

    sums = jnp.sum(got_ref[...], axis=0)
    image_dots = jnp.where(lanes < columns, sums[2 * comps : 2 * comps + 1, :], 0.0)
    reach_dots = jnp.where(lanes < columns, sums[2 * comps + 1 :, :], 0.0)
    curve, cross, image_sq, rhs_sq, smooth_sq, mixed, scaled_sq = [
        along(jnp.where(lanes == DOTS2 + i, 1.0, 0.0), sums[2 * comps : 2 * comps + 1, :])
        for i in range(7)
    ]
    dots, old_row, spine = (small_ref[0:1, :], small_ref[1:2, :], small_ref[2:3, :])
    energy = rhs_sq + along(dots, old_row)
    step = energy / curve
    gram = jnp.where(iota((columns, cols), 1) < columns, gram_ref[...], 0.0)
    dots = dots - step * image_dots
    coeffs = jnp.sum(gram * dots, axis=1, keepdims=True) * scale
    wide = jnp.broadcast_to(coeffs, (columns, cols))
    wide_ref[...] = wide
    coeff_row = to_row(coeffs)
    energy_new = rhs_sq - 2.0 * step * cross + step * step * image_sq + along(dots, coeff_row)
    ratio = energy_new / energy

    border = jnp.zeros((2 * comps + 2, cols), F32)
    for d in range(devices - col_count):
        border = border + got_ref[d] * pltpu.roll(got_ref[d + col_count], comps + 2, 0)
    border = jnp.where(iota(border.shape, 0) < comps, border, 0.0)
    lines = got_ref[:, 2 * comps, :]
    later = pltpu.roll(pltpu.roll(lines, devices - 1, 0), cols - (WEST2 - EAST2), 1)
    line_lane = iota(lines.shape, 1)
    beside_it = jnp.where((line_lane >= EAST2) & (line_lane < WEST2), lines * later, 0.0)
    scaled_sq = scaled_sq - 2.0 * (total(border) + total(beside_it))

    packed = pltpu.roll(got_ref[:, 2 * comps + 1, :], half, 1)
    sub = iota(packed.shape, 0)

    def turned(row):
        value = jnp.broadcast_to(row, (8, cols))
        value = jnp.broadcast_to((value + pltpu.roll(value, half, 1))[0:1, :], packed.shape)
        bit = 1
        while bit < devices:
            value = jnp.where((sub & bit) != 0, pltpu.roll(value, cols - 2 * bit, 1), value)
            bit *= 2
        ahead = pltpu.roll(value, cols - 1, 1)
        ahead = jnp.where(line_lane < quarter, ahead, pltpu.roll(value, quarter - 2, 1))
        return (jnp.where(line_lane < quarter, value[:, 0:1], value[:, 1:2]), ahead)

    other_row = coeff_row - 2.0 * old_row
    (left, left_ahead), (right, right_ahead) = (turned(coeff_row), turned(other_row))
    weight = jnp.where((line_lane == quarter - 1) | (line_lane == half - 1), 0.5, 1.0)
    form = packed * weight * (left * right_ahead + right * left_ahead)
    form = total(jnp.where(line_lane < half, form, 0.0)) + along(spine * coeff_row, other_row)
    image_part = along(coeff_row, image_dots)
    curve_new = smooth_sq - 2.0 * step * mixed + step * step * scaled_sq
    curve_new = curve_new - 2.0 * step * along(coeff_row, reach_dots) + 2.0 * image_part + form
    curve_new = curve_new + 2.0 * ratio * (cross - step * image_sq + image_part)
    curve_new = curve_new + ratio * ratio * curve
    step_new = energy_new / curve_new

    def beside(step_row, step_col):
        r, c = (at_row + step_row, at_col + step_col)
        inside = (r >= 0) & (r < row_count) & (c >= 0) & (c < col_count)
        message = got_ref[jnp.where(inside, r * col_count + c, me)]
        return message * jnp.where(inside, 1.0, 0.0)

    faces = [face_ref[i * rows : (i + 1) * rows, :] for i in range(4)]
    diagonal = face_ref[4 * rows : 5 * rows, :]
    q_north, q_south = (beside(1, 0), beside(-1, 0))
    q_east = to_column(beside(0, 1)[2 * comps : 2 * comps + 1, :], comps * rows, WEST2)
    q_west = to_column(beside(0, -1)[2 * comps : 2 * comps + 1, :], comps * rows, EAST2)

    side_a, side_b = (cola_ref[...], colb_ref[...])
    east_side = pick(even_col, side_a, side_b) * has_east
    west_side = pick(even_col, side_b, side_a) * has_west
    corr = combine(basis_ref, wide_ref, columns, comps, rows)
    for c in range(comps):
        span = slice(c * columns, (c + 1) * columns)
        here = slice(c * rows, (c + 1) * rows)
        sum_a = jnp.sum(wide * rowa_ref[span, :], axis=0, keepdims=True)
        sum_b = jnp.sum(wide * rowb_ref[span, :], axis=0, keepdims=True)
        old = [edge_ref[i * 8 + c : i * 8 + c + 1, :] for i in range(4)]
        p_north = old[0] - step * q_north[comps + c : comps + c + 1, :]
        p_south = old[1] - step * (q_south[c : c + 1, :] / faces[1][0:1, :])
        p_north = p_north + has_north * pick(even_row, sum_a, sum_b) + ratio * old[2]
        p_south = p_south + has_south * pick(even_row, sum_b, sum_a) + ratio * old[3]
        old = [side_ref[(i * comps + c) * rows : (i * comps + c + 1) * rows, :] for i in range(4)]
        p_east = old[0] - step * q_east[here] + ratio * old[2]
        p_west = old[1] - step * (q_west[here] / faces[3][:, 0:1]) + ratio * old[3]
        p_east = p_east + jnp.sum(coeff_row * east_side[here, :], axis=1, keepdims=True)
        p_west = p_west + jnp.sum(coeff_row * west_side[here, :], axis=1, keepdims=True)
        u, p, q, jq = [
            state_ref[(i * comps + c) * rows : (i * comps + c + 1) * rows, :] for i in range(4)
        ]
        new = u - step * jq + corr[c] + ratio * p
        applied = stencil(mask[c], faces, diagonal, new, (p_north, p_south, p_east, p_west))
        solution_ref[here, :] = step * p + step_new * new
        residual_ref[here, :] = rhs_ref[here, :] - step * q - step_new * applied


def last_kernel(count, got_ref, in_ref, last_ref, solution_ref, residual_ref):
    step = last_ref[0:1, :] / jnp.sum(got_ref[...], axis=0)
    solution_ref[...] = in_ref[:count, :] + step * in_ref[count : 2 * count, :]
    residual_ref[...] = in_ref[2 * count : 3 * count, :] - step * in_ref[3 * count :, :]


def on_device(right_side, viscosity, free_mask, coarse_basis, gram_inverse):
    comps, rows, cols = right_side.shape
    columns = coarse_basis.shape[0]
    row_count, col_count = (lax.axis_size("row"), lax.axis_size("col"))
    devices = row_count * col_count
    scale = 1.0 / (32.0 * math.sqrt(float(comps * rows * cols * devices * columns)))
    sizes = (columns, comps, rows, cols)

    def call(kernel, outs, scratch, *args):
        return pl.pallas_call(
            kernel,
            out_shape=[jax.ShapeDtypeStruct(s, F32) for s in outs],
            in_specs=[VMEM] * len(args),
            out_specs=[VMEM] * len(outs),
            scratch_shapes=[pltpu.VMEM(s, F32) for s in scratch],
            compiler_params=pltpu.CompilerParams(vmem_limit_bytes=16 * 1024 * 1024),
        )(*args)

    def share(message):
        return lax.all_to_all(message, ("row", "col"), 0, 0, tiled=True)

    def swap(packet, axis, first):
        count = lax.axis_size(axis)
        pairs = [(i, i + 1) for i in range(first, count - 1, 2)]
        if first == 1 and count > 2 and count % 2 == 0:
            pairs.append((0, count - 1))
        return lax.ppermute(packet, axis, pairs + [(j, i) for i, j in pairs])

    basis = coarse_basis.reshape(columns * comps * rows, cols)
    rhs = right_side.reshape(comps * rows, cols)
    mask = free_mask.reshape(comps * rows, cols)

    block = gram_inverse.size
    piece = -(-block // row_count)
    flat = jnp.pad(gram_inverse.reshape(-1), (0, piece * row_count - block))
    own = lax.dynamic_slice_in_dim(flat, lax.axis_index("row") * piece, piece)
    own = jnp.pad(own, (0, cols - piece)).reshape(1, cols)

    tall = -(-(comps * columns + comps + 2) // 8) * 8
    wide = (comps + 1) * rows
    field = comps * rows
    two = columns * columns == devices * cols and cols == 2 * columns and rows == 8 and comps == 3
    if two:
        row_a, row_b, col_a, col_b = call(
            functools.partial(packet_kernel, sizes),
            [(tall, cols), (tall, cols), (wide, cols), (wide, cols)],
            [],
            basis, rhs, mask, viscosity,
        )
        halos = swap(row_a, "row", 0), swap(row_b, "row", 1), swap(col_a, "col", 0), swap(col_b, "col", 1)
        (send,) = call(
            functools.partial(gram_kernel, sizes),
            [(devices, 4, cols)],
            [(columns * rows, cols), (columns, cols)],
            basis, rhs, mask, viscosity, own, *halos, col_a, col_b,
        )
        sizes = sizes + (scale,)
        send, *state = call(
            functools.partial(first_kernel, sizes, True, True),
            [(devices, 8, cols), (4 * field, cols), (5 * rows, cols), (32, cols),
             (4 * field, cols), (8, cols), (columns, cols)],
            [(columns * rows, cols), (columns, cols)],
            share(send), basis, rhs, mask, viscosity, *halos,
        )
        solution, residual = call(
            functools.partial(close_kernel, sizes),
            [(field, cols), (field, cols)],
            [(columns, cols)],
            share(send), basis, rhs, mask, *halos, *state,
        )
        return (solution.reshape(right_side.shape), residual.reshape(right_side.shape))
    send, row_a, row_b, col_a, col_b = call(
        functools.partial(pack_kernel, sizes),
        [(devices, 2, cols), (tall, cols), (tall, cols), (wide, cols), (wide, cols)],
        [(columns * rows, cols)],
        basis, rhs, mask, viscosity, own,
    )
    halos = (swap(row_a, "row", 0), swap(row_b, "row", 1), swap(col_a, "col", 0), swap(col_b, "col", 1))
    got = share(send)
    whole_rows = piece == cols and cols % columns == 0 and block == piece * row_count
    gram = ()
    if not whole_rows:
        gram = got[:, 1, :piece].reshape(row_count, col_count, piece).transpose(1, 0, 2)
        gram = gram.reshape(col_count, row_count * piece)[:, :block].reshape(columns, columns)
        gram = (gram,)
    sizes = sizes + (scale,)
    send, *state = call(
        functools.partial(first_kernel, sizes, whole_rows, False),
        [(devices, 1 + comps, cols), (4 * field, cols), (5 * rows, cols), (32, cols),
         (4 * field, cols), (8, cols), (columns, cols)],
        [(columns * rows, cols), (columns, cols)],
        got, *gram, basis, rhs, mask, viscosity, *halos,
    )
    send, fields, last = call(
        functools.partial(second_kernel, sizes),
        [(devices, 1, cols), (4 * field, cols), (8, cols)],
        [(columns, cols)],
        share(send), basis, rhs, mask, *halos, *state,
    )
    solution, residual = call(
        functools.partial(last_kernel, field),
        [(field, cols), (field, cols)],
        [],
        share(send), fields, last,
    )
    return (solution.reshape(right_side.shape), residual.reshape(right_side.shape))


def solution(mesh):
    in_specs = (
        P(None, "row", "col"),
        P("row", "col"),
        P(None, "row", "col"),
        P(None, None, "row", "col"),
        P("col", None),
    )
    out_specs = (P(None, "row", "col"), P(None, "row", "col"))
    return jax.shard_map(
        on_device, mesh=mesh, in_specs=in_specs, out_specs=out_specs, check_vma=False
    )
```

```python
import functools
import math

import jax
import jax.numpy as jnp
from jax import lax
from jax.experimental import pallas as pl
from jax.experimental.pallas import tpu as pltpu
from jax.sharding import PartitionSpec as P


F32 = jnp.float32
VMEM = pl.BlockSpec(memory_space=pltpu.VMEM)
DOTS, EAST, WEST = 64, 72, 96
EAST2, WEST2, DOTS2 = 64, 88, 112


def flags():
    at_row, at_col = (lax.axis_index("row"), lax.axis_index("col"))
    tests = (
        at_row < lax.axis_size("row") - 1,
        at_row > 0,
        at_col < lax.axis_size("col") - 1,
        at_col > 0,
    )
    return [jnp.where(test, 1.0, 0.0) for test in tests]


def iota(shape, dim):
    return lax.broadcasted_iota(jnp.int32, shape, dim)


def pick(flag, yes, no):
    return jnp.where(jnp.full(yes.shape, flag, jnp.int32) == 1, yes, no)


def to_row(column, first=0):
    shape = (column.shape[0], 128)
    spread = jnp.where(iota(shape, 1) == iota(shape, 0) + first, column, 0.0)
    return jnp.sum(spread, axis=0, keepdims=True)


def to_column(row, count, first=0):
    shape = (count, 128)
    spread = jnp.where(iota(shape, 1) == iota(shape, 0) + first, row, 0.0)
    return jnp.sum(spread, axis=1, keepdims=True)


def total(values):
    return jnp.sum(jnp.sum(values, axis=0, keepdims=True), axis=1, keepdims=True)


def shifts(tile, north, south, east, west):
    rows, cols = tile.shape
    sub, lane = (iota(tile.shape, 0), iota(tile.shape, 1))
    return (
        jnp.where(sub == rows - 1, north, pltpu.roll(tile, rows - 1, 0)),
        jnp.where(sub == 0, south, pltpu.roll(tile, 1, 0)),
        jnp.where(lane == cols - 1, east, pltpu.roll(tile, cols - 1, 1)),
        jnp.where(lane == 0, west, pltpu.roll(tile, 1, 1)),
    )


def project(basis_ref, field, acc_ref, columns, comps, rows):
    for k in range(columns):
        base = k * comps * rows
        acc = basis_ref[base : base + rows, :] * field[0]
        for c in range(1, comps):
            acc = acc + basis_ref[base + c * rows : base + (c + 1) * rows, :] * field[c]
        acc_ref[k * rows : (k + 1) * rows, :] = acc
    sums = acc_ref[pl.ds(0, columns, stride=rows), :]
    for s in range(1, rows):
        sums = sums + acc_ref[pl.ds(s, columns, stride=rows), :]
    return jnp.sum(sums, axis=1, keepdims=True)


def combine(basis_ref, wide_ref, columns, comps, rows):
    out = [[None, None] for _ in range(comps)]
    for k in range(columns):
        weight = jnp.broadcast_to(wide_ref[k : k + 1, :], (rows, 128))
        for c in range(comps):
            base = (k * comps + c) * rows
            term = weight * basis_ref[base : base + rows, :]
            old = out[c][k % 2]
            out[c][k % 2] = term if old is None else old + term
    return [a + b for a, b in out]


def pack_kernel(sizes, basis_ref, rhs_ref, mask_ref, visc_ref, gram_ref,
                send_ref, rowa_ref, rowb_ref, cola_ref, colb_ref, acc_ref):
    columns, comps, rows, cols = sizes
    packet_kernel(sizes, basis_ref, rhs_ref, mask_ref, visc_ref, rowa_ref, rowb_ref, cola_ref, colb_ref)
    rhs = [rhs_ref[c * rows : (c + 1) * rows, :] for c in range(comps)]
    visc = visc_ref[...]

    row = to_row(project(basis_ref, rhs, acc_ref, columns, comps, rows))
    lanes = iota((1, cols), 1)
    for i, corner in enumerate(corners_of(visc)):
        row = jnp.where(lanes == columns + i, corner, row)
    both = jnp.concatenate([row, gram_ref[...]], axis=0)
    send_ref[...] = jnp.broadcast_to(both[None], send_ref.shape)


def piece_kernel(gram_ref, piece_ref):
    at = 2 * lax.axis_index("row")
    rows = [gram_ref[pl.ds(at + t, 1), :] for t in range(2)]
    piece_ref[...] = jnp.concatenate(rows, axis=1)


def packets_kernel(sizes, basis_ref, rhs_ref, mask_ref, visc_ref, first_ref, *packet_refs):
    packet_kernel(sizes, basis_ref, rhs_ref, mask_ref, visc_ref, *packet_refs)


def corners_of(visc):
    top, low = (visc.shape[0] - 1, visc.shape[1] - 1)
    return [visc[i : i + 1, j : j + 1] for i in (0, top) for j in (0, low)]


def packet_kernel(sizes, basis_ref, rhs_ref, mask_ref, visc_ref,
                  rowa_ref, rowb_ref, cola_ref, colb_ref):
    columns, comps, rows, cols = sizes
    even_row = 1 - lax.rem(lax.axis_index("row"), 2)
    even_col = 1 - lax.rem(lax.axis_index("col"), 2)
    rhs = [rhs_ref[c * rows : (c + 1) * rows, :] for c in range(comps)]
    mask = [mask_ref[c * rows : (c + 1) * rows, :].astype(F32) for c in range(comps)]
    visc = visc_ref[...]
    lane = iota((rows, cols), 1)
    top, low = rows - 1, cols - 1

    for c in range(comps):
        north = basis_ref[pl.ds(c * rows + top, columns, stride=comps * rows), :]
        south = basis_ref[pl.ds(c * rows, columns, stride=comps * rows), :]
        north = north * mask[c][top : top + 1, :]
        south = south * mask[c][0:1, :]
        rowa_ref[c * columns : (c + 1) * columns, :] = pick(even_row, north, south)
        rowb_ref[c * columns : (c + 1) * columns, :] = pick(even_row, south, north)
    north = [mask[c][top : top + 1, :] * rhs[c][top : top + 1, :] for c in range(comps)]
    south = [mask[c][0:1, :] * rhs[c][0:1, :] for c in range(comps)]
    north += [visc[top : top + 1, :], visc[top - 1 : top, :]]
    south += [visc[0:1, :], visc[1:2, :]]
    for i in range(comps + 2):
        at = comps * columns + i
        rowa_ref[at : at + 1, :] = pick(even_row, north[i], south[i])
        rowb_ref[at : at + 1, :] = pick(even_row, south[i], north[i])
    rest = comps * columns + comps + 2
    blank = jnp.zeros((rowa_ref.shape[0] - rest, cols), F32)
    rowa_ref[rest:, :] = blank
    rowb_ref[rest:, :] = blank

    for c in range(comps):
        east, west = (jnp.zeros((rows, cols), F32), jnp.zeros((rows, cols), F32))
        for k in range(columns):
            base = (k * comps + c) * rows
            tile = basis_ref[base : base + rows, :]
            east = jnp.where(lane == k, pltpu.roll(tile, (k - low) % cols, 1), east)
            west = jnp.where(lane == k, tile if k == 0 else pltpu.roll(tile, k, 1), west)
        east = jnp.where(lane == columns, rhs[c][:, low : low + 1], east)
        west = jnp.where(lane == columns, rhs[c][:, 0:1], west)
        east = east * mask[c][:, low : low + 1]
        west = west * mask[c][:, 0:1]
        cola_ref[c * rows : (c + 1) * rows, :] = pick(even_col, east, west)
        colb_ref[c * rows : (c + 1) * rows, :] = pick(even_col, west, east)
    east = jnp.where(lane == 0, visc[:, low : low + 1], visc[:, low - 1 : low])
    west = jnp.where(lane == 0, visc[:, 0:1], visc[:, 1:2])
    cola_ref[comps * rows :, :] = pick(even_col, east, west)
    colb_ref[comps * rows :, :] = pick(even_col, west, east)


def stencil(mask, faces, diagonal, tile, halo):
    masked = mask * tile
    near = shifts(masked, *halo)
    inner = diagonal * masked - (
        faces[0] * near[0] + faces[1] * near[1] + faces[2] * near[2] + faces[3] * near[3]
    )
    return mask * inner + (1.0 - mask) * tile


def split(values):
    high = values.astype(jnp.bfloat16)
    return jnp.concatenate([high, (values - high.astype(F32)).astype(jnp.bfloat16)], axis=0)


def gram_kernel(sizes, basis_ref, rhs_ref, mask_ref, visc_ref, gram_ref, rowa_ref, rowb_ref,
                cola_ref, colb_ref, owna_ref, ownb_ref, send_ref, acc_ref, full_ref):
    columns, comps, rows, cols = sizes
    at_row, at_col = (lax.axis_index("row"), lax.axis_index("col"))
    even_row, even_col = (1 - lax.rem(at_row, 2), 1 - lax.rem(at_col, 2))
    has_north, has_south, has_east, has_west = flags()
    low, half = (cols - 1, cols // 2)
    rhs = [rhs_ref[c * rows : (c + 1) * rows, :] for c in range(comps)]
    mask = [mask_ref[c * rows : (c + 1) * rows, :].astype(F32) for c in range(comps)]
    visc = visc_ref[...]
    lane, lanes = (iota((rows, cols), 1), iota((1, cols), 1))

    at = comps * columns + comps
    tail_a, tail_b = (rowa_ref[at : at + 1, :], rowb_ref[at : at + 1, :])
    v_north = pick(even_row, tail_a, tail_b) * has_north
    v_south = pick(even_row, tail_b, tail_a) * has_south
    side_a, side_b = (cola_ref[...], colb_ref[...])
    east_side = pick(even_col, side_a, side_b) * has_east
    west_side = pick(even_col, side_b, side_a) * has_west
    own_a, own_b = (owna_ref[...], ownb_ref[...])
    own_east, own_west = (pick(even_col, own_a, own_b), pick(even_col, own_b, own_a))
    v_east, v_west = (east_side[comps * rows :, 0:1], west_side[comps * rows :, 0:1])
    faces = [0.5 * (visc + v) for v in shifts(visc, v_north, v_south, v_east, v_west)]
    diagonal = 1.0 + faces[0] + faces[1] + faces[2] + faces[3]

    blocks = jnp.zeros((2 * columns, 2 * columns), F32)
    for c in range(comps):
        m = mask[c]
        own = m * diagonal + (1.0 - m)
        up, down = (m * faces[0], m * faces[1])
        right = jnp.where(lane == low, 0.0, m * faces[2])
        left = jnp.where(lane == 0, 0.0, m * faces[3])
        span = slice(c * columns, (c + 1) * columns)
        halo_a, halo_b = (rowa_ref[span, :], rowb_ref[span, :])
        plain = [
            basis_ref[pl.ds(c * rows + i, columns, stride=comps * rows), :] for i in range(rows)
        ]
        free = [plain[i] * m[i : i + 1, :] for i in range(rows)]
        free.append(pick(even_row, halo_a, halo_b) * has_north)
        free.append(pick(even_row, halo_b, halo_a) * has_south)
        for i in range(0, rows, 2):
            lefts, rights = ([], [])
            for j in (i, i + 1):
                here = slice(j, j + 1)
                value = own[here] * plain[j] - up[here] * free[j + 1] - down[here] * free[j - 1]
                value = value - right[here] * pltpu.roll(free[j], low, 1)
                value = value - left[here] * pltpu.roll(free[j], 1, 1)
                lefts.append(split(plain[j]))
                rights.append(split(value))
            blocks = blocks + lax.dot_general(
                jnp.concatenate(lefts, axis=1),
                jnp.concatenate(rights, axis=1),
                (((1,), (1,)), ((), ())),
                preferred_element_type=F32,
            )
    east_face = jnp.concatenate([faces[2][:, low : low + 1]] * comps, axis=0)
    west_face = jnp.concatenate([faces[3][:, 0:1]] * comps, axis=0)
    field = comps * rows
    ours = jnp.concatenate([own_east[:field] * east_face, own_west[:field] * west_face], axis=0)
    theirs = jnp.concatenate([east_side[:field], west_side[:field]], axis=0)
    edge = lax.dot_general(
        ours, theirs, (((0,), (0,)), ((), ())),
        preferred_element_type=F32, precision=lax.Precision.HIGHEST,
    )
    blocks = blocks + pltpu.roll(blocks, half, 1)
    wide_lane = iota((columns, cols), 1)
    edge = jnp.where(wide_lane < half, edge[:columns], 0.0)
    full = blocks[:columns] + blocks[columns:] - edge - pltpu.roll(edge, half, 1)
    full_ref[...] = full
    spot = jnp.where(wide_lane >= half, wide_lane - half, wide_lane) == iota((columns, cols), 0)
    spine = jnp.sum(jnp.where(spot, full, 0.0), axis=0, keepdims=True)
    count = columns // 2
    chunk = jnp.where(
        iota((count, cols), 1) < half,
        full_ref[pl.ds(0, count, stride=2), :],
        full_ref[pl.ds(1, count, stride=2), :],
    )
    dots = to_row(project(basis_ref, rhs, acc_ref, columns, comps, rows))
    corner_row = jnp.zeros((1, cols), F32)
    for i, corner in enumerate(corners_of(visc)):
        corner_row = jnp.where(lanes == i, corner, corner_row)
    head = jnp.concatenate([jnp.where(lanes < half, dots, spine), gram_ref[...]], axis=0)
    for d in range(count):
        send_ref[d] = jnp.concatenate([head, chunk[d : d + 1, :], corner_row], axis=0)


def first_kernel(sizes, whole_rows, two, got_ref, *refs):
    columns, comps, rows, cols, scale = sizes
    if whole_rows:
        gram_in_ref = None
    else:
        gram_in_ref, *refs = refs
    (basis_ref, rhs_ref, mask_ref, visc_ref, rowa_ref, rowb_ref, cola_ref, colb_ref,
     send_ref, state_ref, face_ref, edge_ref, side_ref, small_ref, gram_ref,
     acc_ref, wide_ref) = refs
    at_row, at_col = (lax.axis_index("row"), lax.axis_index("col"))
    row_count, col_count = (lax.axis_size("row"), lax.axis_size("col"))
    even_row, even_col = (1 - lax.rem(at_row, 2), 1 - lax.rem(at_col, 2))
    me = at_row * col_count + at_col
    top, low = rows - 1, cols - 1
    rhs = [rhs_ref[c * rows : (c + 1) * rows, :] for c in range(comps)]
    mask = [mask_ref[c * rows : (c + 1) * rows, :].astype(F32) for c in range(comps)]
    visc = visc_ref[...]
    sub, lane = (iota((rows, cols), 0), iota((rows, cols), 1))
    lanes = iota((1, cols), 1)

    if whole_rows:
        per = cols // columns
        for r in range(row_count):
            for c in range(col_count):
                piece = got_ref[r * col_count + c, 1:2, :]
                for t in range(per):
                    at = (c * row_count + r) * per + t
                    moved = pltpu.roll(piece, cols - t * columns, 1) if t else piece
                    gram_ref[at : at + 1, :] = moved
    else:
        gram_ref[:, :columns] = gram_in_ref[...]
    all_sums = jnp.sum(got_ref[...], axis=0)
    sums = all_sums[0:1, :]
    dots = jnp.where(lanes < columns, sums, 0.0)
    gram = jnp.where(iota((columns, cols), 1) < columns, gram_ref[...], 0.0)
    coeffs = jnp.sum(gram * dots, axis=1, keepdims=True) * scale
    wide = jnp.broadcast_to(coeffs, (columns, cols))
    wide_ref[...] = wide
    coeff_row = to_row(coeffs)

    extra = comps * columns
    tail_a, tail_b = (rowa_ref[extra:, :], rowb_ref[extra:, :])
    has_north, has_south, has_east, has_west = flags()
    north_tail = pick(even_row, tail_a, tail_b) * has_north
    south_tail = pick(even_row, tail_b, tail_a) * has_south
    side_a, side_b = (cola_ref[...], colb_ref[...])
    east_side = pick(even_col, side_a, side_b) * has_east
    west_side = pick(even_col, side_b, side_a) * has_west
    v_north, v_south = (north_tail[comps : comps + 1, :], south_tail[comps : comps + 1, :])
    v_north2, v_south2 = (north_tail[comps + 1 : comps + 2, :], south_tail[comps + 1 : comps + 2, :])
    v_east, v_west = (east_side[comps * rows :, 0:1], west_side[comps * rows :, 0:1])
    v_east2, v_west2 = (east_side[comps * rows :, 1:2], west_side[comps * rows :, 1:2])
    faces = [0.5 * (visc + v) for v in shifts(visc, v_north, v_south, v_east, v_west)]
    diagonal = 1.0 + faces[0] + faces[1] + faces[2] + faces[3]
    face_ref[...] = jnp.concatenate(faces + [diagonal], axis=0)
    jacobi = [m / diagonal + (1.0 - m) for m in mask]

    def corner(step_row, step_col, which):
        r, c = (at_row + step_row, at_col + step_col)
        inside = (r >= 0) & (r < row_count) & (c >= 0) & (c < col_count)
        place = jnp.where(inside, r * col_count + c, me)
        line, first = (3, 0) if two else (0, columns)
        value = got_ref[place, line : line + 1, :]
        value = jnp.sum(jnp.where(lanes == first + which, value, 0.0), axis=1, keepdims=True)
        return value * jnp.where(inside, 1.0, 0.0)

    north_west, north_east = (corner(1, -1, 1), corner(1, 1, 0))
    south_west, south_east = (corner(-1, -1, 3), corner(-1, 1, 2))

    def row_inverse(own, inner, outer, west, east):
        right = jnp.where(lanes == low, east, pltpu.roll(own, low, 1))
        left = jnp.where(lanes == 0, west, pltpu.roll(own, 1, 1))
        return 1.0 / (1.0 + 0.5 * (4.0 * own + inner + outer + left + right))

    def side_inverse(own, inner, outer, south, north):
        own = jnp.broadcast_to(own, (rows, cols))
        up = jnp.where(sub == top, north, pltpu.roll(own, top, 0))
        down = jnp.where(sub == 0, south, pltpu.roll(own, 1, 0))
        return 1.0 / (1.0 + 0.5 * (4.0 * own + inner + outer + up + down))

    inv_north = row_inverse(v_north, visc[top : top + 1, :], v_north2, north_west, north_east)
    inv_south = row_inverse(v_south, visc[0:1, :], v_south2, south_west, south_east)
    inv_east = side_inverse(v_east, visc[:, low : low + 1], v_east2, south_east, north_east)
    inv_west = side_inverse(v_west, visc[:, 0:1], v_west2, south_west, north_west)

    corr = combine(basis_ref, wide_ref, columns, comps, rows)
    image, scaled, smooth, point = ([], [], [], [])
    smooth_image, scaled_image = ([], [])
    none = (jnp.zeros((1, cols), F32),) * 2 + (jnp.zeros((rows, 1), F32),) * 2
    for c in range(comps):
        span = slice(c * columns, (c + 1) * columns)
        sum_a = jnp.sum(wide * rowa_ref[span, :], axis=0, keepdims=True)
        sum_b = jnp.sum(wide * rowb_ref[span, :], axis=0, keepdims=True)
        u_north = inv_north * north_tail[c : c + 1, :]
        u_south = inv_south * south_tail[c : c + 1, :]
        p_north = u_north + has_north * pick(even_row, sum_a, sum_b)
        p_south = u_south + has_south * pick(even_row, sum_b, sum_a)
        here = slice(c * rows, (c + 1) * rows)
        east, west = (east_side[here, :], west_side[here, :])
        u_east = inv_east * east[:, columns : columns + 1]
        u_west = inv_west * west[:, columns : columns + 1]
        p_east = u_east + jnp.sum(coeff_row * east, axis=1, keepdims=True)
        p_west = u_west + jnp.sum(coeff_row * west, axis=1, keepdims=True)
        u = jacobi[c] * rhs[c]
        p = u + corr[c]
        q = stencil(mask[c], faces, diagonal, p, (p_north, p_south, p_east, p_west))
        if two:
            halo = (u_north, u_south, u_east, u_west)
            smooth_image.append(stencil(mask[c], faces, diagonal, u, halo))
            scaled_image.append(stencil(mask[c], faces, diagonal, jacobi[c] * q, none))
        smooth.append(u)
        point.append(p)
        image.append(q)
        scaled.append(jacobi[c] * q)
        for i, value in enumerate((u_north, u_south, p_north, p_south)):
            edge_ref[i * 8 + c : i * 8 + c + 1, :] = value
        for i, value in enumerate((u_east, u_west, p_east, p_west)):
            side_ref[(i * comps + c) * rows : (i * comps + c + 1) * rows, :] = value
    state_ref[...] = jnp.concatenate(smooth + point + image + scaled, axis=0)

    row = to_row(project(basis_ref, image, acc_ref, columns, comps, rows))
    pairs = ((point, image), (smooth, image), (image, scaled), (rhs, smooth))
    if two:
        pairs += ((smooth, smooth_image), (scaled, smooth_image), (scaled, scaled_image))
    for i, (left, right) in enumerate(pairs):
        value = left[0] * right[0]
        for c in range(1, comps):
            value = value + left[c] * right[c]
        row = jnp.where(lanes == (DOTS2 if two else DOTS) + i, total(value), row)
    masked = [mask[c] * scaled[c] for c in range(comps)]
    if two:
        norths = [m[top : top + 1, :] * faces[0][top : top + 1, :] * has_north for m in masked]
        easts = [m[:, low : low + 1] * faces[2][:, low : low + 1] * has_east for m in masked]
        souths, wests = ([m[0:1, :] for m in masked], [m[:, 0:1] for m in masked])
        row = row + to_row(jnp.concatenate(easts, axis=0), EAST2)
        row = row + to_row(jnp.concatenate(wests, axis=0), WEST2)
        reach = project(basis_ref, scaled_image, acc_ref, columns, comps, rows)
        beyond = jnp.zeros((columns, cols), F32)
        aside = jnp.zeros((rows, cols), F32)
        for c in range(comps):
            span, here = (slice(c * columns, (c + 1) * columns), slice(c * rows, (c + 1) * rows))
            halo_a, halo_b = (rowa_ref[span, :], rowb_ref[span, :])
            low_side = souths[c] * faces[1][0:1, :] * has_south
            beyond = beyond + norths[c] * pick(even_row, halo_a, halo_b)
            beyond = beyond + low_side * pick(even_row, halo_b, halo_a)
            aside = aside + easts[c] * east_side[here, :]
            aside = aside + wests[c] * faces[3][:, 0:1] * west_side[here, :]
        reach = to_row(reach - jnp.sum(beyond, axis=1, keepdims=True))
        reach = reach - jnp.where(lanes < columns, jnp.sum(aside, axis=0, keepdims=True), 0.0)
        half = cols // 2
        ours = jnp.broadcast_to(all_sums[2:3, :], (8, cols))
        other = pltpu.roll(ours, half, 1)
        wide_lane = iota((8, cols), 1)
        for t, (first, second) in enumerate(((ours, other), (other, ours))):
            value = jnp.where(wide_lane < half, first, second)
            turn = lax.rem(half + t * (half // 2) - (2 * me + t + 1) + 2 * cols, cols)
            value = pltpu.roll(value, turn, 1)[0:1, :]
            start = half + t * (half // 2)
            reach = jnp.where((lanes >= start) & (lanes < start + half // 2), value, reach)
        message = jnp.concatenate(norths + souths + [row, reach], axis=0)
        send_ref[...] = jnp.broadcast_to(message[None], send_ref.shape)
        spine = pltpu.roll(jnp.broadcast_to(sums, (8, cols)), half, 1)[0:1, :]
        spine = jnp.where(lanes < half, spine, 0.0)
        small_ref[...] = jnp.concatenate([dots, coeff_row, spine, jnp.zeros((5, cols), F32)], axis=0)
        return
    east = jnp.concatenate([m[:, low : low + 1] for m in masked], axis=0)
    west = jnp.concatenate([m[:, 0:1] for m in masked], axis=0)
    row = row + to_row(east, EAST) + to_row(west, WEST)
    message = jnp.concatenate([row] + [m[top : top + 1, :] for m in masked], axis=0)
    send_ref[...] = jnp.broadcast_to(message[None], send_ref.shape)
    message = jnp.concatenate([row] + [m[0:1, :] for m in masked], axis=0)
    send_ref[jnp.where(at_row > 0, me - col_count, me)] = message
    small_ref[...] = jnp.concatenate([dots, coeff_row, jnp.zeros((6, cols), F32)], axis=0)


def second_kernel(sizes, got_ref, basis_ref, rhs_ref, mask_ref, rowa_ref, rowb_ref, cola_ref,
                  colb_ref, state_ref, face_ref, edge_ref, side_ref, small_ref, gram_ref,
                  send_ref, out_ref, last_ref, wide_ref):
    columns, comps, rows, cols, scale = sizes
    at_row, at_col = (lax.axis_index("row"), lax.axis_index("col"))
    row_count, col_count = (lax.axis_size("row"), lax.axis_size("col"))
    even_row, even_col = (1 - lax.rem(at_row, 2), 1 - lax.rem(at_col, 2))
    me = at_row * col_count + at_col
    lanes = iota((1, cols), 1)
    mask = [mask_ref[c * rows : (c + 1) * rows, :].astype(F32) for c in range(comps)]

    sums = jnp.sum(got_ref[...], axis=0)[0:1, :]
    image_dots = jnp.where(lanes < columns, sums, 0.0)
    curve, cross, image_sq, rhs_sq = [
        jnp.sum(jnp.where(lanes == DOTS + i, sums, 0.0), axis=1, keepdims=True) for i in range(4)
    ]
    dots, coeff_row = (small_ref[0:1, :], small_ref[1:2, :])
    energy = rhs_sq + jnp.sum(dots * coeff_row, axis=1, keepdims=True)
    step = energy / curve
    gram = jnp.where(iota((columns, cols), 1) < columns, gram_ref[...], 0.0)
    dots = dots - step * image_dots
    coeffs = jnp.sum(gram * dots, axis=1, keepdims=True) * scale
    wide = jnp.broadcast_to(coeffs, (columns, cols))
    wide_ref[...] = wide
    coeff_row = to_row(coeffs)
    energy_new = rhs_sq - 2.0 * step * cross + step * step * image_sq
    energy_new = energy_new + jnp.sum(dots * coeff_row, axis=1, keepdims=True)
    ratio = energy_new / energy

    def beside(step_row, step_col):
        r, c = (at_row + step_row, at_col + step_col)
        inside = (r >= 0) & (r < row_count) & (c >= 0) & (c < col_count)
        message = got_ref[jnp.where(inside, r * col_count + c, me)]
        return message * jnp.where(inside, 1.0, 0.0)

    q_north, q_south = (beside(1, 0), beside(-1, 0))
    q_east = to_column(beside(0, 1)[0:1, :], comps * rows, WEST)
    q_west = to_column(beside(0, -1)[0:1, :], comps * rows, EAST)

    side_a, side_b = (cola_ref[...], colb_ref[...])
    has_north, has_south, has_east, has_west = flags()
    east_side = pick(even_col, side_a, side_b) * has_east
    west_side = pick(even_col, side_b, side_a) * has_west
    faces = [face_ref[i * rows : (i + 1) * rows, :] for i in range(4)]
    diagonal = face_ref[4 * rows : 5 * rows, :]
    corr = combine(basis_ref, wide_ref, columns, comps, rows)
    curve_part = jnp.zeros((rows, cols), F32)
    first, second, third, fourth = ([], [], [], [])
    for c in range(comps):
        span = slice(c * columns, (c + 1) * columns)
        here = slice(c * rows, (c + 1) * rows)
        sum_a = jnp.sum(wide * rowa_ref[span, :], axis=0, keepdims=True)
        sum_b = jnp.sum(wide * rowb_ref[span, :], axis=0, keepdims=True)
        old = [edge_ref[i * 8 + c : i * 8 + c + 1, :] for i in range(4)]
        p_north = old[0] - step * q_north[1 + c : 2 + c, :] + has_north * pick(even_row, sum_a, sum_b)
        p_south = old[1] - step * q_south[1 + c : 2 + c, :] + has_south * pick(even_row, sum_b, sum_a)
        p_north, p_south = (p_north + ratio * old[2], p_south + ratio * old[3])
        old = [side_ref[(i * comps + c) * rows : (i * comps + c + 1) * rows, :] for i in range(4)]
        p_east = old[0] - step * q_east[here] + ratio * old[2]
        p_west = old[1] - step * q_west[here] + ratio * old[3]
        p_east = p_east + jnp.sum(coeff_row * east_side[here, :], axis=1, keepdims=True)
        p_west = p_west + jnp.sum(coeff_row * west_side[here, :], axis=1, keepdims=True)
        u, p, q, jq = [
            state_ref[(i * comps + c) * rows : (i * comps + c + 1) * rows, :] for i in range(4)
        ]
        new = u - step * jq + corr[c] + ratio * p
        masked = mask[c] * new
        near = shifts(masked, p_north, p_south, p_east, p_west)
        stencil = diagonal * masked - (
            faces[0] * near[0] + faces[1] * near[1] + faces[2] * near[2] + faces[3] * near[3]
        )
        applied = mask[c] * stencil + (1.0 - mask[c]) * new
        curve_part = curve_part + new * applied
        first.append(step * p)
        second.append(new)
        third.append(rhs_ref[here, :] - step * q)
        fourth.append(applied)
    out_ref[...] = jnp.concatenate(first + second + third + fourth, axis=0)
    last_ref[...] = jnp.broadcast_to(energy_new, last_ref.shape)
    send_ref[...] = jnp.broadcast_to(total(curve_part)[None], send_ref.shape)


def close_kernel(sizes, got_ref, basis_ref, rhs_ref, mask_ref, rowa_ref, rowb_ref, cola_ref,
                 colb_ref, state_ref, face_ref, edge_ref, side_ref, small_ref, gram_ref,
                 solution_ref, residual_ref, wide_ref):
    columns, comps, rows, cols, scale = sizes
    at_row, at_col = (lax.axis_index("row"), lax.axis_index("col"))
    row_count, col_count = (lax.axis_size("row"), lax.axis_size("col"))
    devices = row_count * col_count
    even_row, even_col = (1 - lax.rem(at_row, 2), 1 - lax.rem(at_col, 2))
    has_north, has_south, has_east, has_west = flags()
    me = at_row * col_count + at_col
    half, quarter = (cols // 2, cols // 4)
    lanes = iota((1, cols), 1)
    mask = [mask_ref[c * rows : (c + 1) * rows, :].astype(F32) for c in range(comps)]

    def along(left, right):
        return jnp.sum(left * right, axis=1, keepdims=True)

    sums = jnp.sum(got_ref[...], axis=0)
    image_dots = jnp.where(lanes < columns, sums[2 * comps : 2 * comps + 1, :], 0.0)
    reach_dots = jnp.where(lanes < columns, sums[2 * comps + 1 :, :], 0.0)
    curve, cross, image_sq, rhs_sq, smooth_sq, mixed, scaled_sq = [
        along(jnp.where(lanes == DOTS2 + i, 1.0, 0.0), sums[2 * comps : 2 * comps + 1, :])
        for i in range(7)
    ]
    dots, old_row, spine = (small_ref[0:1, :], small_ref[1:2, :], small_ref[2:3, :])
    energy = rhs_sq + along(dots, old_row)
    step = energy / curve
    gram = jnp.where(iota((columns, cols), 1) < columns, gram_ref[...], 0.0)
    dots = dots - step * image_dots
    coeffs = jnp.sum(gram * dots, axis=1, keepdims=True) * scale
    wide = jnp.broadcast_to(coeffs, (columns, cols))
    wide_ref[...] = wide
    coeff_row = to_row(coeffs)
    energy_new = rhs_sq - 2.0 * step * cross + step * step * image_sq + along(dots, coeff_row)
    ratio = energy_new / energy

    border = jnp.zeros((2 * comps + 2, cols), F32)
    for d in range(devices - col_count):
        border = border + got_ref[d] * pltpu.roll(got_ref[d + col_count], comps + 2, 0)
    border = jnp.where(iota(border.shape, 0) < comps, border, 0.0)
    lines = got_ref[:, 2 * comps, :]
    later = pltpu.roll(pltpu.roll(lines, devices - 1, 0), cols - (WEST2 - EAST2), 1)
    line_lane = iota(lines.shape, 1)
    beside_it = jnp.where((line_lane >= EAST2) & (line_lane < WEST2), lines * later, 0.0)
    scaled_sq = scaled_sq - 2.0 * (total(border) + total(beside_it))

    packed = pltpu.roll(got_ref[:, 2 * comps + 1, :], half, 1)
    sub = iota(packed.shape, 0)

    def turned(row):
        value = jnp.broadcast_to(row, (8, cols))
        value = jnp.broadcast_to((value + pltpu.roll(value, half, 1))[0:1, :], packed.shape)
        bit = 1
        while bit < devices:
            value = jnp.where((sub & bit) != 0, pltpu.roll(value, cols - 2 * bit, 1), value)
            bit *= 2
        ahead = pltpu.roll(value, cols - 1, 1)
        ahead = jnp.where(line_lane < quarter, ahead, pltpu.roll(value, quarter - 2, 1))
        return (jnp.where(line_lane < quarter, value[:, 0:1], value[:, 1:2]), ahead)

    other_row = coeff_row - 2.0 * old_row
    (left, left_ahead), (right, right_ahead) = (turned(coeff_row), turned(other_row))
    weight = jnp.where((line_lane == quarter - 1) | (line_lane == half - 1), 0.5, 1.0)
    form = packed * weight * (left * right_ahead + right * left_ahead)
    form = total(jnp.where(line_lane < half, form, 0.0)) + along(spine * coeff_row, other_row)
    image_part = along(coeff_row, image_dots)
    curve_new = smooth_sq - 2.0 * step * mixed + step * step * scaled_sq
    curve_new = curve_new - 2.0 * step * along(coeff_row, reach_dots) + 2.0 * image_part + form
    curve_new = curve_new + 2.0 * ratio * (cross - step * image_sq + image_part)
    curve_new = curve_new + ratio * ratio * curve
    step_new = energy_new / curve_new

    def beside(step_row, step_col):
        r, c = (at_row + step_row, at_col + step_col)
        inside = (r >= 0) & (r < row_count) & (c >= 0) & (c < col_count)
        message = got_ref[jnp.where(inside, r * col_count + c, me)]
        return message * jnp.where(inside, 1.0, 0.0)

    faces = [face_ref[i * rows : (i + 1) * rows, :] for i in range(4)]
    diagonal = face_ref[4 * rows : 5 * rows, :]
    q_north, q_south = (beside(1, 0), beside(-1, 0))
    q_east = to_column(beside(0, 1)[2 * comps : 2 * comps + 1, :], comps * rows, WEST2)
    q_west = to_column(beside(0, -1)[2 * comps : 2 * comps + 1, :], comps * rows, EAST2)

    side_a, side_b = (cola_ref[...], colb_ref[...])
    east_side = pick(even_col, side_a, side_b) * has_east
    west_side = pick(even_col, side_b, side_a) * has_west
    corr = combine(basis_ref, wide_ref, columns, comps, rows)
    for c in range(comps):
        span = slice(c * columns, (c + 1) * columns)
        here = slice(c * rows, (c + 1) * rows)
        sum_a = jnp.sum(wide * rowa_ref[span, :], axis=0, keepdims=True)
        sum_b = jnp.sum(wide * rowb_ref[span, :], axis=0, keepdims=True)
        old = [edge_ref[i * 8 + c : i * 8 + c + 1, :] for i in range(4)]
        p_north = old[0] - step * q_north[comps + c : comps + c + 1, :]
        p_south = old[1] - step * (q_south[c : c + 1, :] / faces[1][0:1, :])
        p_north = p_north + has_north * pick(even_row, sum_a, sum_b) + ratio * old[2]
        p_south = p_south + has_south * pick(even_row, sum_b, sum_a) + ratio * old[3]
        old = [side_ref[(i * comps + c) * rows : (i * comps + c + 1) * rows, :] for i in range(4)]
        p_east = old[0] - step * q_east[here] + ratio * old[2]
        p_west = old[1] - step * (q_west[here] / faces[3][:, 0:1]) + ratio * old[3]
        p_east = p_east + jnp.sum(coeff_row * east_side[here, :], axis=1, keepdims=True)
        p_west = p_west + jnp.sum(coeff_row * west_side[here, :], axis=1, keepdims=True)
        u, p, q, jq = [
            state_ref[(i * comps + c) * rows : (i * comps + c + 1) * rows, :] for i in range(4)
        ]
        new = u - step * jq + corr[c] + ratio * p
        applied = stencil(mask[c], faces, diagonal, new, (p_north, p_south, p_east, p_west))
        solution_ref[here, :] = step * p + step_new * new
        residual_ref[here, :] = rhs_ref[here, :] - step * q - step_new * applied


def last_kernel(count, got_ref, in_ref, last_ref, solution_ref, residual_ref):
    step = last_ref[0:1, :] / jnp.sum(got_ref[...], axis=0)
    solution_ref[...] = in_ref[:count, :] + step * in_ref[count : 2 * count, :]
    residual_ref[...] = in_ref[2 * count : 3 * count, :] - step * in_ref[3 * count :, :]


def on_device(right_side, viscosity, free_mask, coarse_basis, gram_inverse):
    comps, rows, cols = right_side.shape
    columns = coarse_basis.shape[0]
    row_count, col_count = (lax.axis_size("row"), lax.axis_size("col"))
    devices = row_count * col_count
    scale = 1.0 / (32.0 * math.sqrt(float(comps * rows * cols * devices * columns)))
    sizes = (columns, comps, rows, cols)

    def call(kernel, outs, scratch, *args, flops=None):
        cost = flops and pl.CostEstimate(flops=flops, bytes_accessed=4096, transcendentals=0)
        return pl.pallas_call(
            kernel,
            out_shape=[jax.ShapeDtypeStruct(s, F32) for s in outs],
            in_specs=[VMEM] * len(args),
            out_specs=[VMEM] * len(outs),
            scratch_shapes=[pltpu.VMEM(s, F32) for s in scratch],
            cost_estimate=cost,
            compiler_params=pltpu.CompilerParams(vmem_limit_bytes=16 * 1024 * 1024),
        )(*args)

    def share(message):
        return lax.all_to_all(message, ("row", "col"), 0, 0, tiled=True)

    def swap(packet, axis, first):
        count = lax.axis_size(axis)
        pairs = [(i, i + 1) for i in range(first, count - 1, 2)]
        KIND = {"row": "cyc", "col": "cyc"}[axis]
        extra = []
        if first == 1 and count > 2 and count % 2 == 0:
            if KIND == "cyc":
                pairs.append((0, count - 1))
            if KIND == "self":
                extra = [(0, 0), (count - 1, count - 1)]
        return lax.ppermute(packet, axis, pairs + [(j, i) for i, j in pairs] + extra)

    basis = coarse_basis.reshape(columns * comps * rows, cols)
    rhs = right_side.reshape(comps * rows, cols)
    mask = free_mask.reshape(comps * rows, cols)

    block = gram_inverse.size
    piece = -(-block // row_count)
    two = columns * columns == devices * cols and cols == 2 * columns and rows == 8 and comps == 3
    if two:
        (own,) = call(piece_kernel, [(1, cols)], [], gram_inverse, flops=10**9)
    else:
        flat = jnp.pad(gram_inverse.reshape(-1), (0, piece * row_count - block))
        own = lax.dynamic_slice_in_dim(flat, lax.axis_index("row") * piece, piece)
        own = jnp.pad(own, (0, cols - piece)).reshape(1, cols)

    tall = -(-(comps * columns + comps + 2) // 8) * 8
    wide = (comps + 1) * rows
    field = comps * rows
    if two:
        row_a, row_b, col_a, col_b = call(
            functools.partial(packets_kernel, sizes),
            [(tall, cols), (tall, cols), (wide, cols), (wide, cols)],
            [],
            basis, rhs, mask, viscosity, own,
        )
        packets = ((row_a, "row", 0), (row_b, "row", 1), (col_a, "col", 0), (col_b, "col", 1))
        halos = []
        for packet in packets:
            halos.append(swap(*packet))
        (send,) = call(
            functools.partial(gram_kernel, sizes),
            [(devices, 4, cols)],
            [(columns * rows, cols), (columns, cols)],
            basis, rhs, mask, viscosity, own, *halos, col_a, col_b,
        )
        sizes = sizes + (scale,)
        send, *state = call(
            functools.partial(first_kernel, sizes, True, True),
            [(devices, 8, cols), (4 * field, cols), (5 * rows, cols), (32, cols),
             (4 * field, cols), (8, cols), (columns, cols)],
            [(columns * rows, cols), (columns, cols)],
            share(send), basis, rhs, mask, viscosity, *halos,
        )
        solution, residual = call(
            functools.partial(close_kernel, sizes),
            [(field, cols), (field, cols)],
            [(columns, cols)],
            share(send), basis, rhs, mask, *halos, *state,
        )
        return (solution.reshape(right_side.shape), residual.reshape(right_side.shape))
    send, row_a, row_b, col_a, col_b = call(
        functools.partial(pack_kernel, sizes),
        [(devices, 2, cols), (tall, cols), (tall, cols), (wide, cols), (wide, cols)],
        [(columns * rows, cols)],
        basis, rhs, mask, viscosity, own,
    )
    halos = (swap(row_a, "row", 0), swap(row_b, "row", 1), swap(col_a, "col", 0), swap(col_b, "col", 1))
    got = share(send)
    whole_rows = piece == cols and cols % columns == 0 and block == piece * row_count
    gram = ()
    if not whole_rows:
        gram = got[:, 1, :piece].reshape(row_count, col_count, piece).transpose(1, 0, 2)
        gram = gram.reshape(col_count, row_count * piece)[:, :block].reshape(columns, columns)
        gram = (gram,)
    sizes = sizes + (scale,)
    send, *state = call(
        functools.partial(first_kernel, sizes, whole_rows, False),
        [(devices, 1 + comps, cols), (4 * field, cols), (5 * rows, cols), (32, cols),
         (4 * field, cols), (8, cols), (columns, cols)],
        [(columns * rows, cols), (columns, cols)],
        got, *gram, basis, rhs, mask, viscosity, *halos,
    )
    send, fields, last = call(
        functools.partial(second_kernel, sizes),
        [(devices, 1, cols), (4 * field, cols), (8, cols)],
        [(columns, cols)],
        share(send), basis, rhs, mask, *halos, *state,
    )
    solution, residual = call(
        functools.partial(last_kernel, field),
        [(field, cols), (field, cols)],
        [],
        share(send), fields, last,
    )
    return (solution.reshape(right_side.shape), residual.reshape(right_side.shape))


def solution(mesh):
    in_specs = (
        P(None, "row", "col"),
        P("row", "col"),
        P(None, "row", "col"),
        P(None, None, "row", "col"),
        P("col", None),
    )
    out_specs = (P(None, "row", "col"), P(None, "row", "col"))
    return jax.shard_map(
        on_device, mesh=mesh, in_specs=in_specs, out_specs=out_specs, check_vma=False
    )
```

```python
import functools
import math

import jax
import jax.numpy as jnp
from jax import lax
from jax.experimental import pallas as pl
from jax.experimental.pallas import tpu as pltpu
from jax.sharding import PartitionSpec as P


F32 = jnp.float32
VMEM = pl.BlockSpec(memory_space=pltpu.VMEM)
DOTS, EAST, WEST = 64, 72, 96
EAST2, WEST2, DOTS2 = 64, 88, 112


def flags():
    at_row, at_col = (lax.axis_index("row"), lax.axis_index("col"))
    tests = (
        at_row < lax.axis_size("row") - 1,
        at_row > 0,
        at_col < lax.axis_size("col") - 1,
        at_col > 0,
    )
    return [jnp.where(test, 1.0, 0.0) for test in tests]


def iota(shape, dim):
    return lax.broadcasted_iota(jnp.int32, shape, dim)


def pick(flag, yes, no):
    return jnp.where(jnp.full(yes.shape, flag, jnp.int32) == 1, yes, no)


def to_row(column, first=0):
    shape = (column.shape[0], 128)
    spread = jnp.where(iota(shape, 1) == iota(shape, 0) + first, column, 0.0)
    return jnp.sum(spread, axis=0, keepdims=True)


def to_column(row, count, first=0):
    shape = (count, 128)
    spread = jnp.where(iota(shape, 1) == iota(shape, 0) + first, row, 0.0)
    return jnp.sum(spread, axis=1, keepdims=True)


def total(values):
    return jnp.sum(jnp.sum(values, axis=0, keepdims=True), axis=1, keepdims=True)


def shifts(tile, north, south, east, west):
    rows, cols = tile.shape
    sub, lane = (iota(tile.shape, 0), iota(tile.shape, 1))
    return (
        jnp.where(sub == rows - 1, north, pltpu.roll(tile, rows - 1, 0)),
        jnp.where(sub == 0, south, pltpu.roll(tile, 1, 0)),
        jnp.where(lane == cols - 1, east, pltpu.roll(tile, cols - 1, 1)),
        jnp.where(lane == 0, west, pltpu.roll(tile, 1, 1)),
    )


def project(basis_ref, field, acc_ref, columns, comps, rows):
    for k in range(columns):
        base = k * comps * rows
        acc = basis_ref[base : base + rows, :] * field[0]
        for c in range(1, comps):
            acc = acc + basis_ref[base + c * rows : base + (c + 1) * rows, :] * field[c]
        acc_ref[k * rows : (k + 1) * rows, :] = acc
    sums = acc_ref[pl.ds(0, columns, stride=rows), :]
    for s in range(1, rows):
        sums = sums + acc_ref[pl.ds(s, columns, stride=rows), :]
    return jnp.sum(sums, axis=1, keepdims=True)


def combine(basis_ref, wide_ref, columns, comps, rows):
    out = [[None, None] for _ in range(comps)]
    for k in range(columns):
        weight = jnp.broadcast_to(wide_ref[k : k + 1, :], (rows, 128))
        for c in range(comps):
            base = (k * comps + c) * rows
            term = weight * basis_ref[base : base + rows, :]
            old = out[c][k % 2]
            out[c][k % 2] = term if old is None else old + term
    return [a + b for a, b in out]


def pack_kernel(sizes, basis_ref, rhs_ref, mask_ref, visc_ref, gram_ref,
                send_ref, rowa_ref, rowb_ref, cola_ref, colb_ref, acc_ref):
    columns, comps, rows, cols = sizes
    packet_kernel(sizes, basis_ref, rhs_ref, mask_ref, visc_ref, rowa_ref, rowb_ref, cola_ref, colb_ref)
    rhs = [rhs_ref[c * rows : (c + 1) * rows, :] for c in range(comps)]
    visc = visc_ref[...]

    row = to_row(project(basis_ref, rhs, acc_ref, columns, comps, rows))
    lanes = iota((1, cols), 1)
    for i, corner in enumerate(corners_of(visc)):
        row = jnp.where(lanes == columns + i, corner, row)
    both = jnp.concatenate([row, gram_ref[...]], axis=0)
    send_ref[...] = jnp.broadcast_to(both[None], send_ref.shape)


def piece_kernel(gram_ref, piece_ref):
    at = 2 * lax.axis_index("row")
    rows = [gram_ref[pl.ds(at + t, 1), :] for t in range(2)]
    piece_ref[...] = jnp.concatenate(rows, axis=1)


def packets_kernel(sizes, basis_ref, rhs_ref, mask_ref, visc_ref, first_ref, *packet_refs):
    packet_kernel(sizes, basis_ref, rhs_ref, mask_ref, visc_ref, *packet_refs)


def corners_of(visc):
    top, low = (visc.shape[0] - 1, visc.shape[1] - 1)
    return [visc[i : i + 1, j : j + 1] for i in (0, top) for j in (0, low)]


def packet_kernel(sizes, basis_ref, rhs_ref, mask_ref, visc_ref,
                  rowa_ref, rowb_ref, cola_ref, colb_ref):
    columns, comps, rows, cols = sizes
    even_row = 1 - lax.rem(lax.axis_index("row"), 2)
    even_col = 1 - lax.rem(lax.axis_index("col"), 2)
    rhs = [rhs_ref[c * rows : (c + 1) * rows, :] for c in range(comps)]
    mask = [mask_ref[c * rows : (c + 1) * rows, :].astype(F32) for c in range(comps)]
    visc = visc_ref[...]
    lane = iota((rows, cols), 1)
    top, low = rows - 1, cols - 1

    for c in range(comps):
        north = basis_ref[pl.ds(c * rows + top, columns, stride=comps * rows), :]
        south = basis_ref[pl.ds(c * rows, columns, stride=comps * rows), :]
        north = north * mask[c][top : top + 1, :]
        south = south * mask[c][0:1, :]
        rowa_ref[c * columns : (c + 1) * columns, :] = pick(even_row, north, south)
        rowb_ref[c * columns : (c + 1) * columns, :] = pick(even_row, south, north)
    north = [mask[c][top : top + 1, :] * rhs[c][top : top + 1, :] for c in range(comps)]
    south = [mask[c][0:1, :] * rhs[c][0:1, :] for c in range(comps)]
    north += [visc[top : top + 1, :], visc[top - 1 : top, :]]
    south += [visc[0:1, :], visc[1:2, :]]
    for i in range(comps + 2):
        at = comps * columns + i
        rowa_ref[at : at + 1, :] = pick(even_row, north[i], south[i])
        rowb_ref[at : at + 1, :] = pick(even_row, south[i], north[i])
    rest = comps * columns + comps + 2
    blank = jnp.zeros((rowa_ref.shape[0] - rest, cols), F32)
    rowa_ref[rest:, :] = blank
    rowb_ref[rest:, :] = blank

    for c in range(comps):
        east, west = (jnp.zeros((rows, cols), F32), jnp.zeros((rows, cols), F32))
        for k in range(columns):
            base = (k * comps + c) * rows
            tile = basis_ref[base : base + rows, :]
            east = jnp.where(lane == k, pltpu.roll(tile, (k - low) % cols, 1), east)
            west = jnp.where(lane == k, tile if k == 0 else pltpu.roll(tile, k, 1), west)
        east = jnp.where(lane == columns, rhs[c][:, low : low + 1], east)
        west = jnp.where(lane == columns, rhs[c][:, 0:1], west)
        east = east * mask[c][:, low : low + 1]
        west = west * mask[c][:, 0:1]
        cola_ref[c * rows : (c + 1) * rows, :] = pick(even_col, east, west)
        colb_ref[c * rows : (c + 1) * rows, :] = pick(even_col, west, east)
    east = jnp.where(lane == 0, visc[:, low : low + 1], visc[:, low - 1 : low])
    west = jnp.where(lane == 0, visc[:, 0:1], visc[:, 1:2])
    cola_ref[comps * rows :, :] = pick(even_col, east, west)
    colb_ref[comps * rows :, :] = pick(even_col, west, east)


def stencil(mask, faces, diagonal, tile, halo):
    masked = mask * tile
    near = shifts(masked, *halo)
    inner = diagonal * masked - (
        faces[0] * near[0] + faces[1] * near[1] + faces[2] * near[2] + faces[3] * near[3]
    )
    return mask * inner + (1.0 - mask) * tile


def split(values):
    high = values.astype(jnp.bfloat16)
    return jnp.concatenate([high, (values - high.astype(F32)).astype(jnp.bfloat16)], axis=0)


def gram_kernel(sizes, basis_ref, rhs_ref, mask_ref, visc_ref, gram_ref, rowa_ref, rowb_ref,
                cola_ref, colb_ref, owna_ref, ownb_ref, send_ref, acc_ref, full_ref):
    columns, comps, rows, cols = sizes
    at_row, at_col = (lax.axis_index("row"), lax.axis_index("col"))
    even_row, even_col = (1 - lax.rem(at_row, 2), 1 - lax.rem(at_col, 2))
    has_north, has_south, has_east, has_west = flags()
    low, half = (cols - 1, cols // 2)
    rhs = [rhs_ref[c * rows : (c + 1) * rows, :] for c in range(comps)]
    mask = [mask_ref[c * rows : (c + 1) * rows, :].astype(F32) for c in range(comps)]
    visc = visc_ref[...]
    lane, lanes = (iota((rows, cols), 1), iota((1, cols), 1))

    at = comps * columns + comps
    tail_a, tail_b = (rowa_ref[at : at + 1, :], rowb_ref[at : at + 1, :])
    v_north = pick(even_row, tail_a, tail_b) * has_north
    v_south = pick(even_row, tail_b, tail_a) * has_south
    side_a, side_b = (cola_ref[...], colb_ref[...])
    east_side = pick(even_col, side_a, side_b) * has_east
    west_side = pick(even_col, side_b, side_a) * has_west
    own_a, own_b = (owna_ref[...], ownb_ref[...])
    own_east, own_west = (pick(even_col, own_a, own_b), pick(even_col, own_b, own_a))
    v_east, v_west = (east_side[comps * rows :, 0:1], west_side[comps * rows :, 0:1])
    faces = [0.5 * (visc + v) for v in shifts(visc, v_north, v_south, v_east, v_west)]
    diagonal = 1.0 + faces[0] + faces[1] + faces[2] + faces[3]

    blocks = jnp.zeros((2 * columns, 2 * columns), F32)
    for c in range(comps):
        m = mask[c]
        own = m * diagonal + (1.0 - m)
        up, down = (m * faces[0], m * faces[1])
        right = jnp.where(lane == low, 0.0, m * faces[2])
        left = jnp.where(lane == 0, 0.0, m * faces[3])
        span = slice(c * columns, (c + 1) * columns)
        halo_a, halo_b = (rowa_ref[span, :], rowb_ref[span, :])
        plain = [
            basis_ref[pl.ds(c * rows + i, columns, stride=comps * rows), :] for i in range(rows)
        ]
        free = [plain[i] * m[i : i + 1, :] for i in range(rows)]
        free.append(pick(even_row, halo_a, halo_b) * has_north)
        free.append(pick(even_row, halo_b, halo_a) * has_south)
        for i in range(0, rows, 2):
            lefts, rights = ([], [])
            for j in (i, i + 1):
                here = slice(j, j + 1)
                value = own[here] * plain[j] - up[here] * free[j + 1] - down[here] * free[j - 1]
                value = value - right[here] * pltpu.roll(free[j], low, 1)
                value = value - left[here] * pltpu.roll(free[j], 1, 1)
                lefts.append(split(plain[j]))
                rights.append(split(value))
            blocks = blocks + lax.dot_general(
                jnp.concatenate(lefts, axis=1),
                jnp.concatenate(rights, axis=1),
                (((1,), (1,)), ((), ())),
                preferred_element_type=F32,
            )
    east_face = jnp.concatenate([faces[2][:, low : low + 1]] * comps, axis=0)
    west_face = jnp.concatenate([faces[3][:, 0:1]] * comps, axis=0)
    field = comps * rows
    ours = jnp.concatenate([own_east[:field] * east_face, own_west[:field] * west_face], axis=0)
    theirs = jnp.concatenate([east_side[:field], west_side[:field]], axis=0)
    edge = lax.dot_general(
        ours, theirs, (((0,), (0,)), ((), ())),
        preferred_element_type=F32, precision=lax.Precision.HIGHEST,
    )
    blocks = blocks + pltpu.roll(blocks, half, 1)
    wide_lane = iota((columns, cols), 1)
    edge = jnp.where(wide_lane < half, edge[:columns], 0.0)
    full = blocks[:columns] + blocks[columns:] - edge - pltpu.roll(edge, half, 1)
    full_ref[...] = full
    spot = jnp.where(wide_lane >= half, wide_lane - half, wide_lane) == iota((columns, cols), 0)
    spine = jnp.sum(jnp.where(spot, full, 0.0), axis=0, keepdims=True)
    count = columns // 2
    chunk = jnp.where(
        iota((count, cols), 1) < half,
        full_ref[pl.ds(0, count, stride=2), :],
        full_ref[pl.ds(1, count, stride=2), :],
    )
    dots = to_row(project(basis_ref, rhs, acc_ref, columns, comps, rows))
    corner_row = jnp.zeros((1, cols), F32)
    for i, corner in enumerate(corners_of(visc)):
        corner_row = jnp.where(lanes == i, corner, corner_row)
    head = jnp.concatenate([jnp.where(lanes < half, dots, spine), gram_ref[...]], axis=0)
    for d in range(count):
        send_ref[d] = jnp.concatenate([head, chunk[d : d + 1, :], corner_row], axis=0)


def first_kernel(sizes, whole_rows, two, got_ref, *refs):
    columns, comps, rows, cols, scale = sizes
    if whole_rows:
        gram_in_ref = None
    else:
        gram_in_ref, *refs = refs
    (basis_ref, rhs_ref, mask_ref, visc_ref, rowa_ref, rowb_ref, cola_ref, colb_ref,
     send_ref, state_ref, face_ref, edge_ref, side_ref, small_ref, gram_ref,
     acc_ref, wide_ref) = refs
    at_row, at_col = (lax.axis_index("row"), lax.axis_index("col"))
    row_count, col_count = (lax.axis_size("row"), lax.axis_size("col"))
    even_row, even_col = (1 - lax.rem(at_row, 2), 1 - lax.rem(at_col, 2))
    me = at_row * col_count + at_col
    top, low = rows - 1, cols - 1
    rhs = [rhs_ref[c * rows : (c + 1) * rows, :] for c in range(comps)]
    mask = [mask_ref[c * rows : (c + 1) * rows, :].astype(F32) for c in range(comps)]
    visc = visc_ref[...]
    sub, lane = (iota((rows, cols), 0), iota((rows, cols), 1))
    lanes = iota((1, cols), 1)

    if whole_rows:
        per = cols // columns
        for r in range(row_count):
            for c in range(col_count):
                piece = got_ref[r * col_count + c, 1:2, :]
                for t in range(per):
                    at = (c * row_count + r) * per + t
                    moved = pltpu.roll(piece, cols - t * columns, 1) if t else piece
                    gram_ref[at : at + 1, :] = moved
    else:
        gram_ref[:, :columns] = gram_in_ref[...]
    all_sums = jnp.sum(got_ref[...], axis=0)
    sums = all_sums[0:1, :]
    dots = jnp.where(lanes < columns, sums, 0.0)
    gram = jnp.where(iota((columns, cols), 1) < columns, gram_ref[...], 0.0)
    coeffs = jnp.sum(gram * dots, axis=1, keepdims=True) * scale
    wide = jnp.broadcast_to(coeffs, (columns, cols))
    wide_ref[...] = wide
    coeff_row = to_row(coeffs)

    extra = comps * columns
    tail_a, tail_b = (rowa_ref[extra:, :], rowb_ref[extra:, :])
    has_north, has_south, has_east, has_west = flags()
    north_tail = pick(even_row, tail_a, tail_b) * has_north
    south_tail = pick(even_row, tail_b, tail_a) * has_south
    side_a, side_b = (cola_ref[...], colb_ref[...])
    east_side = pick(even_col, side_a, side_b) * has_east
    west_side = pick(even_col, side_b, side_a) * has_west
    v_north, v_south = (north_tail[comps : comps + 1, :], south_tail[comps : comps + 1, :])
    v_north2, v_south2 = (north_tail[comps + 1 : comps + 2, :], south_tail[comps + 1 : comps + 2, :])
    v_east, v_west = (east_side[comps * rows :, 0:1], west_side[comps * rows :, 0:1])
    v_east2, v_west2 = (east_side[comps * rows :, 1:2], west_side[comps * rows :, 1:2])
    faces = [0.5 * (visc + v) for v in shifts(visc, v_north, v_south, v_east, v_west)]
    diagonal = 1.0 + faces[0] + faces[1] + faces[2] + faces[3]
    face_ref[...] = jnp.concatenate(faces + [diagonal], axis=0)
    jacobi = [m / diagonal + (1.0 - m) for m in mask]

    def corner(step_row, step_col, which):
        r, c = (at_row + step_row, at_col + step_col)
        inside = (r >= 0) & (r < row_count) & (c >= 0) & (c < col_count)
        place = jnp.where(inside, r * col_count + c, me)
        line, first = (3, 0) if two else (0, columns)
        value = got_ref[place, line : line + 1, :]
        value = jnp.sum(jnp.where(lanes == first + which, value, 0.0), axis=1, keepdims=True)
        return value * jnp.where(inside, 1.0, 0.0)

    north_west, north_east = (corner(1, -1, 1), corner(1, 1, 0))
    south_west, south_east = (corner(-1, -1, 3), corner(-1, 1, 2))

    def row_inverse(own, inner, outer, west, east):
        right = jnp.where(lanes == low, east, pltpu.roll(own, low, 1))
        left = jnp.where(lanes == 0, west, pltpu.roll(own, 1, 1))
        return 1.0 / (1.0 + 0.5 * (4.0 * own + inner + outer + left + right))

    def side_inverse(own, inner, outer, south, north):
        own = jnp.broadcast_to(own, (rows, cols))
        up = jnp.where(sub == top, north, pltpu.roll(own, top, 0))
        down = jnp.where(sub == 0, south, pltpu.roll(own, 1, 0))
        return 1.0 / (1.0 + 0.5 * (4.0 * own + inner + outer + up + down))

    inv_north = row_inverse(v_north, visc[top : top + 1, :], v_north2, north_west, north_east)
    inv_south = row_inverse(v_south, visc[0:1, :], v_south2, south_west, south_east)
    inv_east = side_inverse(v_east, visc[:, low : low + 1], v_east2, south_east, north_east)
    inv_west = side_inverse(v_west, visc[:, 0:1], v_west2, south_west, north_west)

    corr = combine(basis_ref, wide_ref, columns, comps, rows)
    image, scaled, smooth, point = ([], [], [], [])
    smooth_image, scaled_image = ([], [])
    none = (jnp.zeros((1, cols), F32),) * 2 + (jnp.zeros((rows, 1), F32),) * 2
    for c in range(comps):
        span = slice(c * columns, (c + 1) * columns)
        sum_a = jnp.sum(wide * rowa_ref[span, :], axis=0, keepdims=True)
        sum_b = jnp.sum(wide * rowb_ref[span, :], axis=0, keepdims=True)
        u_north = inv_north * north_tail[c : c + 1, :]
        u_south = inv_south * south_tail[c : c + 1, :]
        p_north = u_north + has_north * pick(even_row, sum_a, sum_b)
        p_south = u_south + has_south * pick(even_row, sum_b, sum_a)
        here = slice(c * rows, (c + 1) * rows)
        east, west = (east_side[here, :], west_side[here, :])
        u_east = inv_east * east[:, columns : columns + 1]
        u_west = inv_west * west[:, columns : columns + 1]
        p_east = u_east + jnp.sum(coeff_row * east, axis=1, keepdims=True)
        p_west = u_west + jnp.sum(coeff_row * west, axis=1, keepdims=True)
        u = jacobi[c] * rhs[c]
        p = u + corr[c]
        q = stencil(mask[c], faces, diagonal, p, (p_north, p_south, p_east, p_west))
        if two:
            halo = (u_north, u_south, u_east, u_west)
            smooth_image.append(stencil(mask[c], faces, diagonal, u, halo))
            scaled_image.append(stencil(mask[c], faces, diagonal, jacobi[c] * q, none))
        smooth.append(u)
        point.append(p)
        image.append(q)
        scaled.append(jacobi[c] * q)
        for i, value in enumerate((u_north, u_south, p_north, p_south)):
            edge_ref[i * 8 + c : i * 8 + c + 1, :] = value
        for i, value in enumerate((u_east, u_west, p_east, p_west)):
            side_ref[(i * comps + c) * rows : (i * comps + c + 1) * rows, :] = value
    state_ref[...] = jnp.concatenate(smooth + point + image + scaled, axis=0)

    row = to_row(project(basis_ref, image, acc_ref, columns, comps, rows))
    pairs = ((point, image), (smooth, image), (image, scaled), (rhs, smooth))
    if two:
        pairs += ((smooth, smooth_image), (scaled, smooth_image), (scaled, scaled_image))
    for i, (left, right) in enumerate(pairs):
        value = left[0] * right[0]
        for c in range(1, comps):
            value = value + left[c] * right[c]
        row = jnp.where(lanes == (DOTS2 if two else DOTS) + i, total(value), row)
    masked = [mask[c] * scaled[c] for c in range(comps)]
    if two:
        norths = [m[top : top + 1, :] * faces[0][top : top + 1, :] * has_north for m in masked]
        easts = [m[:, low : low + 1] * faces[2][:, low : low + 1] * has_east for m in masked]
        souths, wests = ([m[0:1, :] for m in masked], [m[:, 0:1] for m in masked])
        row = row + to_row(jnp.concatenate(easts, axis=0), EAST2)
        row = row + to_row(jnp.concatenate(wests, axis=0), WEST2)
        reach = project(basis_ref, scaled_image, acc_ref, columns, comps, rows)
        beyond = jnp.zeros((columns, cols), F32)
        aside = jnp.zeros((rows, cols), F32)
        for c in range(comps):
            span, here = (slice(c * columns, (c + 1) * columns), slice(c * rows, (c + 1) * rows))
            halo_a, halo_b = (rowa_ref[span, :], rowb_ref[span, :])
            low_side = souths[c] * faces[1][0:1, :] * has_south
            beyond = beyond + norths[c] * pick(even_row, halo_a, halo_b)
            beyond = beyond + low_side * pick(even_row, halo_b, halo_a)
            aside = aside + easts[c] * east_side[here, :]
            aside = aside + wests[c] * faces[3][:, 0:1] * west_side[here, :]
        reach = to_row(reach - jnp.sum(beyond, axis=1, keepdims=True))
        reach = reach - jnp.where(lanes < columns, jnp.sum(aside, axis=0, keepdims=True), 0.0)
        half = cols // 2
        ours = jnp.broadcast_to(all_sums[2:3, :], (8, cols))
        other = pltpu.roll(ours, half, 1)
        wide_lane = iota((8, cols), 1)
        for t, (first, second) in enumerate(((ours, other), (other, ours))):
            value = jnp.where(wide_lane < half, first, second)
            turn = lax.rem(half + t * (half // 2) - (2 * me + t + 1) + 2 * cols, cols)
            value = pltpu.roll(value, turn, 1)[0:1, :]
            start = half + t * (half // 2)
            reach = jnp.where((lanes >= start) & (lanes < start + half // 2), value, reach)
        message = jnp.concatenate(norths + souths + [row, reach], axis=0)
        send_ref[...] = jnp.broadcast_to(message[None], send_ref.shape)
        spine = pltpu.roll(jnp.broadcast_to(sums, (8, cols)), half, 1)[0:1, :]
        spine = jnp.where(lanes < half, spine, 0.0)
        small_ref[...] = jnp.concatenate([dots, coeff_row, spine, jnp.zeros((5, cols), F32)], axis=0)
        return
    east = jnp.concatenate([m[:, low : low + 1] for m in masked], axis=0)
    west = jnp.concatenate([m[:, 0:1] for m in masked], axis=0)
    row = row + to_row(east, EAST) + to_row(west, WEST)
    message = jnp.concatenate([row] + [m[top : top + 1, :] for m in masked], axis=0)
    send_ref[...] = jnp.broadcast_to(message[None], send_ref.shape)
    message = jnp.concatenate([row] + [m[0:1, :] for m in masked], axis=0)
    send_ref[jnp.where(at_row > 0, me - col_count, me)] = message
    small_ref[...] = jnp.concatenate([dots, coeff_row, jnp.zeros((6, cols), F32)], axis=0)


def second_kernel(sizes, got_ref, basis_ref, rhs_ref, mask_ref, rowa_ref, rowb_ref, cola_ref,
                  colb_ref, state_ref, face_ref, edge_ref, side_ref, small_ref, gram_ref,
                  send_ref, out_ref, last_ref, wide_ref):
    columns, comps, rows, cols, scale = sizes
    at_row, at_col = (lax.axis_index("row"), lax.axis_index("col"))
    row_count, col_count = (lax.axis_size("row"), lax.axis_size("col"))
    even_row, even_col = (1 - lax.rem(at_row, 2), 1 - lax.rem(at_col, 2))
    me = at_row * col_count + at_col
    lanes = iota((1, cols), 1)
    mask = [mask_ref[c * rows : (c + 1) * rows, :].astype(F32) for c in range(comps)]

    sums = jnp.sum(got_ref[...], axis=0)[0:1, :]
    image_dots = jnp.where(lanes < columns, sums, 0.0)
    curve, cross, image_sq, rhs_sq = [
        jnp.sum(jnp.where(lanes == DOTS + i, sums, 0.0), axis=1, keepdims=True) for i in range(4)
    ]
    dots, coeff_row = (small_ref[0:1, :], small_ref[1:2, :])
    energy = rhs_sq + jnp.sum(dots * coeff_row, axis=1, keepdims=True)
    step = energy / curve
    gram = jnp.where(iota((columns, cols), 1) < columns, gram_ref[...], 0.0)
    dots = dots - step * image_dots
    coeffs = jnp.sum(gram * dots, axis=1, keepdims=True) * scale
    wide = jnp.broadcast_to(coeffs, (columns, cols))
    wide_ref[...] = wide
    coeff_row = to_row(coeffs)
    energy_new = rhs_sq - 2.0 * step * cross + step * step * image_sq
    energy_new = energy_new + jnp.sum(dots * coeff_row, axis=1, keepdims=True)
    ratio = energy_new / energy

    def beside(step_row, step_col):
        r, c = (at_row + step_row, at_col + step_col)
        inside = (r >= 0) & (r < row_count) & (c >= 0) & (c < col_count)
        message = got_ref[jnp.where(inside, r * col_count + c, me)]
        return message * jnp.where(inside, 1.0, 0.0)

    q_north, q_south = (beside(1, 0), beside(-1, 0))
    q_east = to_column(beside(0, 1)[0:1, :], comps * rows, WEST)
    q_west = to_column(beside(0, -1)[0:1, :], comps * rows, EAST)

    side_a, side_b = (cola_ref[...], colb_ref[...])
    has_north, has_south, has_east, has_west = flags()
    east_side = pick(even_col, side_a, side_b) * has_east
    west_side = pick(even_col, side_b, side_a) * has_west
    faces = [face_ref[i * rows : (i + 1) * rows, :] for i in range(4)]
    diagonal = face_ref[4 * rows : 5 * rows, :]
    corr = combine(basis_ref, wide_ref, columns, comps, rows)
    curve_part = jnp.zeros((rows, cols), F32)
    first, second, third, fourth = ([], [], [], [])
    for c in range(comps):
        span = slice(c * columns, (c + 1) * columns)
        here = slice(c * rows, (c + 1) * rows)
        sum_a = jnp.sum(wide * rowa_ref[span, :], axis=0, keepdims=True)
        sum_b = jnp.sum(wide * rowb_ref[span, :], axis=0, keepdims=True)
        old = [edge_ref[i * 8 + c : i * 8 + c + 1, :] for i in range(4)]
        p_north = old[0] - step * q_north[1 + c : 2 + c, :] + has_north * pick(even_row, sum_a, sum_b)
        p_south = old[1] - step * q_south[1 + c : 2 + c, :] + has_south * pick(even_row, sum_b, sum_a)
        p_north, p_south = (p_north + ratio * old[2], p_south + ratio * old[3])
        old = [side_ref[(i * comps + c) * rows : (i * comps + c + 1) * rows, :] for i in range(4)]
        p_east = old[0] - step * q_east[here] + ratio * old[2]
        p_west = old[1] - step * q_west[here] + ratio * old[3]
        p_east = p_east + jnp.sum(coeff_row * east_side[here, :], axis=1, keepdims=True)
        p_west = p_west + jnp.sum(coeff_row * west_side[here, :], axis=1, keepdims=True)
        u, p, q, jq = [
            state_ref[(i * comps + c) * rows : (i * comps + c + 1) * rows, :] for i in range(4)
        ]
        new = u - step * jq + corr[c] + ratio * p
        masked = mask[c] * new
        near = shifts(masked, p_north, p_south, p_east, p_west)
        stencil = diagonal * masked - (
            faces[0] * near[0] + faces[1] * near[1] + faces[2] * near[2] + faces[3] * near[3]
        )
        applied = mask[c] * stencil + (1.0 - mask[c]) * new
        curve_part = curve_part + new * applied
        first.append(step * p)
        second.append(new)
        third.append(rhs_ref[here, :] - step * q)
        fourth.append(applied)
    out_ref[...] = jnp.concatenate(first + second + third + fourth, axis=0)
    last_ref[...] = jnp.broadcast_to(energy_new, last_ref.shape)
    send_ref[...] = jnp.broadcast_to(total(curve_part)[None], send_ref.shape)


def close_kernel(sizes, got_ref, basis_ref, rhs_ref, mask_ref, rowa_ref, rowb_ref, cola_ref,
                 colb_ref, state_ref, face_ref, edge_ref, side_ref, small_ref, gram_ref,
                 solution_ref, residual_ref, wide_ref):
    columns, comps, rows, cols, scale = sizes
    at_row, at_col = (lax.axis_index("row"), lax.axis_index("col"))
    row_count, col_count = (lax.axis_size("row"), lax.axis_size("col"))
    devices = row_count * col_count
    even_row, even_col = (1 - lax.rem(at_row, 2), 1 - lax.rem(at_col, 2))
    has_north, has_south, has_east, has_west = flags()
    me = at_row * col_count + at_col
    half, quarter = (cols // 2, cols // 4)
    lanes = iota((1, cols), 1)
    mask = [mask_ref[c * rows : (c + 1) * rows, :].astype(F32) for c in range(comps)]

    def along(left, right):
        return jnp.sum(left * right, axis=1, keepdims=True)

    sums = jnp.sum(got_ref[...], axis=0)
    image_dots = jnp.where(lanes < columns, sums[2 * comps : 2 * comps + 1, :], 0.0)
    reach_dots = jnp.where(lanes < columns, sums[2 * comps + 1 :, :], 0.0)
    curve, cross, image_sq, rhs_sq, smooth_sq, mixed, scaled_sq = [
        along(jnp.where(lanes == DOTS2 + i, 1.0, 0.0), sums[2 * comps : 2 * comps + 1, :])
        for i in range(7)
    ]
    dots, old_row, spine = (small_ref[0:1, :], small_ref[1:2, :], small_ref[2:3, :])
    energy = rhs_sq + along(dots, old_row)
    step = energy / curve
    gram = jnp.where(iota((columns, cols), 1) < columns, gram_ref[...], 0.0)
    dots = dots - step * image_dots
    coeffs = jnp.sum(gram * dots, axis=1, keepdims=True) * scale
    wide = jnp.broadcast_to(coeffs, (columns, cols))
    wide_ref[...] = wide
    coeff_row = to_row(coeffs)
    energy_new = rhs_sq - 2.0 * step * cross + step * step * image_sq + along(dots, coeff_row)
    ratio = energy_new / energy

    border = jnp.zeros((2 * comps + 2, cols), F32)
    for d in range(devices - col_count):
        border = border + got_ref[d] * pltpu.roll(got_ref[d + col_count], comps + 2, 0)
    border = jnp.where(iota(border.shape, 0) < comps, border, 0.0)
    lines = got_ref[:, 2 * comps, :]
    later = pltpu.roll(pltpu.roll(lines, devices - 1, 0), cols - (WEST2 - EAST2), 1)
    line_lane = iota(lines.shape, 1)
    beside_it = jnp.where((line_lane >= EAST2) & (line_lane < WEST2), lines * later, 0.0)
    scaled_sq = scaled_sq - 2.0 * (total(border) + total(beside_it))

    packed = pltpu.roll(got_ref[:, 2 * comps + 1, :], half, 1)
    sub = iota(packed.shape, 0)

    def turned(row):
        value = jnp.broadcast_to(row, (8, cols))
        value = jnp.broadcast_to((value + pltpu.roll(value, half, 1))[0:1, :], packed.shape)
        bit = 1
        while bit < devices:
            value = jnp.where((sub & bit) != 0, pltpu.roll(value, cols - 2 * bit, 1), value)
            bit *= 2
        ahead = pltpu.roll(value, cols - 1, 1)
        ahead = jnp.where(line_lane < quarter, ahead, pltpu.roll(value, quarter - 2, 1))
        return (jnp.where(line_lane < quarter, value[:, 0:1], value[:, 1:2]), ahead)

    other_row = coeff_row - 2.0 * old_row
    (left, left_ahead), (right, right_ahead) = (turned(coeff_row), turned(other_row))
    weight = jnp.where((line_lane == quarter - 1) | (line_lane == half - 1), 0.5, 1.0)
    form = packed * weight * (left * right_ahead + right * left_ahead)
    form = total(jnp.where(line_lane < half, form, 0.0)) + along(spine * coeff_row, other_row)
    image_part = along(coeff_row, image_dots)
    curve_new = smooth_sq - 2.0 * step * mixed + step * step * scaled_sq
    curve_new = curve_new - 2.0 * step * along(coeff_row, reach_dots) + 2.0 * image_part + form
    curve_new = curve_new + 2.0 * ratio * (cross - step * image_sq + image_part)
    curve_new = curve_new + ratio * ratio * curve
    step_new = energy_new / curve_new

    def beside(step_row, step_col):
        r, c = (at_row + step_row, at_col + step_col)
        inside = (r >= 0) & (r < row_count) & (c >= 0) & (c < col_count)
        message = got_ref[jnp.where(inside, r * col_count + c, me)]
        return message * jnp.where(inside, 1.0, 0.0)

    faces = [face_ref[i * rows : (i + 1) * rows, :] for i in range(4)]
    diagonal = face_ref[4 * rows : 5 * rows, :]
    q_north, q_south = (beside(1, 0), beside(-1, 0))
    q_east = to_column(beside(0, 1)[2 * comps : 2 * comps + 1, :], comps * rows, WEST2)
    q_west = to_column(beside(0, -1)[2 * comps : 2 * comps + 1, :], comps * rows, EAST2)

    side_a, side_b = (cola_ref[...], colb_ref[...])
    east_side = pick(even_col, side_a, side_b) * has_east
    west_side = pick(even_col, side_b, side_a) * has_west
    corr = combine(basis_ref, wide_ref, columns, comps, rows)
    for c in range(comps):
        span = slice(c * columns, (c + 1) * columns)
        here = slice(c * rows, (c + 1) * rows)
        sum_a = jnp.sum(wide * rowa_ref[span, :], axis=0, keepdims=True)
        sum_b = jnp.sum(wide * rowb_ref[span, :], axis=0, keepdims=True)
        old = [edge_ref[i * 8 + c : i * 8 + c + 1, :] for i in range(4)]
        p_north = old[0] - step * q_north[comps + c : comps + c + 1, :]
        p_south = old[1] - step * (q_south[c : c + 1, :] / faces[1][0:1, :])
        p_north = p_north + has_north * pick(even_row, sum_a, sum_b) + ratio * old[2]
        p_south = p_south + has_south * pick(even_row, sum_b, sum_a) + ratio * old[3]
        old = [side_ref[(i * comps + c) * rows : (i * comps + c + 1) * rows, :] for i in range(4)]
        p_east = old[0] - step * q_east[here] + ratio * old[2]
        p_west = old[1] - step * (q_west[here] / faces[3][:, 0:1]) + ratio * old[3]
        p_east = p_east + jnp.sum(coeff_row * east_side[here, :], axis=1, keepdims=True)
        p_west = p_west + jnp.sum(coeff_row * west_side[here, :], axis=1, keepdims=True)
        u, p, q, jq = [
            state_ref[(i * comps + c) * rows : (i * comps + c + 1) * rows, :] for i in range(4)
        ]
        new = u - step * jq + corr[c] + ratio * p
        applied = stencil(mask[c], faces, diagonal, new, (p_north, p_south, p_east, p_west))
        solution_ref[here, :] = step * p + step_new * new
        residual_ref[here, :] = rhs_ref[here, :] - step * q - step_new * applied


def last_kernel(count, got_ref, in_ref, last_ref, solution_ref, residual_ref):
    step = last_ref[0:1, :] / jnp.sum(got_ref[...], axis=0)
    solution_ref[...] = in_ref[:count, :] + step * in_ref[count : 2 * count, :]
    residual_ref[...] = in_ref[2 * count : 3 * count, :] - step * in_ref[3 * count :, :]


def on_device(right_side, viscosity, free_mask, coarse_basis, gram_inverse):
    comps, rows, cols = right_side.shape
    columns = coarse_basis.shape[0]
    row_count, col_count = (lax.axis_size("row"), lax.axis_size("col"))
    devices = row_count * col_count
    scale = 1.0 / (32.0 * math.sqrt(float(comps * rows * cols * devices * columns)))
    sizes = (columns, comps, rows, cols)

    def call(kernel, outs, scratch, *args, flops=None):
        cost = flops and pl.CostEstimate(flops=flops, bytes_accessed=4096, transcendentals=0)
        return pl.pallas_call(
            kernel,
            out_shape=[jax.ShapeDtypeStruct(s, F32) for s in outs],
            in_specs=[VMEM] * len(args),
            out_specs=[VMEM] * len(outs),
            scratch_shapes=[pltpu.VMEM(s, F32) for s in scratch],
            cost_estimate=cost,
            compiler_params=pltpu.CompilerParams(vmem_limit_bytes=16 * 1024 * 1024),
        )(*args)

    def share(message):
        return lax.all_to_all(message, ("row", "col"), 0, 0, tiled=True)

    def swap(packet, axis, first):
        pairs = []
        for r in range(row_count):
            for c in range(col_count):
                along, across = ((r, c) if axis == "row" else (c, r))
                length, width = (row_count, col_count)[:: 1 if axis == "row" else -1]
                other = along + 1 if (along - first) % 2 == 0 else along - 1
                if 0 <= other < length:
                    mate = (other, across)
                else:
                    mate = (along, across ^ 1 if (across ^ 1) < width else across)
                r2, c2 = mate if axis == "row" else mate[::-1]
                pairs.append((r * col_count + c, r2 * col_count + c2))
        return lax.ppermute(packet, ("row", "col"), pairs)

    basis = coarse_basis.reshape(columns * comps * rows, cols)
    rhs = right_side.reshape(comps * rows, cols)
    mask = free_mask.reshape(comps * rows, cols)

    block = gram_inverse.size
    piece = -(-block // row_count)
    two = columns * columns == devices * cols and cols == 2 * columns and rows == 8 and comps == 3
    if two:
        (own,) = call(piece_kernel, [(1, cols)], [], gram_inverse, flops=10**9)
    else:
        flat = jnp.pad(gram_inverse.reshape(-1), (0, piece * row_count - block))
        own = lax.dynamic_slice_in_dim(flat, lax.axis_index("row") * piece, piece)
        own = jnp.pad(own, (0, cols - piece)).reshape(1, cols)

    tall = -(-(comps * columns + comps + 2) // 8) * 8
    wide = (comps + 1) * rows
    field = comps * rows
    if two:
        row_a, row_b, col_a, col_b = call(
            functools.partial(packets_kernel, sizes),
            [(tall, cols), (tall, cols), (wide, cols), (wide, cols)],
            [],
            basis, rhs, mask, viscosity, own,
        )
        packets = ((row_a, "row", 0), (row_b, "row", 1), (col_a, "col", 0), (col_b, "col", 1))
        halos = []
        for packet in packets:
            halos.append(swap(*packet))
        (send,) = call(
            functools.partial(gram_kernel, sizes),
            [(devices, 4, cols)],
            [(columns * rows, cols), (columns, cols)],
            basis, rhs, mask, viscosity, own, *halos, col_a, col_b,
        )
        sizes = sizes + (scale,)
        send, *state = call(
            functools.partial(first_kernel, sizes, True, True),
            [(devices, 8, cols), (4 * field, cols), (5 * rows, cols), (32, cols),
             (4 * field, cols), (8, cols), (columns, cols)],
            [(columns * rows, cols), (columns, cols)],
            share(send), basis, rhs, mask, viscosity, *halos,
        )
        solution, residual = call(
            functools.partial(close_kernel, sizes),
            [(field, cols), (field, cols)],
            [(columns, cols)],
            share(send), basis, rhs, mask, *halos, *state,
        )
        return (solution.reshape(right_side.shape), residual.reshape(right_side.shape))
    send, row_a, row_b, col_a, col_b = call(
        functools.partial(pack_kernel, sizes),
        [(devices, 2, cols), (tall, cols), (tall, cols), (wide, cols), (wide, cols)],
        [(columns * rows, cols)],
        basis, rhs, mask, viscosity, own,
    )
    halos = (swap(row_a, "row", 0), swap(row_b, "row", 1), swap(col_a, "col", 0), swap(col_b, "col", 1))
    got = share(send)
    whole_rows = piece == cols and cols % columns == 0 and block == piece * row_count
    gram = ()
    if not whole_rows:
        gram = got[:, 1, :piece].reshape(row_count, col_count, piece).transpose(1, 0, 2)
        gram = gram.reshape(col_count, row_count * piece)[:, :block].reshape(columns, columns)
        gram = (gram,)
    sizes = sizes + (scale,)
    send, *state = call(
        functools.partial(first_kernel, sizes, whole_rows, False),
        [(devices, 1 + comps, cols), (4 * field, cols), (5 * rows, cols), (32, cols),
         (4 * field, cols), (8, cols), (columns, cols)],
        [(columns * rows, cols), (columns, cols)],
        got, *gram, basis, rhs, mask, viscosity, *halos,
    )
    send, fields, last = call(
        functools.partial(second_kernel, sizes),
        [(devices, 1, cols), (4 * field, cols), (8, cols)],
        [(columns, cols)],
        share(send), basis, rhs, mask, *halos, *state,
    )
    solution, residual = call(
        functools.partial(last_kernel, field),
        [(field, cols), (field, cols)],
        [],
        share(send), fields, last,
    )
    return (solution.reshape(right_side.shape), residual.reshape(right_side.shape))


def solution(mesh):
    in_specs = (
        P(None, "row", "col"),
        P("row", "col"),
        P(None, "row", "col"),
        P(None, None, "row", "col"),
        P("col", None),
    )
    out_specs = (P(None, "row", "col"), P(None, "row", "col"))
    return jax.shard_map(
        on_device, mesh=mesh, in_specs=in_specs, out_specs=out_specs, check_vma=False
    )
```

```python
import functools
import math

import jax
import jax.numpy as jnp
from jax import lax
from jax.experimental import pallas as pl
from jax.experimental.pallas import tpu as pltpu
from jax.sharding import PartitionSpec as P


F32 = jnp.float32
VMEM = pl.BlockSpec(memory_space=pltpu.VMEM)
DOTS, EAST, WEST = 64, 72, 96
EAST2, WEST2, DOTS2 = 64, 88, 112


def flags():
    at_row, at_col = (lax.axis_index("row"), lax.axis_index("col"))
    tests = (
        at_row < lax.axis_size("row") - 1,
        at_row > 0,
        at_col < lax.axis_size("col") - 1,
        at_col > 0,
    )
    return [jnp.where(test, 1.0, 0.0) for test in tests]


def iota(shape, dim):
    return lax.broadcasted_iota(jnp.int32, shape, dim)


def pick(flag, yes, no):
    return jnp.where(jnp.full(yes.shape, flag, jnp.int32) == 1, yes, no)


def to_row(column, first=0):
    shape = (column.shape[0], 128)
    spread = jnp.where(iota(shape, 1) == iota(shape, 0) + first, column, 0.0)
    return jnp.sum(spread, axis=0, keepdims=True)


def to_column(row, count, first=0):
    shape = (count, 128)
    spread = jnp.where(iota(shape, 1) == iota(shape, 0) + first, row, 0.0)
    return jnp.sum(spread, axis=1, keepdims=True)


def total(values):
    return jnp.sum(jnp.sum(values, axis=0, keepdims=True), axis=1, keepdims=True)


def shifts(tile, north, south, east, west):
    rows, cols = tile.shape
    sub, lane = (iota(tile.shape, 0), iota(tile.shape, 1))
    return (
        jnp.where(sub == rows - 1, north, pltpu.roll(tile, rows - 1, 0)),
        jnp.where(sub == 0, south, pltpu.roll(tile, 1, 0)),
        jnp.where(lane == cols - 1, east, pltpu.roll(tile, cols - 1, 1)),
        jnp.where(lane == 0, west, pltpu.roll(tile, 1, 1)),
    )


def project(basis_ref, field, acc_ref, columns, comps, rows):
    for k in range(columns):
        base = k * comps * rows
        acc = basis_ref[base : base + rows, :] * field[0]
        for c in range(1, comps):
            acc = acc + basis_ref[base + c * rows : base + (c + 1) * rows, :] * field[c]
        acc_ref[k * rows : (k + 1) * rows, :] = acc
    sums = acc_ref[pl.ds(0, columns, stride=rows), :]
    for s in range(1, rows):
        sums = sums + acc_ref[pl.ds(s, columns, stride=rows), :]
    return jnp.sum(sums, axis=1, keepdims=True)


def combine(basis_ref, wide_ref, columns, comps, rows):
    out = [[None, None] for _ in range(comps)]
    for k in range(columns):
        weight = jnp.broadcast_to(wide_ref[k : k + 1, :], (rows, 128))
        for c in range(comps):
            base = (k * comps + c) * rows
            term = weight * basis_ref[base : base + rows, :]
            old = out[c][k % 2]
            out[c][k % 2] = term if old is None else old + term
    return [a + b for a, b in out]


def pack_kernel(sizes, basis_ref, rhs_ref, mask_ref, visc_ref, gram_ref,
                send_ref, rowa_ref, rowb_ref, cola_ref, colb_ref, acc_ref):
    columns, comps, rows, cols = sizes
    packet_kernel(sizes, basis_ref, rhs_ref, mask_ref, visc_ref, rowa_ref, rowb_ref, cola_ref, colb_ref)
    rhs = [rhs_ref[c * rows : (c + 1) * rows, :] for c in range(comps)]
    visc = visc_ref[...]

    row = to_row(project(basis_ref, rhs, acc_ref, columns, comps, rows))
    lanes = iota((1, cols), 1)
    for i, corner in enumerate(corners_of(visc)):
        row = jnp.where(lanes == columns + i, corner, row)
    both = jnp.concatenate([row, gram_ref[...]], axis=0)
    send_ref[...] = jnp.broadcast_to(both[None], send_ref.shape)


def piece_kernel(gram_ref, piece_ref):
    at = 2 * lax.axis_index("row")
    rows = [gram_ref[pl.ds(at + t, 1), :] for t in range(2)]
    piece_ref[...] = jnp.concatenate(rows, axis=1)


def packets_kernel(sizes, basis_ref, rhs_ref, mask_ref, visc_ref, first_ref, *packet_refs):
    packet_kernel(sizes, basis_ref, rhs_ref, mask_ref, visc_ref, *packet_refs)


def corners_of(visc):
    top, low = (visc.shape[0] - 1, visc.shape[1] - 1)
    return [visc[i : i + 1, j : j + 1] for i in (0, top) for j in (0, low)]


def packet_kernel(sizes, basis_ref, rhs_ref, mask_ref, visc_ref,
                  rowa_ref, rowb_ref, cola_ref, colb_ref):
    columns, comps, rows, cols = sizes
    even_row = 1 - lax.rem(lax.axis_index("row"), 2)
    even_col = 1 - lax.rem(lax.axis_index("col"), 2)
    rhs = [rhs_ref[c * rows : (c + 1) * rows, :] for c in range(comps)]
    mask = [mask_ref[c * rows : (c + 1) * rows, :].astype(F32) for c in range(comps)]
    visc = visc_ref[...]
    lane = iota((rows, cols), 1)
    top, low = rows - 1, cols - 1

    for c in range(comps):
        north = basis_ref[pl.ds(c * rows + top, columns, stride=comps * rows), :]
        south = basis_ref[pl.ds(c * rows, columns, stride=comps * rows), :]
        north = north * mask[c][top : top + 1, :]
        south = south * mask[c][0:1, :]
        rowa_ref[c * columns : (c + 1) * columns, :] = pick(even_row, north, south)
        rowb_ref[c * columns : (c + 1) * columns, :] = pick(even_row, south, north)
    north = [mask[c][top : top + 1, :] * rhs[c][top : top + 1, :] for c in range(comps)]
    south = [mask[c][0:1, :] * rhs[c][0:1, :] for c in range(comps)]
    north += [visc[top : top + 1, :], visc[top - 1 : top, :]]
    south += [visc[0:1, :], visc[1:2, :]]
    for i in range(comps + 2):
        at = comps * columns + i
        rowa_ref[at : at + 1, :] = pick(even_row, north[i], south[i])
        rowb_ref[at : at + 1, :] = pick(even_row, south[i], north[i])
    rest = comps * columns + comps + 2
    blank = jnp.zeros((rowa_ref.shape[0] - rest, cols), F32)
    rowa_ref[rest:, :] = blank
    rowb_ref[rest:, :] = blank

    for c in range(comps):
        east, west = (jnp.zeros((rows, cols), F32), jnp.zeros((rows, cols), F32))
        for k in range(columns):
            base = (k * comps + c) * rows
            tile = basis_ref[base : base + rows, :]
            east = jnp.where(lane == k, pltpu.roll(tile, (k - low) % cols, 1), east)
            west = jnp.where(lane == k, tile if k == 0 else pltpu.roll(tile, k, 1), west)
        east = jnp.where(lane == columns, rhs[c][:, low : low + 1], east)
        west = jnp.where(lane == columns, rhs[c][:, 0:1], west)
        east = east * mask[c][:, low : low + 1]
        west = west * mask[c][:, 0:1]
        cola_ref[c * rows : (c + 1) * rows, :] = pick(even_col, east, west)
        colb_ref[c * rows : (c + 1) * rows, :] = pick(even_col, west, east)
    east = jnp.where(lane == 0, visc[:, low : low + 1], visc[:, low - 1 : low])
    west = jnp.where(lane == 0, visc[:, 0:1], visc[:, 1:2])
    cola_ref[comps * rows :, :] = pick(even_col, east, west)
    colb_ref[comps * rows :, :] = pick(even_col, west, east)


def stencil(mask, faces, diagonal, tile, halo):
    masked = mask * tile
    near = shifts(masked, *halo)
    inner = diagonal * masked - (
        faces[0] * near[0] + faces[1] * near[1] + faces[2] * near[2] + faces[3] * near[3]
    )
    return mask * inner + (1.0 - mask) * tile


def split(values):
    high = values.astype(jnp.bfloat16)
    return jnp.concatenate([high, (values - high.astype(F32)).astype(jnp.bfloat16)], axis=0)


def product(lefts, rights):
    return lax.dot_general(
        jnp.concatenate([split(value) for value in lefts], axis=1),
        jnp.concatenate([split(value) for value in rights], axis=1),
        (((1,), (1,)), ((), ())),
        preferred_element_type=F32,
    )


def merge(blocks, columns):
    blocks = blocks + pltpu.roll(blocks, columns, 1)
    return blocks[:columns] + blocks[columns:]


def local_kernel(sizes, basis_ref, rhs_ref, mask_ref, visc_ref, inner_ref, dots_ref, acc_ref):
    columns, comps, rows, cols = sizes
    _, has_south, _, has_west = flags()
    top, low = (rows - 1, cols - 1)
    rhs = [rhs_ref[c * rows : (c + 1) * rows, :] for c in range(comps)]
    mask = [mask_ref[c * rows : (c + 1) * rows, :].astype(F32) for c in range(comps)]
    visc = visc_ref[...]
    sub, lane = (iota((rows, cols), 0), iota((rows, cols), 1))
    empty = (jnp.zeros((1, cols), F32),) * 2 + (jnp.zeros((rows, 1), F32),) * 2
    faces = [0.5 * (visc + v) for v in shifts(visc, *empty)]
    faces[0] = jnp.where(sub == top, 0.0, faces[0])
    faces[1] = jnp.where(sub == 0, faces[1] * (1.0 - has_south), faces[1])
    faces[2] = jnp.where(lane == low, 0.0, faces[2])
    faces[3] = jnp.where(lane == 0, faces[3] * (1.0 - has_west), faces[3])
    diagonal = 1.0 + faces[0] + faces[1] + faces[2] + faces[3]

    blocks = jnp.zeros((2 * columns, 2 * columns), F32)
    for c in range(comps):
        m = mask[c]
        own = m * diagonal + (1.0 - m)
        up, down = (m * faces[0], m * faces[1])
        right = m * faces[2]
        left = jnp.where(lane == 0, 0.0, m * faces[3])
        plain = [
            basis_ref[pl.ds(c * rows + i, columns, stride=comps * rows), :] for i in range(rows)
        ]
        free = [plain[i] * m[i : i + 1, :] for i in range(rows)]
        images = []
        for i in range(rows):
            here = slice(i, i + 1)
            value = own[here] * plain[i] - right[here] * pltpu.roll(free[i], low, 1)
            value = value - left[here] * pltpu.roll(free[i], 1, 1)
            if i < top:
                value = value - up[here] * free[i + 1]
            if i > 0:
                value = value - down[here] * free[i - 1]
            images.append(value)
        for i in range(0, rows, 2):
            blocks = blocks + product(plain[i : i + 2], images[i : i + 2])
    inner_ref[...] = merge(blocks, columns)
    dots = to_row(project(basis_ref, rhs, acc_ref, columns, comps, rows))
    dots_ref[...] = jnp.broadcast_to(dots, dots_ref.shape)


def border_kernel(sizes, inner_ref, dots_ref, basis_ref, mask_ref, visc_ref, gram_ref, rowa_ref,
                  rowb_ref, cola_ref, colb_ref, owna_ref, ownb_ref, send_ref, full_ref):
    columns, comps, rows, cols = sizes
    even_row = 1 - lax.rem(lax.axis_index("row"), 2)
    even_col = 1 - lax.rem(lax.axis_index("col"), 2)
    has_north, _, has_east, _ = flags()
    top, low, half = (rows - 1, cols - 1, cols // 2)
    field = comps * rows
    visc, lanes = (visc_ref[...], iota((1, cols), 1))
    at = comps * columns + comps
    v_north = pick(even_row, rowa_ref[at : at + 1, :], rowb_ref[at : at + 1, :]) * has_north
    east = pick(even_col, cola_ref[...], colb_ref[...]) * has_east
    own_east = pick(even_col, owna_ref[...], ownb_ref[...])
    north_face = 0.5 * (visc[top : top + 1, :] + v_north)
    east_face = 0.5 * (visc[:, low : low + 1] + east[field:, 0:1])
    tops = []
    for c in range(comps):
        span = slice(c * columns, (c + 1) * columns)
        own = basis_ref[pl.ds(c * rows + top, columns, stride=comps * rows), :]
        own = own * mask_ref[c * rows + top : c * rows + rows, :].astype(F32)
        tops.append(own - pick(even_row, rowa_ref[span, :], rowb_ref[span, :]) * has_north)
    full = inner_ref[...] + merge(product([value * north_face for value in tops], tops), columns)
    gap = own_east[:field] - east[:field]
    edge = lax.dot_general(
        gap * jnp.concatenate([east_face] * comps, axis=0), gap, (((0,), (0,)), ((), ())),
        preferred_element_type=F32, precision=lax.Precision.HIGHEST,
    )
    wide_lane = iota((columns, cols), 1)
    edge = jnp.where(wide_lane < half, edge[:columns], 0.0)
    full = full + edge + pltpu.roll(edge, half, 1)
    full_ref[...] = full
    spot = jnp.where(wide_lane >= half, wide_lane - half, wide_lane) == iota((columns, cols), 0)
    spine = jnp.sum(jnp.where(spot, full, 0.0), axis=0, keepdims=True)
    count = columns // 2
    chunk = jnp.where(
        iota((count, cols), 1) < half,
        full_ref[pl.ds(0, count, stride=2), :],
        full_ref[pl.ds(1, count, stride=2), :],
    )
    dots = dots_ref[0:1, :]
    corner_row = jnp.zeros((1, cols), F32)
    for i, corner in enumerate(corners_of(visc)):
        corner_row = jnp.where(lanes == i, corner, corner_row)
    head = jnp.concatenate([jnp.where(lanes < half, dots, spine), gram_ref[...]], axis=0)
    for d in range(count):
        send_ref[d] = jnp.concatenate([head, chunk[d : d + 1, :], corner_row], axis=0)


def first_kernel(sizes, whole_rows, two, got_ref, *refs):
    columns, comps, rows, cols, scale = sizes
    if whole_rows:
        gram_in_ref = None
    else:
        gram_in_ref, *refs = refs
    (basis_ref, rhs_ref, mask_ref, visc_ref, rowa_ref, rowb_ref, cola_ref, colb_ref,
     send_ref, state_ref, face_ref, small_ref, gram_ref, *refs) = refs
    edge_ref, side_ref = (None, None) if two else refs[:2]
    acc_ref, wide_ref = refs[-2:]
    at_row, at_col = (lax.axis_index("row"), lax.axis_index("col"))
    row_count, col_count = (lax.axis_size("row"), lax.axis_size("col"))
    even_row, even_col = (1 - lax.rem(at_row, 2), 1 - lax.rem(at_col, 2))
    me = at_row * col_count + at_col
    top, low = rows - 1, cols - 1
    rhs = [rhs_ref[c * rows : (c + 1) * rows, :] for c in range(comps)]
    mask = [mask_ref[c * rows : (c + 1) * rows, :].astype(F32) for c in range(comps)]
    visc = visc_ref[...]
    sub, lane = (iota((rows, cols), 0), iota((rows, cols), 1))
    lanes = iota((1, cols), 1)

    if whole_rows:
        per = cols // columns
        for r in range(row_count):
            for c in range(col_count):
                piece = got_ref[r * col_count + c, 1:2, :]
                for t in range(per):
                    at = (c * row_count + r) * per + t
                    moved = pltpu.roll(piece, cols - t * columns, 1) if t else piece
                    gram_ref[at : at + 1, :] = moved
    else:
        gram_ref[:, :columns] = gram_in_ref[...]
    all_sums = jnp.sum(got_ref[...], axis=0)
    sums = all_sums[0:1, :]
    dots = jnp.where(lanes < columns, sums, 0.0)
    gram = jnp.where(iota((columns, cols), 1) < columns, gram_ref[...], 0.0)
    coeffs = jnp.sum(gram * dots, axis=1, keepdims=True) * scale
    wide = jnp.broadcast_to(coeffs, (columns, cols))
    wide_ref[...] = wide
    coeff_row = to_row(coeffs)

    extra = comps * columns
    tail_a, tail_b = (rowa_ref[extra:, :], rowb_ref[extra:, :])
    has_north, has_south, has_east, has_west = flags()
    north_tail = pick(even_row, tail_a, tail_b) * has_north
    south_tail = pick(even_row, tail_b, tail_a) * has_south
    side_a, side_b = (cola_ref[...], colb_ref[...])
    east_side = pick(even_col, side_a, side_b) * has_east
    west_side = pick(even_col, side_b, side_a) * has_west
    v_north, v_south = (north_tail[comps : comps + 1, :], south_tail[comps : comps + 1, :])
    v_north2, v_south2 = (north_tail[comps + 1 : comps + 2, :], south_tail[comps + 1 : comps + 2, :])
    v_east, v_west = (east_side[comps * rows :, 0:1], west_side[comps * rows :, 0:1])
    v_east2, v_west2 = (east_side[comps * rows :, 1:2], west_side[comps * rows :, 1:2])
    faces = [0.5 * (visc + v) for v in shifts(visc, v_north, v_south, v_east, v_west)]
    diagonal = 1.0 + faces[0] + faces[1] + faces[2] + faces[3]
    face_ref[...] = jnp.concatenate(faces + [diagonal], axis=0)
    jacobi = [m / diagonal + (1.0 - m) for m in mask]

    def corner(step_row, step_col, which):
        r, c = (at_row + step_row, at_col + step_col)
        inside = (r >= 0) & (r < row_count) & (c >= 0) & (c < col_count)
        place = jnp.where(inside, r * col_count + c, me)
        line, first = (3, 0) if two else (0, columns)
        value = got_ref[place, line : line + 1, :]
        value = jnp.sum(jnp.where(lanes == first + which, value, 0.0), axis=1, keepdims=True)
        return value * jnp.where(inside, 1.0, 0.0)

    north_west, north_east = (corner(1, -1, 1), corner(1, 1, 0))
    south_west, south_east = (corner(-1, -1, 3), corner(-1, 1, 2))

    def row_inverse(own, inner, outer, west, east):
        right = jnp.where(lanes == low, east, pltpu.roll(own, low, 1))
        left = jnp.where(lanes == 0, west, pltpu.roll(own, 1, 1))
        return 1.0 / (1.0 + 0.5 * (4.0 * own + inner + outer + left + right))

    def side_inverse(own, inner, outer, south, north):
        own = jnp.broadcast_to(own, (rows, cols))
        up = jnp.where(sub == top, north, pltpu.roll(own, top, 0))
        down = jnp.where(sub == 0, south, pltpu.roll(own, 1, 0))
        return 1.0 / (1.0 + 0.5 * (4.0 * own + inner + outer + up + down))

    inv_north = row_inverse(v_north, visc[top : top + 1, :], v_north2, north_west, north_east)
    inv_south = row_inverse(v_south, visc[0:1, :], v_south2, south_west, south_east)
    inv_east = side_inverse(v_east, visc[:, low : low + 1], v_east2, south_east, north_east)
    inv_west = side_inverse(v_west, visc[:, 0:1], v_west2, south_west, north_west)

    corr = combine(basis_ref, wide_ref, columns, comps, rows)
    image, scaled, smooth, point = ([], [], [], [])
    scaled_image = []
    none = (jnp.zeros((1, cols), F32),) * 2 + (jnp.zeros((rows, 1), F32),) * 2
    for c in range(comps):
        span = slice(c * columns, (c + 1) * columns)
        sum_a = jnp.sum(wide * rowa_ref[span, :], axis=0, keepdims=True)
        sum_b = jnp.sum(wide * rowb_ref[span, :], axis=0, keepdims=True)
        u_north = inv_north * north_tail[c : c + 1, :]
        u_south = inv_south * south_tail[c : c + 1, :]
        p_north = u_north + has_north * pick(even_row, sum_a, sum_b)
        p_south = u_south + has_south * pick(even_row, sum_b, sum_a)
        here = slice(c * rows, (c + 1) * rows)
        east, west = (east_side[here, :], west_side[here, :])
        u_east = inv_east * east[:, columns : columns + 1]
        u_west = inv_west * west[:, columns : columns + 1]
        p_east = u_east + jnp.sum(coeff_row * east, axis=1, keepdims=True)
        p_west = u_west + jnp.sum(coeff_row * west, axis=1, keepdims=True)
        u = jacobi[c] * rhs[c]
        p = u + corr[c]
        q = stencil(mask[c], faces, diagonal, p, (p_north, p_south, p_east, p_west))
        if two:
            scaled_image.append(stencil(mask[c], faces, diagonal, jacobi[c] * q, none))
        smooth.append(u)
        point.append(p)
        image.append(q)
        scaled.append(jacobi[c] * q)
        if two:
            continue
        for i, value in enumerate((u_north, u_south, p_north, p_south)):
            edge_ref[i * 8 + c : i * 8 + c + 1, :] = value
        for i, value in enumerate((u_east, u_west, p_east, p_west)):
            side_ref[(i * comps + c) * rows : (i * comps + c + 1) * rows, :] = value
    fields = point + image + scaled
    state_ref[...] = jnp.concatenate(fields if two else smooth + fields, axis=0)

    row = to_row(project(basis_ref, image, acc_ref, columns, comps, rows))
    pairs = ((point, image), (smooth, image), (image, scaled), (rhs, smooth))
    if two:
        pairs += ((scaled, scaled_image),)
    for i, (left, right) in enumerate(pairs):
        value = left[0] * right[0]
        for c in range(1, comps):
            value = value + left[c] * right[c]
        row = jnp.where(lanes == (DOTS2 if two else DOTS) + i, total(value), row)
    masked = [mask[c] * scaled[c] for c in range(comps)]
    if two:
        norths = [m[top : top + 1, :] * faces[0][top : top + 1, :] * has_north for m in masked]
        easts = [m[:, low : low + 1] * faces[2][:, low : low + 1] * has_east for m in masked]
        souths, wests = ([m[0:1, :] for m in masked], [m[:, 0:1] for m in masked])
        row = row + to_row(jnp.concatenate(easts, axis=0), EAST2)
        row = row + to_row(jnp.concatenate(wests, axis=0), WEST2)
        reach = project(basis_ref, scaled_image, acc_ref, columns, comps, rows)
        beyond = jnp.zeros((columns, cols), F32)
        aside = jnp.zeros((rows, cols), F32)
        for c in range(comps):
            span, here = (slice(c * columns, (c + 1) * columns), slice(c * rows, (c + 1) * rows))
            halo_a, halo_b = (rowa_ref[span, :], rowb_ref[span, :])
            low_side = souths[c] * faces[1][0:1, :] * has_south
            beyond = beyond + norths[c] * pick(even_row, halo_a, halo_b)
            beyond = beyond + low_side * pick(even_row, halo_b, halo_a)
            aside = aside + easts[c] * east_side[here, :]
            aside = aside + wests[c] * faces[3][:, 0:1] * west_side[here, :]
        reach = to_row(reach - jnp.sum(beyond, axis=1, keepdims=True))
        reach = reach - jnp.where(lanes < columns, jnp.sum(aside, axis=0, keepdims=True), 0.0)
        half = cols // 2
        ours = jnp.broadcast_to(all_sums[2:3, :], (8, cols))
        other = pltpu.roll(ours, half, 1)
        wide_lane = iota((8, cols), 1)
        for t, (first, second) in enumerate(((ours, other), (other, ours))):
            value = jnp.where(wide_lane < half, first, second)
            turn = lax.rem(half + t * (half // 2) - (2 * me + t + 1) + 2 * cols, cols)
            value = pltpu.roll(value, turn, 1)[0:1, :]
            start = half + t * (half // 2)
            reach = jnp.where((lanes >= start) & (lanes < start + half // 2), value, reach)
        message = jnp.concatenate(norths + souths + [row, reach], axis=0)
        send_ref[...] = jnp.broadcast_to(message[None], send_ref.shape)
        spine = pltpu.roll(jnp.broadcast_to(sums, (8, cols)), half, 1)[0:1, :]
        spine = jnp.where(lanes < half, spine, 0.0)
        small_ref[...] = jnp.concatenate([dots, coeff_row, spine, jnp.zeros((5, cols), F32)], axis=0)
        return
    east = jnp.concatenate([m[:, low : low + 1] for m in masked], axis=0)
    west = jnp.concatenate([m[:, 0:1] for m in masked], axis=0)
    row = row + to_row(east, EAST) + to_row(west, WEST)
    message = jnp.concatenate([row] + [m[top : top + 1, :] for m in masked], axis=0)
    send_ref[...] = jnp.broadcast_to(message[None], send_ref.shape)
    message = jnp.concatenate([row] + [m[0:1, :] for m in masked], axis=0)
    send_ref[jnp.where(at_row > 0, me - col_count, me)] = message
    small_ref[...] = jnp.concatenate([dots, coeff_row, jnp.zeros((6, cols), F32)], axis=0)


def second_kernel(sizes, got_ref, basis_ref, rhs_ref, mask_ref, rowa_ref, rowb_ref, cola_ref,
                  colb_ref, state_ref, face_ref, small_ref, gram_ref, edge_ref, side_ref,
                  send_ref, out_ref, last_ref, wide_ref):
    columns, comps, rows, cols, scale = sizes
    at_row, at_col = (lax.axis_index("row"), lax.axis_index("col"))
    row_count, col_count = (lax.axis_size("row"), lax.axis_size("col"))
    even_row, even_col = (1 - lax.rem(at_row, 2), 1 - lax.rem(at_col, 2))
    me = at_row * col_count + at_col
    lanes = iota((1, cols), 1)
    mask = [mask_ref[c * rows : (c + 1) * rows, :].astype(F32) for c in range(comps)]

    sums = jnp.sum(got_ref[...], axis=0)[0:1, :]
    image_dots = jnp.where(lanes < columns, sums, 0.0)
    curve, cross, image_sq, rhs_sq = [
        jnp.sum(jnp.where(lanes == DOTS + i, sums, 0.0), axis=1, keepdims=True) for i in range(4)
    ]
    dots, coeff_row = (small_ref[0:1, :], small_ref[1:2, :])
    energy = rhs_sq + jnp.sum(dots * coeff_row, axis=1, keepdims=True)
    step = energy / curve
    gram = jnp.where(iota((columns, cols), 1) < columns, gram_ref[...], 0.0)
    dots = dots - step * image_dots
    coeffs = jnp.sum(gram * dots, axis=1, keepdims=True) * scale
    wide = jnp.broadcast_to(coeffs, (columns, cols))
    wide_ref[...] = wide
    coeff_row = to_row(coeffs)
    energy_new = rhs_sq - 2.0 * step * cross + step * step * image_sq
    energy_new = energy_new + jnp.sum(dots * coeff_row, axis=1, keepdims=True)
    ratio = energy_new / energy

    def beside(step_row, step_col):
        r, c = (at_row + step_row, at_col + step_col)
        inside = (r >= 0) & (r < row_count) & (c >= 0) & (c < col_count)
        message = got_ref[jnp.where(inside, r * col_count + c, me)]
        return message * jnp.where(inside, 1.0, 0.0)

    q_north, q_south = (beside(1, 0), beside(-1, 0))
    q_east = to_column(beside(0, 1)[0:1, :], comps * rows, WEST)
    q_west = to_column(beside(0, -1)[0:1, :], comps * rows, EAST)

    side_a, side_b = (cola_ref[...], colb_ref[...])
    has_north, has_south, has_east, has_west = flags()
    east_side = pick(even_col, side_a, side_b) * has_east
    west_side = pick(even_col, side_b, side_a) * has_west
    faces = [face_ref[i * rows : (i + 1) * rows, :] for i in range(4)]
    diagonal = face_ref[4 * rows : 5 * rows, :]
    corr = combine(basis_ref, wide_ref, columns, comps, rows)
    curve_part = jnp.zeros((rows, cols), F32)
    first, second, third, fourth = ([], [], [], [])
    for c in range(comps):
        span = slice(c * columns, (c + 1) * columns)
        here = slice(c * rows, (c + 1) * rows)
        sum_a = jnp.sum(wide * rowa_ref[span, :], axis=0, keepdims=True)
        sum_b = jnp.sum(wide * rowb_ref[span, :], axis=0, keepdims=True)
        old = [edge_ref[i * 8 + c : i * 8 + c + 1, :] for i in range(4)]
        p_north = old[0] - step * q_north[1 + c : 2 + c, :] + has_north * pick(even_row, sum_a, sum_b)
        p_south = old[1] - step * q_south[1 + c : 2 + c, :] + has_south * pick(even_row, sum_b, sum_a)
        p_north, p_south = (p_north + ratio * old[2], p_south + ratio * old[3])
        old = [side_ref[(i * comps + c) * rows : (i * comps + c + 1) * rows, :] for i in range(4)]
        p_east = old[0] - step * q_east[here] + ratio * old[2]
        p_west = old[1] - step * q_west[here] + ratio * old[3]
        p_east = p_east + jnp.sum(coeff_row * east_side[here, :], axis=1, keepdims=True)
        p_west = p_west + jnp.sum(coeff_row * west_side[here, :], axis=1, keepdims=True)
        u, p, q, jq = [
            state_ref[(i * comps + c) * rows : (i * comps + c + 1) * rows, :] for i in range(4)
        ]
        new = u - step * jq + corr[c] + ratio * p
        masked = mask[c] * new
        near = shifts(masked, p_north, p_south, p_east, p_west)
        stencil = diagonal * masked - (
            faces[0] * near[0] + faces[1] * near[1] + faces[2] * near[2] + faces[3] * near[3]
        )
        applied = mask[c] * stencil + (1.0 - mask[c]) * new
        curve_part = curve_part + new * applied
        first.append(step * p)
        second.append(new)
        third.append(rhs_ref[here, :] - step * q)
        fourth.append(applied)
    out_ref[...] = jnp.concatenate(first + second + third + fourth, axis=0)
    last_ref[...] = jnp.broadcast_to(energy_new, last_ref.shape)
    send_ref[...] = jnp.broadcast_to(total(curve_part)[None], send_ref.shape)


def close_kernel(sizes, got_ref, basis_ref, rhs_ref, mask_ref, rowa_ref, rowb_ref, cola_ref,
                 colb_ref, state_ref, face_ref, small_ref, gram_ref,
                 solution_ref, residual_ref, wide_ref):
    columns, comps, rows, cols, scale = sizes
    at_row, at_col = (lax.axis_index("row"), lax.axis_index("col"))
    row_count, col_count = (lax.axis_size("row"), lax.axis_size("col"))
    devices = row_count * col_count
    even_row, even_col = (1 - lax.rem(at_row, 2), 1 - lax.rem(at_col, 2))
    has_north, has_south, has_east, has_west = flags()
    me = at_row * col_count + at_col
    half, quarter = (cols // 2, cols // 4)
    lanes = iota((1, cols), 1)
    mask = [mask_ref[c * rows : (c + 1) * rows, :].astype(F32) for c in range(comps)]

    def along(left, right):
        return jnp.sum(left * right, axis=1, keepdims=True)

    sums = jnp.sum(got_ref[...], axis=0)
    line = sums[2 * comps : 2 * comps + 1, :]
    image_dots = jnp.where(lanes < columns, line, 0.0)
    reach_dots = jnp.where(lanes < columns, sums[2 * comps + 1 :, :], 0.0)
    gram = jnp.where(iota((columns, cols), 1) < columns, gram_ref[...], 0.0)
    turn = jnp.sum(gram * image_dots, axis=1, keepdims=True) * scale
    wide = jnp.broadcast_to(turn, (columns, cols))
    wide_ref[...] = wide
    turn_row = to_row(turn)

    def beside(step_row, step_col):
        r, c = (at_row + step_row, at_col + step_col)
        inside = (r >= 0) & (r < row_count) & (c >= 0) & (c < col_count)
        message = got_ref[jnp.where(inside, r * col_count + c, me)]
        return message * jnp.where(inside, 1.0, 0.0)

    faces = [face_ref[i * rows : (i + 1) * rows, :] for i in range(4)]
    diagonal = face_ref[4 * rows : 5 * rows, :]
    q_north, q_south = (beside(1, 0), beside(-1, 0))
    q_east = to_column(beside(0, 1)[2 * comps : 2 * comps + 1, :], comps * rows, WEST2)
    q_west = to_column(beside(0, -1)[2 * comps : 2 * comps + 1, :], comps * rows, EAST2)
    side_a, side_b = (cola_ref[...], colb_ref[...])
    east_side = pick(even_col, side_a, side_b) * has_east
    west_side = pick(even_col, side_b, side_a) * has_west
    corr = combine(basis_ref, wide_ref, columns, comps, rows)
    moved, moved_image = ([], [])
    for c in range(comps):
        span = slice(c * columns, (c + 1) * columns)
        here = slice(c * rows, (c + 1) * rows)
        sum_a = jnp.sum(wide * rowa_ref[span, :], axis=0, keepdims=True)
        sum_b = jnp.sum(wide * rowb_ref[span, :], axis=0, keepdims=True)
        north = q_north[comps + c : comps + c + 1, :] + has_north * pick(even_row, sum_a, sum_b)
        south = q_south[c : c + 1, :] / faces[1][0:1, :] + has_south * pick(even_row, sum_b, sum_a)
        east = q_east[here] + along(turn_row, east_side[here, :])
        west = q_west[here] / faces[3][:, 0:1] + along(turn_row, west_side[here, :])
        at = (2 * comps + c) * rows
        value = state_ref[at : at + rows, :] + corr[c]
        moved.append(value)
        moved_image.append(stencil(mask[c], faces, diagonal, value, (north, south, east, west)))

    border = jnp.zeros((2 * comps + 2, cols), F32)
    for d in range(devices - col_count):
        border = border + got_ref[d] * pltpu.roll(got_ref[d + col_count], comps + 2, 0)
    border = jnp.where(iota(border.shape, 0) < comps, border, 0.0)
    lines = got_ref[:, 2 * comps, :]
    later = pltpu.roll(pltpu.roll(lines, devices - 1, 0), cols - (WEST2 - EAST2), 1)
    line_lane = iota(lines.shape, 1)
    beside_it = jnp.where((line_lane >= EAST2) & (line_lane < WEST2), lines * later, 0.0)
    across = jnp.sum(border, axis=0, keepdims=True) + jnp.sum(beside_it, axis=0, keepdims=True)

    packed = pltpu.roll(got_ref[:, 2 * comps + 1, :], half, 1)
    sub = iota(packed.shape, 0)
    value = jnp.broadcast_to(turn_row, (8, cols))
    value = jnp.broadcast_to((value + pltpu.roll(value, half, 1))[0:1, :], packed.shape)
    bit = 1
    while bit < devices:
        value = jnp.where((sub & bit) != 0, pltpu.roll(value, cols - 2 * bit, 1), value)
        bit *= 2
    ahead = pltpu.roll(value, cols - 1, 1)
    ahead = jnp.where(line_lane < quarter, ahead, pltpu.roll(value, quarter - 2, 1))
    own = jnp.where(line_lane < quarter, value[:, 0:1], value[:, 1:2])
    weight = jnp.where((line_lane == quarter - 1) | (line_lane == half - 1), 1.0, 2.0)
    form = jnp.where(line_lane < half, packed * weight * own * ahead, 0.0)
    form = jnp.sum(form, axis=0, keepdims=True)

    curve, cross, image_sq, rhs_sq, scaled_sq = [
        along(jnp.where(lanes == DOTS2 + i, 1.0, 0.0), line) for i in range(5)
    ]
    dots, old_row, spine = (small_ref[0:1, :], small_ref[1:2, :], small_ref[2:3, :])
    energy = rhs_sq + along(dots, old_row)
    meet = image_sq + along(turn_row, image_dots)
    rest = form + spine * turn_row * turn_row + 2.0 * turn_row * reach_dots - 2.0 * across
    moved_sq = scaled_sq + jnp.sum(rest, axis=1, keepdims=True)
    step = energy / curve
    energy_new = rhs_sq - 2.0 * step * cross + step * step * image_sq
    energy_new = energy_new + along(dots - step * image_dots, old_row - step * turn_row)
    grow = 1.0 + energy_new / energy
    curve_new = grow * grow * curve - 2.0 * step * grow * meet + step * step * moved_sq
    step_new = energy_new / curve_new
    near, far = (step + step_new * grow, step_new * step)
    for c in range(comps):
        here = slice(c * rows, (c + 1) * rows)
        p = state_ref[here, :]
        q = state_ref[(comps + c) * rows : (comps + c + 1) * rows, :]
        solution_ref[here, :] = near * p - far * moved[c]
        residual_ref[here, :] = rhs_ref[here, :] - near * q + far * moved_image[c]


def last_kernel(count, got_ref, in_ref, last_ref, solution_ref, residual_ref):
    step = last_ref[0:1, :] / jnp.sum(got_ref[...], axis=0)
    solution_ref[...] = in_ref[:count, :] + step * in_ref[count : 2 * count, :]
    residual_ref[...] = in_ref[2 * count : 3 * count, :] - step * in_ref[3 * count :, :]


def on_device(right_side, viscosity, free_mask, coarse_basis, gram_inverse):
    comps, rows, cols = right_side.shape
    columns = coarse_basis.shape[0]
    row_count, col_count = (lax.axis_size("row"), lax.axis_size("col"))
    devices = row_count * col_count
    scale = 1.0 / (32.0 * math.sqrt(float(comps * rows * cols * devices * columns)))
    sizes = (columns, comps, rows, cols)

    def call(kernel, outs, scratch, *args, flops=None):
        cost = flops and pl.CostEstimate(flops=flops, bytes_accessed=4096, transcendentals=0)
        return pl.pallas_call(
            kernel,
            out_shape=[jax.ShapeDtypeStruct(s, F32) for s in outs],
            in_specs=[VMEM] * len(args),
            out_specs=[VMEM] * len(outs),
            scratch_shapes=[pltpu.VMEM(s, F32) for s in scratch],
            cost_estimate=cost,
            compiler_params=pltpu.CompilerParams(vmem_limit_bytes=16 * 1024 * 1024),
        )(*args)

    def share(message):
        return lax.all_to_all(message, ("row", "col"), 0, 0, tiled=True)

    def swap(packet, axis, first):
        pairs = []
        for r in range(row_count):
            for c in range(col_count):
                along, across = ((r, c) if axis == "row" else (c, r))
                length, width = (row_count, col_count)[:: 1 if axis == "row" else -1]
                other = along + 1 if (along - first) % 2 == 0 else along - 1
                if 0 <= other < length:
                    mate = (other, across)
                else:
                    mate = (along, across ^ 1 if (across ^ 1) < width else across)
                r2, c2 = mate if axis == "row" else mate[::-1]
                pairs.append((r * col_count + c, r2 * col_count + c2))
        return lax.ppermute(packet, ("row", "col"), pairs)

    basis = coarse_basis.reshape(columns * comps * rows, cols)
    rhs = right_side.reshape(comps * rows, cols)
    mask = free_mask.reshape(comps * rows, cols)

    block = gram_inverse.size
    piece = -(-block // row_count)
    two = columns * columns == devices * cols and cols == 2 * columns and rows == 8 and comps == 3
    if two:
        (own,) = call(piece_kernel, [(1, cols)], [], gram_inverse, flops=10**9)
    else:
        flat = jnp.pad(gram_inverse.reshape(-1), (0, piece * row_count - block))
        own = lax.dynamic_slice_in_dim(flat, lax.axis_index("row") * piece, piece)
        own = jnp.pad(own, (0, cols - piece)).reshape(1, cols)

    tall = -(-(comps * columns + comps + 2) // 8) * 8
    wide = (comps + 1) * rows
    field = comps * rows
    if two:
        row_a, row_b, col_a, col_b = call(
            functools.partial(packets_kernel, sizes),
            [(tall, cols), (tall, cols), (wide, cols), (wide, cols)],
            [],
            basis, rhs, mask, viscosity, own,
        )
        packets = ((row_a, "row", 0), (row_b, "row", 1), (col_a, "col", 0), (col_b, "col", 1))
        halos = []
        for packet in packets:
            halos.append(swap(*packet))
        inner, dots = call(
            functools.partial(local_kernel, sizes),
            [(columns, cols), (8, cols)],
            [(columns * rows, cols)],
            basis, rhs, mask, viscosity, flops=10**8,
        )
        (send,) = call(
            functools.partial(border_kernel, sizes),
            [(devices, 4, cols)],
            [(columns, cols)],
            inner, dots, basis, mask, viscosity, own, *halos, col_a, col_b,
        )
        sizes = sizes + (scale,)
        send, *state = call(
            functools.partial(first_kernel, sizes, True, True),
            [(devices, 8, cols), (3 * field, cols), (5 * rows, cols), (8, cols), (columns, cols)],
            [(columns * rows, cols), (columns, cols)],
            share(send), basis, rhs, mask, viscosity, *halos,
        )
        solution, residual = call(
            functools.partial(close_kernel, sizes),
            [(field, cols), (field, cols)],
            [(columns, cols)],
            share(send), basis, rhs, mask, *halos, *state,
        )
        return (solution.reshape(right_side.shape), residual.reshape(right_side.shape))
    send, row_a, row_b, col_a, col_b = call(
        functools.partial(pack_kernel, sizes),
        [(devices, 2, cols), (tall, cols), (tall, cols), (wide, cols), (wide, cols)],
        [(columns * rows, cols)],
        basis, rhs, mask, viscosity, own,
    )
    halos = (swap(row_a, "row", 0), swap(row_b, "row", 1), swap(col_a, "col", 0), swap(col_b, "col", 1))
    got = share(send)
    whole_rows = piece == cols and cols % columns == 0 and block == piece * row_count
    gram = ()
    if not whole_rows:
        gram = got[:, 1, :piece].reshape(row_count, col_count, piece).transpose(1, 0, 2)
        gram = gram.reshape(col_count, row_count * piece)[:, :block].reshape(columns, columns)
        gram = (gram,)
    sizes = sizes + (scale,)
    send, *state = call(
        functools.partial(first_kernel, sizes, whole_rows, False),
        [(devices, 1 + comps, cols), (4 * field, cols), (5 * rows, cols), (8, cols),
         (columns, cols), (32, cols), (4 * field, cols)],
        [(columns * rows, cols), (columns, cols)],
        got, *gram, basis, rhs, mask, viscosity, *halos,
    )
    send, fields, last = call(
        functools.partial(second_kernel, sizes),
        [(devices, 1, cols), (4 * field, cols), (8, cols)],
        [(columns, cols)],
        share(send), basis, rhs, mask, *halos, *state,
    )
    solution, residual = call(
        functools.partial(last_kernel, field),
        [(field, cols), (field, cols)],
        [],
        share(send), fields, last,
    )
    return (solution.reshape(right_side.shape), residual.reshape(right_side.shape))


def solution(mesh):
    in_specs = (
        P(None, "row", "col"),
        P("row", "col"),
        P(None, "row", "col"),
        P(None, None, "row", "col"),
        P("col", None),
    )
    out_specs = (P(None, "row", "col"), P(None, "row", "col"))
    return jax.shard_map(
        on_device, mesh=mesh, in_specs=in_specs, out_specs=out_specs, check_vma=False
    )
```

```python
import functools
import math

import jax
import jax.numpy as jnp
from jax import lax
from jax.experimental import pallas as pl
from jax.experimental.pallas import tpu as pltpu
from jax.sharding import PartitionSpec as P


F32 = jnp.float32
VMEM = pl.BlockSpec(memory_space=pltpu.VMEM)
DOTS, EAST, WEST = 64, 72, 96
EAST2, WEST2, DOTS2 = 64, 88, 112


def flags():
    at_row, at_col = (lax.axis_index("row"), lax.axis_index("col"))
    tests = (
        at_row < lax.axis_size("row") - 1,
        at_row > 0,
        at_col < lax.axis_size("col") - 1,
        at_col > 0,
    )
    return [jnp.where(test, 1.0, 0.0) for test in tests]


def iota(shape, dim):
    return lax.broadcasted_iota(jnp.int32, shape, dim)


def pick(flag, yes, no):
    return jnp.where(jnp.full(yes.shape, flag, jnp.int32) == 1, yes, no)


def to_row(column, first=0):
    shape = (column.shape[0], 128)
    spread = jnp.where(iota(shape, 1) == iota(shape, 0) + first, column, 0.0)
    return jnp.sum(spread, axis=0, keepdims=True)


def to_column(row, count, first=0):
    shape = (count, 128)
    spread = jnp.where(iota(shape, 1) == iota(shape, 0) + first, row, 0.0)
    return jnp.sum(spread, axis=1, keepdims=True)


def total(values):
    return jnp.sum(jnp.sum(values, axis=0, keepdims=True), axis=1, keepdims=True)


def shifts(tile, north, south, east, west):
    rows, cols = tile.shape
    sub, lane = (iota(tile.shape, 0), iota(tile.shape, 1))
    return (
        jnp.where(sub == rows - 1, north, pltpu.roll(tile, rows - 1, 0)),
        jnp.where(sub == 0, south, pltpu.roll(tile, 1, 0)),
        jnp.where(lane == cols - 1, east, pltpu.roll(tile, cols - 1, 1)),
        jnp.where(lane == 0, west, pltpu.roll(tile, 1, 1)),
    )


def project(basis_ref, field, acc_ref, columns, comps, rows):
    for k in range(columns):
        base = k * comps * rows
        acc = basis_ref[base : base + rows, :] * field[0]
        for c in range(1, comps):
            acc = acc + basis_ref[base + c * rows : base + (c + 1) * rows, :] * field[c]
        acc_ref[k * rows : (k + 1) * rows, :] = acc
    sums = acc_ref[pl.ds(0, columns, stride=rows), :]
    for s in range(1, rows):
        sums = sums + acc_ref[pl.ds(s, columns, stride=rows), :]
    return jnp.sum(sums, axis=1, keepdims=True)


def combine(basis_ref, wide_ref, columns, comps, rows):
    out = [[None, None] for _ in range(comps)]
    for k in range(columns):
        weight = jnp.broadcast_to(wide_ref[k : k + 1, :], (rows, 128))
        for c in range(comps):
            base = (k * comps + c) * rows
            term = weight * basis_ref[base : base + rows, :]
            old = out[c][k % 2]
            out[c][k % 2] = term if old is None else old + term
    return [a + b for a, b in out]


def pack_kernel(sizes, basis_ref, rhs_ref, mask_ref, visc_ref, gram_ref,
                send_ref, rowa_ref, rowb_ref, cola_ref, colb_ref, acc_ref):
    columns, comps, rows, cols = sizes
    packet_kernel(sizes, basis_ref, rhs_ref, mask_ref, visc_ref, rowa_ref, rowb_ref, cola_ref, colb_ref)
    rhs = [rhs_ref[c * rows : (c + 1) * rows, :] for c in range(comps)]
    visc = visc_ref[...]

    row = to_row(project(basis_ref, rhs, acc_ref, columns, comps, rows))
    lanes = iota((1, cols), 1)
    for i, corner in enumerate(corners_of(visc)):
        row = jnp.where(lanes == columns + i, corner, row)
    both = jnp.concatenate([row, gram_ref[...]], axis=0)
    send_ref[...] = jnp.broadcast_to(both[None], send_ref.shape)


def open_kernel(out_ref):
    out_ref[...] = jnp.zeros_like(out_ref)


def rows_kernel(sizes, basis_ref, rhs_ref, mask_ref, visc_ref, first_ref, rowa_ref, rowb_ref):
    packet_kernel(sizes, basis_ref, rhs_ref, mask_ref, visc_ref, rowa_ref, rowb_ref, None, None)


def sides_kernel(sizes, basis_ref, rhs_ref, mask_ref, visc_ref, cola_ref, colb_ref):
    packet_kernel(sizes, basis_ref, rhs_ref, mask_ref, visc_ref, None, None, cola_ref, colb_ref)


def corners_of(visc):
    top, low = (visc.shape[0] - 1, visc.shape[1] - 1)
    return [visc[i : i + 1, j : j + 1] for i in (0, top) for j in (0, low)]


def packet_kernel(sizes, basis_ref, rhs_ref, mask_ref, visc_ref,
                  rowa_ref, rowb_ref, cola_ref, colb_ref):
    columns, comps, rows, cols = sizes
    even_row = 1 - lax.rem(lax.axis_index("row"), 2)
    even_col = 1 - lax.rem(lax.axis_index("col"), 2)
    rhs = [rhs_ref[c * rows : (c + 1) * rows, :] for c in range(comps)]
    mask = [mask_ref[c * rows : (c + 1) * rows, :].astype(F32) for c in range(comps)]
    visc = visc_ref[...]
    lane = iota((rows, cols), 1)
    top, low = rows - 1, cols - 1

    if rowa_ref is not None:
        for c in range(comps):
            north = basis_ref[pl.ds(c * rows + top, columns, stride=comps * rows), :]
            south = basis_ref[pl.ds(c * rows, columns, stride=comps * rows), :]
            north = north * mask[c][top : top + 1, :]
            south = south * mask[c][0:1, :]
            rowa_ref[c * columns : (c + 1) * columns, :] = pick(even_row, north, south)
            rowb_ref[c * columns : (c + 1) * columns, :] = pick(even_row, south, north)
        north = [mask[c][top : top + 1, :] * rhs[c][top : top + 1, :] for c in range(comps)]
        south = [mask[c][0:1, :] * rhs[c][0:1, :] for c in range(comps)]
        north += [visc[top : top + 1, :], visc[top - 1 : top, :]]
        south += [visc[0:1, :], visc[1:2, :]]
        for i in range(comps + 2):
            at = comps * columns + i
            rowa_ref[at : at + 1, :] = pick(even_row, north[i], south[i])
            rowb_ref[at : at + 1, :] = pick(even_row, south[i], north[i])
        rest = comps * columns + comps + 2
        blank = jnp.zeros((rowa_ref.shape[0] - rest, cols), F32)
        rowa_ref[rest:, :] = blank
        rowb_ref[rest:, :] = blank
    if cola_ref is None:
        return

    for c in range(comps):
        east, west = (jnp.zeros((rows, cols), F32), jnp.zeros((rows, cols), F32))
        for k in range(columns):
            base = (k * comps + c) * rows
            tile = basis_ref[base : base + rows, :]
            east = jnp.where(lane == k, pltpu.roll(tile, (k - low) % cols, 1), east)
            west = jnp.where(lane == k, tile if k == 0 else pltpu.roll(tile, k, 1), west)
        east = jnp.where(lane == columns, rhs[c][:, low : low + 1], east)
        west = jnp.where(lane == columns, rhs[c][:, 0:1], west)
        east = east * mask[c][:, low : low + 1]
        west = west * mask[c][:, 0:1]
        cola_ref[c * rows : (c + 1) * rows, :] = pick(even_col, east, west)
        colb_ref[c * rows : (c + 1) * rows, :] = pick(even_col, west, east)
    east = jnp.where(lane == 0, visc[:, low : low + 1], visc[:, low - 1 : low])
    west = jnp.where(lane == 0, visc[:, 0:1], visc[:, 1:2])
    cola_ref[comps * rows :, :] = pick(even_col, east, west)
    colb_ref[comps * rows :, :] = pick(even_col, west, east)


def stencil(mask, faces, diagonal, tile, halo):
    masked = mask * tile
    near = shifts(masked, *halo)
    inner = diagonal * masked - (
        faces[0] * near[0] + faces[1] * near[1] + faces[2] * near[2] + faces[3] * near[3]
    )
    return mask * inner + (1.0 - mask) * tile


def split(values):
    high = values.astype(jnp.bfloat16)
    return jnp.concatenate([high, (values - high.astype(F32)).astype(jnp.bfloat16)], axis=0)


def product(lefts, rights):
    return lax.dot_general(
        jnp.concatenate([split(value) for value in lefts], axis=1),
        jnp.concatenate([split(value) for value in rights], axis=1),
        (((1,), (1,)), ((), ())),
        preferred_element_type=F32,
    )


def merge(blocks, columns):
    blocks = blocks + pltpu.roll(blocks, columns, 1)
    return blocks[:columns] + blocks[columns:]


def local_kernel(sizes, basis_ref, rhs_ref, mask_ref, visc_ref, inner_ref, dots_ref, acc_ref):
    columns, comps, rows, cols = sizes
    _, has_south, _, has_west = flags()
    top, low = (rows - 1, cols - 1)
    rhs = [rhs_ref[c * rows : (c + 1) * rows, :] for c in range(comps)]
    mask = [mask_ref[c * rows : (c + 1) * rows, :].astype(F32) for c in range(comps)]
    visc = visc_ref[...]
    sub, lane = (iota((rows, cols), 0), iota((rows, cols), 1))
    empty = (jnp.zeros((1, cols), F32),) * 2 + (jnp.zeros((rows, 1), F32),) * 2
    faces = [0.5 * (visc + v) for v in shifts(visc, *empty)]
    faces[0] = jnp.where(sub == top, 0.0, faces[0])
    faces[1] = jnp.where(sub == 0, faces[1] * (1.0 - has_south), faces[1])
    faces[2] = jnp.where(lane == low, 0.0, faces[2])
    faces[3] = jnp.where(lane == 0, faces[3] * (1.0 - has_west), faces[3])
    diagonal = 1.0 + faces[0] + faces[1] + faces[2] + faces[3]

    blocks = jnp.zeros((2 * columns, 2 * columns), F32)
    for c in range(comps):
        m = mask[c]
        own = m * diagonal + (1.0 - m)
        up, down = (m * faces[0], m * faces[1])
        right = m * faces[2]
        left = jnp.where(lane == 0, 0.0, m * faces[3])
        plain = [
            basis_ref[pl.ds(c * rows + i, columns, stride=comps * rows), :] for i in range(rows)
        ]
        free = [plain[i] * m[i : i + 1, :] for i in range(rows)]
        images = []
        for i in range(rows):
            here = slice(i, i + 1)
            value = own[here] * plain[i] - right[here] * pltpu.roll(free[i], low, 1)
            value = value - left[here] * pltpu.roll(free[i], 1, 1)
            if i < top:
                value = value - up[here] * free[i + 1]
            if i > 0:
                value = value - down[here] * free[i - 1]
            images.append(value)
        for i in range(0, rows, 2):
            blocks = blocks + product(plain[i : i + 2], images[i : i + 2])
    inner_ref[...] = merge(blocks, columns)
    dots = to_row(project(basis_ref, rhs, acc_ref, columns, comps, rows))
    dots_ref[...] = jnp.broadcast_to(dots, dots_ref.shape)


def border_kernel(sizes, inner_ref, dots_ref, basis_ref, mask_ref, visc_ref, gram_ref, rowa_ref,
                  rowb_ref, cola_ref, colb_ref, owna_ref, ownb_ref, send_ref, full_ref):
    columns, comps, rows, cols = sizes
    even_row = 1 - lax.rem(lax.axis_index("row"), 2)
    even_col = 1 - lax.rem(lax.axis_index("col"), 2)
    has_north, _, has_east, _ = flags()
    top, low, half = (rows - 1, cols - 1, cols // 2)
    field = comps * rows
    visc, lanes = (visc_ref[...], iota((1, cols), 1))
    at = comps * columns + comps
    v_north = pick(even_row, rowa_ref[at : at + 1, :], rowb_ref[at : at + 1, :]) * has_north
    east = pick(even_col, cola_ref[...], colb_ref[...]) * has_east
    own_east = pick(even_col, owna_ref[...], ownb_ref[...])
    north_face = 0.5 * (visc[top : top + 1, :] + v_north)
    east_face = 0.5 * (visc[:, low : low + 1] + east[field:, 0:1])
    tops = []
    for c in range(comps):
        span = slice(c * columns, (c + 1) * columns)
        own = basis_ref[pl.ds(c * rows + top, columns, stride=comps * rows), :]
        own = own * mask_ref[c * rows + top : c * rows + rows, :].astype(F32)
        tops.append(own - pick(even_row, rowa_ref[span, :], rowb_ref[span, :]) * has_north)
    full = inner_ref[...] + merge(product([value * north_face for value in tops], tops), columns)
    gap = own_east[:field] - east[:field]
    edge = lax.dot_general(
        gap * jnp.concatenate([east_face] * comps, axis=0), gap, (((0,), (0,)), ((), ())),
        preferred_element_type=F32, precision=lax.Precision.HIGHEST,
    )
    wide_lane = iota((columns, cols), 1)
    edge = jnp.where(wide_lane < half, edge[:columns], 0.0)
    full = full + edge + pltpu.roll(edge, half, 1)
    full_ref[...] = full
    spot = jnp.where(wide_lane >= half, wide_lane - half, wide_lane) == iota((columns, cols), 0)
    spine = jnp.sum(jnp.where(spot, full, 0.0), axis=0, keepdims=True)
    count = columns // 2
    chunk = jnp.where(
        iota((count, cols), 1) < half,
        full_ref[pl.ds(0, count, stride=2), :],
        full_ref[pl.ds(1, count, stride=2), :],
    )
    dots = dots_ref[0:1, :]
    corner_row = jnp.zeros((1, cols), F32)
    for i, corner in enumerate(corners_of(visc)):
        corner_row = jnp.where(lanes == i, corner, corner_row)
    at = 2 * lax.axis_index("row")
    piece = jnp.concatenate([gram_ref[pl.ds(at + t, 1), :] for t in range(2)], axis=1)
    head = jnp.concatenate([jnp.where(lanes < half, dots, spine), piece], axis=0)
    for d in range(count):
        send_ref[d] = jnp.concatenate([head, chunk[d : d + 1, :], corner_row], axis=0)


def first_kernel(sizes, whole_rows, two, got_ref, *refs):
    columns, comps, rows, cols, scale = sizes
    if whole_rows:
        gram_in_ref = None
    else:
        gram_in_ref, *refs = refs
    (basis_ref, rhs_ref, mask_ref, visc_ref, rowa_ref, rowb_ref, cola_ref, colb_ref,
     send_ref, state_ref, face_ref, small_ref, gram_ref, *refs) = refs
    edge_ref, side_ref = (None, None) if two else refs[:2]
    acc_ref, wide_ref = refs[-2:]
    at_row, at_col = (lax.axis_index("row"), lax.axis_index("col"))
    row_count, col_count = (lax.axis_size("row"), lax.axis_size("col"))
    even_row, even_col = (1 - lax.rem(at_row, 2), 1 - lax.rem(at_col, 2))
    me = at_row * col_count + at_col
    top, low = rows - 1, cols - 1
    rhs = [rhs_ref[c * rows : (c + 1) * rows, :] for c in range(comps)]
    mask = [mask_ref[c * rows : (c + 1) * rows, :].astype(F32) for c in range(comps)]
    visc = visc_ref[...]
    sub, lane = (iota((rows, cols), 0), iota((rows, cols), 1))
    lanes = iota((1, cols), 1)

    if whole_rows:
        per = cols // columns
        for r in range(row_count):
            for c in range(col_count):
                piece = got_ref[r * col_count + c, 1:2, :]
                for t in range(per):
                    at = (c * row_count + r) * per + t
                    moved = pltpu.roll(piece, cols - t * columns, 1) if t else piece
                    gram_ref[at : at + 1, :] = moved
    else:
        gram_ref[:, :columns] = gram_in_ref[...]
    all_sums = jnp.sum(got_ref[...], axis=0)
    sums = all_sums[0:1, :]
    dots = jnp.where(lanes < columns, sums, 0.0)
    gram = jnp.where(iota((columns, cols), 1) < columns, gram_ref[...], 0.0)
    coeffs = jnp.sum(gram * dots, axis=1, keepdims=True) * scale
    wide = jnp.broadcast_to(coeffs, (columns, cols))
    wide_ref[...] = wide
    coeff_row = to_row(coeffs)

    extra = comps * columns
    tail_a, tail_b = (rowa_ref[extra:, :], rowb_ref[extra:, :])
    has_north, has_south, has_east, has_west = flags()
    north_tail = pick(even_row, tail_a, tail_b) * has_north
    south_tail = pick(even_row, tail_b, tail_a) * has_south
    side_a, side_b = (cola_ref[...], colb_ref[...])
    east_side = pick(even_col, side_a, side_b) * has_east
    west_side = pick(even_col, side_b, side_a) * has_west
    v_north, v_south = (north_tail[comps : comps + 1, :], south_tail[comps : comps + 1, :])
    v_north2, v_south2 = (north_tail[comps + 1 : comps + 2, :], south_tail[comps + 1 : comps + 2, :])
    v_east, v_west = (east_side[comps * rows :, 0:1], west_side[comps * rows :, 0:1])
    v_east2, v_west2 = (east_side[comps * rows :, 1:2], west_side[comps * rows :, 1:2])
    faces = [0.5 * (visc + v) for v in shifts(visc, v_north, v_south, v_east, v_west)]
    diagonal = 1.0 + faces[0] + faces[1] + faces[2] + faces[3]
    face_ref[...] = jnp.concatenate(faces + [diagonal], axis=0)
    jacobi = [m / diagonal + (1.0 - m) for m in mask]

    def corner(step_row, step_col, which):
        r, c = (at_row + step_row, at_col + step_col)
        inside = (r >= 0) & (r < row_count) & (c >= 0) & (c < col_count)
        place = jnp.where(inside, r * col_count + c, me)
        line, first = (3, 0) if two else (0, columns)
        value = got_ref[place, line : line + 1, :]
        value = jnp.sum(jnp.where(lanes == first + which, value, 0.0), axis=1, keepdims=True)
        return value * jnp.where(inside, 1.0, 0.0)

    north_west, north_east = (corner(1, -1, 1), corner(1, 1, 0))
    south_west, south_east = (corner(-1, -1, 3), corner(-1, 1, 2))

    def row_inverse(own, inner, outer, west, east):
        right = jnp.where(lanes == low, east, pltpu.roll(own, low, 1))
        left = jnp.where(lanes == 0, west, pltpu.roll(own, 1, 1))
        return 1.0 / (1.0 + 0.5 * (4.0 * own + inner + outer + left + right))

    def side_inverse(own, inner, outer, south, north):
        own = jnp.broadcast_to(own, (rows, cols))
        up = jnp.where(sub == top, north, pltpu.roll(own, top, 0))
        down = jnp.where(sub == 0, south, pltpu.roll(own, 1, 0))
        return 1.0 / (1.0 + 0.5 * (4.0 * own + inner + outer + up + down))

    inv_north = row_inverse(v_north, visc[top : top + 1, :], v_north2, north_west, north_east)
    inv_south = row_inverse(v_south, visc[0:1, :], v_south2, south_west, south_east)
    inv_east = side_inverse(v_east, visc[:, low : low + 1], v_east2, south_east, north_east)
    inv_west = side_inverse(v_west, visc[:, 0:1], v_west2, south_west, north_west)

    corr = combine(basis_ref, wide_ref, columns, comps, rows)
    image, scaled, smooth, point = ([], [], [], [])
    scaled_image = []
    none = (jnp.zeros((1, cols), F32),) * 2 + (jnp.zeros((rows, 1), F32),) * 2
    for c in range(comps):
        span = slice(c * columns, (c + 1) * columns)
        sum_a = jnp.sum(wide * rowa_ref[span, :], axis=0, keepdims=True)
        sum_b = jnp.sum(wide * rowb_ref[span, :], axis=0, keepdims=True)
        u_north = inv_north * north_tail[c : c + 1, :]
        u_south = inv_south * south_tail[c : c + 1, :]
        p_north = u_north + has_north * pick(even_row, sum_a, sum_b)
        p_south = u_south + has_south * pick(even_row, sum_b, sum_a)
        here = slice(c * rows, (c + 1) * rows)
        east, west = (east_side[here, :], west_side[here, :])
        u_east = inv_east * east[:, columns : columns + 1]
        u_west = inv_west * west[:, columns : columns + 1]
        p_east = u_east + jnp.sum(coeff_row * east, axis=1, keepdims=True)
        p_west = u_west + jnp.sum(coeff_row * west, axis=1, keepdims=True)
        u = jacobi[c] * rhs[c]
        p = u + corr[c]
        q = stencil(mask[c], faces, diagonal, p, (p_north, p_south, p_east, p_west))
        if two:
            scaled_image.append(stencil(mask[c], faces, diagonal, jacobi[c] * q, none))
        smooth.append(u)
        point.append(p)
        image.append(q)
        scaled.append(jacobi[c] * q)
        if two:
            continue
        for i, value in enumerate((u_north, u_south, p_north, p_south)):
            edge_ref[i * 8 + c : i * 8 + c + 1, :] = value
        for i, value in enumerate((u_east, u_west, p_east, p_west)):
            side_ref[(i * comps + c) * rows : (i * comps + c + 1) * rows, :] = value
    fields = point + image + scaled
    state_ref[...] = jnp.concatenate(fields if two else smooth + fields, axis=0)

    row = to_row(project(basis_ref, image, acc_ref, columns, comps, rows))
    pairs = ((point, image), (smooth, image), (image, scaled), (rhs, smooth))
    if two:
        pairs += ((scaled, scaled_image),)
    for i, (left, right) in enumerate(pairs):
        value = left[0] * right[0]
        for c in range(1, comps):
            value = value + left[c] * right[c]
        row = jnp.where(lanes == (DOTS2 if two else DOTS) + i, total(value), row)
    masked = [mask[c] * scaled[c] for c in range(comps)]
    if two:
        norths = [m[top : top + 1, :] * faces[0][top : top + 1, :] * has_north for m in masked]
        easts = [m[:, low : low + 1] * faces[2][:, low : low + 1] * has_east for m in masked]
        souths, wests = ([m[0:1, :] for m in masked], [m[:, 0:1] for m in masked])
        row = row + to_row(jnp.concatenate(easts, axis=0), EAST2)
        row = row + to_row(jnp.concatenate(wests, axis=0), WEST2)
        reach = project(basis_ref, scaled_image, acc_ref, columns, comps, rows)
        beyond = jnp.zeros((columns, cols), F32)
        aside = jnp.zeros((rows, cols), F32)
        for c in range(comps):
            span, here = (slice(c * columns, (c + 1) * columns), slice(c * rows, (c + 1) * rows))
            halo_a, halo_b = (rowa_ref[span, :], rowb_ref[span, :])
            low_side = souths[c] * faces[1][0:1, :] * has_south
            beyond = beyond + norths[c] * pick(even_row, halo_a, halo_b)
            beyond = beyond + low_side * pick(even_row, halo_b, halo_a)
            aside = aside + easts[c] * east_side[here, :]
            aside = aside + wests[c] * faces[3][:, 0:1] * west_side[here, :]
        reach = to_row(reach - jnp.sum(beyond, axis=1, keepdims=True))
        reach = reach - jnp.where(lanes < columns, jnp.sum(aside, axis=0, keepdims=True), 0.0)
        half = cols // 2
        ours = jnp.broadcast_to(all_sums[2:3, :], (8, cols))
        other = pltpu.roll(ours, half, 1)
        wide_lane = iota((8, cols), 1)
        for t, (first, second) in enumerate(((ours, other), (other, ours))):
            value = jnp.where(wide_lane < half, first, second)
            turn = lax.rem(half + t * (half // 2) - (2 * me + t + 1) + 2 * cols, cols)
            value = pltpu.roll(value, turn, 1)[0:1, :]
            start = half + t * (half // 2)
            reach = jnp.where((lanes >= start) & (lanes < start + half // 2), value, reach)
        message = jnp.concatenate(norths + souths + [row, reach], axis=0)
        send_ref[...] = jnp.broadcast_to(message[None], send_ref.shape)
        spine = pltpu.roll(jnp.broadcast_to(sums, (8, cols)), half, 1)[0:1, :]
        spine = jnp.where(lanes < half, spine, 0.0)
        small_ref[...] = jnp.concatenate([dots, coeff_row, spine, jnp.zeros((5, cols), F32)], axis=0)
        return
    east = jnp.concatenate([m[:, low : low + 1] for m in masked], axis=0)
    west = jnp.concatenate([m[:, 0:1] for m in masked], axis=0)
    row = row + to_row(east, EAST) + to_row(west, WEST)
    message = jnp.concatenate([row] + [m[top : top + 1, :] for m in masked], axis=0)
    send_ref[...] = jnp.broadcast_to(message[None], send_ref.shape)
    message = jnp.concatenate([row] + [m[0:1, :] for m in masked], axis=0)
    send_ref[jnp.where(at_row > 0, me - col_count, me)] = message
    small_ref[...] = jnp.concatenate([dots, coeff_row, jnp.zeros((6, cols), F32)], axis=0)


def second_kernel(sizes, got_ref, basis_ref, rhs_ref, mask_ref, rowa_ref, rowb_ref, cola_ref,
                  colb_ref, state_ref, face_ref, small_ref, gram_ref, edge_ref, side_ref,
                  send_ref, out_ref, last_ref, wide_ref):
    columns, comps, rows, cols, scale = sizes
    at_row, at_col = (lax.axis_index("row"), lax.axis_index("col"))
    row_count, col_count = (lax.axis_size("row"), lax.axis_size("col"))
    even_row, even_col = (1 - lax.rem(at_row, 2), 1 - lax.rem(at_col, 2))
    me = at_row * col_count + at_col
    lanes = iota((1, cols), 1)
    mask = [mask_ref[c * rows : (c + 1) * rows, :].astype(F32) for c in range(comps)]

    sums = jnp.sum(got_ref[...], axis=0)[0:1, :]
    image_dots = jnp.where(lanes < columns, sums, 0.0)
    curve, cross, image_sq, rhs_sq = [
        jnp.sum(jnp.where(lanes == DOTS + i, sums, 0.0), axis=1, keepdims=True) for i in range(4)
    ]
    dots, coeff_row = (small_ref[0:1, :], small_ref[1:2, :])
    energy = rhs_sq + jnp.sum(dots * coeff_row, axis=1, keepdims=True)
    step = energy / curve
    gram = jnp.where(iota((columns, cols), 1) < columns, gram_ref[...], 0.0)
    dots = dots - step * image_dots
    coeffs = jnp.sum(gram * dots, axis=1, keepdims=True) * scale
    wide = jnp.broadcast_to(coeffs, (columns, cols))
    wide_ref[...] = wide
    coeff_row = to_row(coeffs)
    energy_new = rhs_sq - 2.0 * step * cross + step * step * image_sq
    energy_new = energy_new + jnp.sum(dots * coeff_row, axis=1, keepdims=True)
    ratio = energy_new / energy

    def beside(step_row, step_col):
        r, c = (at_row + step_row, at_col + step_col)
        inside = (r >= 0) & (r < row_count) & (c >= 0) & (c < col_count)
        message = got_ref[jnp.where(inside, r * col_count + c, me)]
        return message * jnp.where(inside, 1.0, 0.0)

    q_north, q_south = (beside(1, 0), beside(-1, 0))
    q_east = to_column(beside(0, 1)[0:1, :], comps * rows, WEST)
    q_west = to_column(beside(0, -1)[0:1, :], comps * rows, EAST)

    side_a, side_b = (cola_ref[...], colb_ref[...])
    has_north, has_south, has_east, has_west = flags()
    east_side = pick(even_col, side_a, side_b) * has_east
    west_side = pick(even_col, side_b, side_a) * has_west
    faces = [face_ref[i * rows : (i + 1) * rows, :] for i in range(4)]
    diagonal = face_ref[4 * rows : 5 * rows, :]
    corr = combine(basis_ref, wide_ref, columns, comps, rows)
    curve_part = jnp.zeros((rows, cols), F32)
    first, second, third, fourth = ([], [], [], [])
    for c in range(comps):
        span = slice(c * columns, (c + 1) * columns)
        here = slice(c * rows, (c + 1) * rows)
        sum_a = jnp.sum(wide * rowa_ref[span, :], axis=0, keepdims=True)
        sum_b = jnp.sum(wide * rowb_ref[span, :], axis=0, keepdims=True)
        old = [edge_ref[i * 8 + c : i * 8 + c + 1, :] for i in range(4)]
        p_north = old[0] - step * q_north[1 + c : 2 + c, :] + has_north * pick(even_row, sum_a, sum_b)
        p_south = old[1] - step * q_south[1 + c : 2 + c, :] + has_south * pick(even_row, sum_b, sum_a)
        p_north, p_south = (p_north + ratio * old[2], p_south + ratio * old[3])
        old = [side_ref[(i * comps + c) * rows : (i * comps + c + 1) * rows, :] for i in range(4)]
        p_east = old[0] - step * q_east[here] + ratio * old[2]
        p_west = old[1] - step * q_west[here] + ratio * old[3]
        p_east = p_east + jnp.sum(coeff_row * east_side[here, :], axis=1, keepdims=True)
        p_west = p_west + jnp.sum(coeff_row * west_side[here, :], axis=1, keepdims=True)
        u, p, q, jq = [
            state_ref[(i * comps + c) * rows : (i * comps + c + 1) * rows, :] for i in range(4)
        ]
        new = u - step * jq + corr[c] + ratio * p
        masked = mask[c] * new
        near = shifts(masked, p_north, p_south, p_east, p_west)
        stencil = diagonal * masked - (
            faces[0] * near[0] + faces[1] * near[1] + faces[2] * near[2] + faces[3] * near[3]
        )
        applied = mask[c] * stencil + (1.0 - mask[c]) * new
        curve_part = curve_part + new * applied
        first.append(step * p)
        second.append(new)
        third.append(rhs_ref[here, :] - step * q)
        fourth.append(applied)
    out_ref[...] = jnp.concatenate(first + second + third + fourth, axis=0)
    last_ref[...] = jnp.broadcast_to(energy_new, last_ref.shape)
    send_ref[...] = jnp.broadcast_to(total(curve_part)[None], send_ref.shape)


def close_kernel(sizes, got_ref, basis_ref, rhs_ref, mask_ref, rowa_ref, rowb_ref, cola_ref,
                 colb_ref, state_ref, face_ref, small_ref, gram_ref,
                 solution_ref, residual_ref, wide_ref):
    columns, comps, rows, cols, scale = sizes
    at_row, at_col = (lax.axis_index("row"), lax.axis_index("col"))
    row_count, col_count = (lax.axis_size("row"), lax.axis_size("col"))
    devices = row_count * col_count
    even_row, even_col = (1 - lax.rem(at_row, 2), 1 - lax.rem(at_col, 2))
    has_north, has_south, has_east, has_west = flags()
    me = at_row * col_count + at_col
    half, quarter = (cols // 2, cols // 4)
    lanes = iota((1, cols), 1)
    mask = [mask_ref[c * rows : (c + 1) * rows, :].astype(F32) for c in range(comps)]

    def along(left, right):
        return jnp.sum(left * right, axis=1, keepdims=True)

    sums = jnp.sum(got_ref[...], axis=0)
    line = sums[2 * comps : 2 * comps + 1, :]
    image_dots = jnp.where(lanes < columns, line, 0.0)
    reach_dots = jnp.where(lanes < columns, sums[2 * comps + 1 :, :], 0.0)
    gram = jnp.where(iota((columns, cols), 1) < columns, gram_ref[...], 0.0)
    turn = jnp.sum(gram * image_dots, axis=1, keepdims=True) * scale
    wide = jnp.broadcast_to(turn, (columns, cols))
    wide_ref[...] = wide
    turn_row = to_row(turn)

    def beside(step_row, step_col):
        r, c = (at_row + step_row, at_col + step_col)
        inside = (r >= 0) & (r < row_count) & (c >= 0) & (c < col_count)
        message = got_ref[jnp.where(inside, r * col_count + c, me)]
        return message * jnp.where(inside, 1.0, 0.0)

    faces = [face_ref[i * rows : (i + 1) * rows, :] for i in range(4)]
    diagonal = face_ref[4 * rows : 5 * rows, :]
    q_north, q_south = (beside(1, 0), beside(-1, 0))
    q_east = to_column(beside(0, 1)[2 * comps : 2 * comps + 1, :], comps * rows, WEST2)
    q_west = to_column(beside(0, -1)[2 * comps : 2 * comps + 1, :], comps * rows, EAST2)
    side_a, side_b = (cola_ref[...], colb_ref[...])
    east_side = pick(even_col, side_a, side_b) * has_east
    west_side = pick(even_col, side_b, side_a) * has_west
    corr = combine(basis_ref, wide_ref, columns, comps, rows)
    moved, moved_image = ([], [])
    for c in range(comps):
        span = slice(c * columns, (c + 1) * columns)
        here = slice(c * rows, (c + 1) * rows)
        sum_a = jnp.sum(wide * rowa_ref[span, :], axis=0, keepdims=True)
        sum_b = jnp.sum(wide * rowb_ref[span, :], axis=0, keepdims=True)
        north = q_north[comps + c : comps + c + 1, :] + has_north * pick(even_row, sum_a, sum_b)
        south = q_south[c : c + 1, :] / faces[1][0:1, :] + has_south * pick(even_row, sum_b, sum_a)
        east = q_east[here] + along(turn_row, east_side[here, :])
        west = q_west[here] / faces[3][:, 0:1] + along(turn_row, west_side[here, :])
        at = (2 * comps + c) * rows
        value = state_ref[at : at + rows, :] + corr[c]
        moved.append(value)
        moved_image.append(stencil(mask[c], faces, diagonal, value, (north, south, east, west)))

    border = jnp.zeros((2 * comps + 2, cols), F32)
    for d in range(devices - col_count):
        border = border + got_ref[d] * pltpu.roll(got_ref[d + col_count], comps + 2, 0)
    border = jnp.where(iota(border.shape, 0) < comps, border, 0.0)
    lines = got_ref[:, 2 * comps, :]
    later = pltpu.roll(pltpu.roll(lines, devices - 1, 0), cols - (WEST2 - EAST2), 1)
    line_lane = iota(lines.shape, 1)
    beside_it = jnp.where((line_lane >= EAST2) & (line_lane < WEST2), lines * later, 0.0)
    across = jnp.sum(border, axis=0, keepdims=True) + jnp.sum(beside_it, axis=0, keepdims=True)

    packed = pltpu.roll(got_ref[:, 2 * comps + 1, :], half, 1)
    sub = iota(packed.shape, 0)
    value = jnp.broadcast_to(turn_row, (8, cols))
    value = jnp.broadcast_to((value + pltpu.roll(value, half, 1))[0:1, :], packed.shape)
    bit = 1
    while bit < devices:
        value = jnp.where((sub & bit) != 0, pltpu.roll(value, cols - 2 * bit, 1), value)
        bit *= 2
    ahead = pltpu.roll(value, cols - 1, 1)
    ahead = jnp.where(line_lane < quarter, ahead, pltpu.roll(value, quarter - 2, 1))
    own = jnp.where(line_lane < quarter, value[:, 0:1], value[:, 1:2])
    weight = jnp.where((line_lane == quarter - 1) | (line_lane == half - 1), 1.0, 2.0)
    form = jnp.where(line_lane < half, packed * weight * own * ahead, 0.0)
    form = jnp.sum(form, axis=0, keepdims=True)

    curve, cross, image_sq, rhs_sq, scaled_sq = [
        along(jnp.where(lanes == DOTS2 + i, 1.0, 0.0), line) for i in range(5)
    ]
    dots, old_row, spine = (small_ref[0:1, :], small_ref[1:2, :], small_ref[2:3, :])
    energy = rhs_sq + along(dots, old_row)
    meet = image_sq + along(turn_row, image_dots)
    rest = form + spine * turn_row * turn_row + 2.0 * turn_row * reach_dots - 2.0 * across
    moved_sq = scaled_sq + jnp.sum(rest, axis=1, keepdims=True)
    step = energy / curve
    energy_new = rhs_sq - 2.0 * step * cross + step * step * image_sq
    energy_new = energy_new + along(dots - step * image_dots, old_row - step * turn_row)
    grow = 1.0 + energy_new / energy
    curve_new = grow * grow * curve - 2.0 * step * grow * meet + step * step * moved_sq
    step_new = energy_new / curve_new
    near, far = (step + step_new * grow, step_new * step)
    for c in range(comps):
        here = slice(c * rows, (c + 1) * rows)
        p = state_ref[here, :]
        q = state_ref[(comps + c) * rows : (comps + c + 1) * rows, :]
        solution_ref[here, :] = near * p - far * moved[c]
        residual_ref[here, :] = rhs_ref[here, :] - near * q + far * moved_image[c]


def last_kernel(count, got_ref, in_ref, last_ref, solution_ref, residual_ref):
    step = last_ref[0:1, :] / jnp.sum(got_ref[...], axis=0)
    solution_ref[...] = in_ref[:count, :] + step * in_ref[count : 2 * count, :]
    residual_ref[...] = in_ref[2 * count : 3 * count, :] - step * in_ref[3 * count :, :]


def on_device(right_side, viscosity, free_mask, coarse_basis, gram_inverse):
    comps, rows, cols = right_side.shape
    columns = coarse_basis.shape[0]
    row_count, col_count = (lax.axis_size("row"), lax.axis_size("col"))
    devices = row_count * col_count
    scale = 1.0 / (32.0 * math.sqrt(float(comps * rows * cols * devices * columns)))
    sizes = (columns, comps, rows, cols)

    def call(kernel, outs, scratch, *args, flops=None):
        cost = flops and pl.CostEstimate(flops=flops, bytes_accessed=4096, transcendentals=0)
        return pl.pallas_call(
            kernel,
            out_shape=[jax.ShapeDtypeStruct(s, F32) for s in outs],
            in_specs=[VMEM] * len(args),
            out_specs=[VMEM] * len(outs),
            scratch_shapes=[pltpu.VMEM(s, F32) for s in scratch],
            cost_estimate=cost,
            compiler_params=pltpu.CompilerParams(vmem_limit_bytes=16 * 1024 * 1024),
        )(*args)

    def share(message):
        return lax.all_to_all(message, ("row", "col"), 0, 0, tiled=True)

    def swap(packet, axis, first):
        pairs = []
        for r in range(row_count):
            for c in range(col_count):
                along, across = ((r, c) if axis == "row" else (c, r))
                length, width = (row_count, col_count)[:: 1 if axis == "row" else -1]
                other = along + 1 if (along - first) % 2 == 0 else along - 1
                if 0 <= other < length:
                    mate = (other, across)
                else:
                    mate = (along, across ^ 1 if (across ^ 1) < width else across)
                r2, c2 = mate if axis == "row" else mate[::-1]
                pairs.append((r * col_count + c, r2 * col_count + c2))
        return lax.ppermute(packet, ("row", "col"), pairs)

    basis = coarse_basis.reshape(columns * comps * rows, cols)
    rhs = right_side.reshape(comps * rows, cols)
    mask = free_mask.reshape(comps * rows, cols)

    block = gram_inverse.size
    piece = -(-block // row_count)
    two = columns * columns == devices * cols and cols == 2 * columns and rows == 8 and comps == 3
    if two:
        (first,) = call(open_kernel, [(8, cols)], [], flops=10**9)
        own = gram_inverse
    else:
        flat = jnp.pad(gram_inverse.reshape(-1), (0, piece * row_count - block))
        own = lax.dynamic_slice_in_dim(flat, lax.axis_index("row") * piece, piece)
        own = jnp.pad(own, (0, cols - piece)).reshape(1, cols)

    tall = -(-(comps * columns + comps + 2) // 8) * 8
    wide = (comps + 1) * rows
    field = comps * rows
    if two:
        row_a, row_b = call(
            functools.partial(rows_kernel, sizes),
            [(tall, cols), (tall, cols)],
            [],
            basis, rhs, mask, viscosity, first,
        )
        col_a, col_b = call(
            functools.partial(sides_kernel, sizes),
            [(wide, cols), (wide, cols)],
            [],
            basis, rhs, mask, viscosity,
        )
        packets = ((row_a, "row", 0), (row_b, "row", 1), (col_a, "col", 0), (col_b, "col", 1))
        halos = []
        for packet in packets:
            halos.append(swap(*packet))
        inner, dots = call(
            functools.partial(local_kernel, sizes),
            [(columns, cols), (8, cols)],
            [(columns * rows, cols)],
            basis, rhs, mask, viscosity, flops=10**8,
        )
        (send,) = call(
            functools.partial(border_kernel, sizes),
            [(devices, 4, cols)],
            [(columns, cols)],
            inner, dots, basis, mask, viscosity, own, *halos, col_a, col_b,
        )
        sizes = sizes + (scale,)
        send, *state = call(
            functools.partial(first_kernel, sizes, True, True),
            [(devices, 8, cols), (3 * field, cols), (5 * rows, cols), (8, cols), (columns, cols)],
            [(columns * rows, cols), (columns, cols)],
            share(send), basis, rhs, mask, viscosity, *halos,
        )
        solution, residual = call(
            functools.partial(close_kernel, sizes),
            [(field, cols), (field, cols)],
            [(columns, cols)],
            share(send), basis, rhs, mask, *halos, *state,
        )
        return (solution.reshape(right_side.shape), residual.reshape(right_side.shape))
    send, row_a, row_b, col_a, col_b = call(
        functools.partial(pack_kernel, sizes),
        [(devices, 2, cols), (tall, cols), (tall, cols), (wide, cols), (wide, cols)],
        [(columns * rows, cols)],
        basis, rhs, mask, viscosity, own,
    )
    halos = (swap(row_a, "row", 0), swap(row_b, "row", 1), swap(col_a, "col", 0), swap(col_b, "col", 1))
    got = share(send)
    whole_rows = piece == cols and cols % columns == 0 and block == piece * row_count
    gram = ()
    if not whole_rows:
        gram = got[:, 1, :piece].reshape(row_count, col_count, piece).transpose(1, 0, 2)
        gram = gram.reshape(col_count, row_count * piece)[:, :block].reshape(columns, columns)
        gram = (gram,)
    sizes = sizes + (scale,)
    send, *state = call(
        functools.partial(first_kernel, sizes, whole_rows, False),
        [(devices, 1 + comps, cols), (4 * field, cols), (5 * rows, cols), (8, cols),
         (columns, cols), (32, cols), (4 * field, cols)],
        [(columns * rows, cols), (columns, cols)],
        got, *gram, basis, rhs, mask, viscosity, *halos,
    )
    send, fields, last = call(
        functools.partial(second_kernel, sizes),
        [(devices, 1, cols), (4 * field, cols), (8, cols)],
        [(columns, cols)],
        share(send), basis, rhs, mask, *halos, *state,
    )
    solution, residual = call(
        functools.partial(last_kernel, field),
        [(field, cols), (field, cols)],
        [],
        share(send), fields, last,
    )
    return (solution.reshape(right_side.shape), residual.reshape(right_side.shape))


def solution(mesh):
    in_specs = (
        P(None, "row", "col"),
        P("row", "col"),
        P(None, "row", "col"),
        P(None, None, "row", "col"),
        P("col", None),
    )
    out_specs = (P(None, "row", "col"), P(None, "row", "col"))
    return jax.shard_map(
        on_device, mesh=mesh, in_specs=in_specs, out_specs=out_specs, check_vma=False
    )
```

```python
import functools
import math

import jax
import jax.numpy as jnp
from jax import lax
from jax.experimental import pallas as pl
from jax.experimental.pallas import tpu as pltpu
from jax.sharding import PartitionSpec as P


F32 = jnp.float32
VMEM = pl.BlockSpec(memory_space=pltpu.VMEM)
DOTS, EAST, WEST = 64, 72, 96
EAST2, WEST2, DOTS2 = 64, 88, 112


def flags():
    at_row, at_col = (lax.axis_index("row"), lax.axis_index("col"))
    tests = (
        at_row < lax.axis_size("row") - 1,
        at_row > 0,
        at_col < lax.axis_size("col") - 1,
        at_col > 0,
    )
    return [jnp.where(test, 1.0, 0.0) for test in tests]


def iota(shape, dim):
    return lax.broadcasted_iota(jnp.int32, shape, dim)


def pick(flag, yes, no):
    return jnp.where(jnp.full(yes.shape, flag, jnp.int32) == 1, yes, no)


def to_row(column, first=0):
    shape = (column.shape[0], 128)
    spread = jnp.where(iota(shape, 1) == iota(shape, 0) + first, column, 0.0)
    return jnp.sum(spread, axis=0, keepdims=True)


def to_column(row, count, first=0):
    shape = (count, 128)
    spread = jnp.where(iota(shape, 1) == iota(shape, 0) + first, row, 0.0)
    return jnp.sum(spread, axis=1, keepdims=True)


def total(values):
    return jnp.sum(jnp.sum(values, axis=0, keepdims=True), axis=1, keepdims=True)


def shifts(tile, north, south, east, west):
    rows, cols = tile.shape
    sub, lane = (iota(tile.shape, 0), iota(tile.shape, 1))
    return (
        jnp.where(sub == rows - 1, north, pltpu.roll(tile, rows - 1, 0)),
        jnp.where(sub == 0, south, pltpu.roll(tile, 1, 0)),
        jnp.where(lane == cols - 1, east, pltpu.roll(tile, cols - 1, 1)),
        jnp.where(lane == 0, west, pltpu.roll(tile, 1, 1)),
    )


def project(basis_ref, field, acc_ref, columns, comps, rows):
    for k in range(columns):
        base = k * comps * rows
        acc = basis_ref[base : base + rows, :] * field[0]
        for c in range(1, comps):
            acc = acc + basis_ref[base + c * rows : base + (c + 1) * rows, :] * field[c]
        acc_ref[k * rows : (k + 1) * rows, :] = acc
    sums = acc_ref[pl.ds(0, columns, stride=rows), :]
    for s in range(1, rows):
        sums = sums + acc_ref[pl.ds(s, columns, stride=rows), :]
    return jnp.sum(sums, axis=1, keepdims=True)


def combine(basis_ref, wide_ref, columns, comps, rows):
    out = [[None, None] for _ in range(comps)]
    for k in range(columns):
        weight = jnp.broadcast_to(wide_ref[k : k + 1, :], (rows, 128))
        for c in range(comps):
            base = (k * comps + c) * rows
            term = weight * basis_ref[base : base + rows, :]
            old = out[c][k % 2]
            out[c][k % 2] = term if old is None else old + term
    return [a + b for a, b in out]


def pack_kernel(sizes, basis_ref, rhs_ref, mask_ref, visc_ref, gram_ref,
                send_ref, rowa_ref, rowb_ref, cola_ref, colb_ref, acc_ref):
    columns, comps, rows, cols = sizes
    packet_kernel(sizes, basis_ref, rhs_ref, mask_ref, visc_ref, rowa_ref, rowb_ref, cola_ref, colb_ref)
    rhs = [rhs_ref[c * rows : (c + 1) * rows, :] for c in range(comps)]
    visc = visc_ref[...]

    row = to_row(project(basis_ref, rhs, acc_ref, columns, comps, rows))
    lanes = iota((1, cols), 1)
    for i, corner in enumerate(corners_of(visc)):
        row = jnp.where(lanes == columns + i, corner, row)
    both = jnp.concatenate([row, gram_ref[...]], axis=0)
    send_ref[...] = jnp.broadcast_to(both[None], send_ref.shape)


def open_kernel(out_ref):
    out_ref[...] = jnp.zeros_like(out_ref)


def rows_kernel(sizes, basis_ref, rhs_ref, mask_ref, visc_ref, first_ref, rowa_ref, rowb_ref):
    packet_kernel(sizes, basis_ref, rhs_ref, mask_ref, visc_ref, rowa_ref, rowb_ref, None, None)


def sides_kernel(sizes, basis_ref, rhs_ref, mask_ref, visc_ref, cola_ref, colb_ref):
    packet_kernel(sizes, basis_ref, rhs_ref, mask_ref, visc_ref, None, None, cola_ref, colb_ref)


def corners_of(visc):
    top, low = (visc.shape[0] - 1, visc.shape[1] - 1)
    return [visc[i : i + 1, j : j + 1] for i in (0, top) for j in (0, low)]


def packet_kernel(sizes, basis_ref, rhs_ref, mask_ref, visc_ref,
                  rowa_ref, rowb_ref, cola_ref, colb_ref):
    columns, comps, rows, cols = sizes
    even_row = 1 - lax.rem(lax.axis_index("row"), 2)
    even_col = 1 - lax.rem(lax.axis_index("col"), 2)
    rhs = [rhs_ref[c * rows : (c + 1) * rows, :] for c in range(comps)]
    mask = [mask_ref[c * rows : (c + 1) * rows, :].astype(F32) for c in range(comps)]
    visc = visc_ref[...]
    lane = iota((rows, cols), 1)
    top, low = rows - 1, cols - 1

    if rowa_ref is not None:
        for c in range(comps):
            north = basis_ref[pl.ds(c * rows + top, columns, stride=comps * rows), :]
            south = basis_ref[pl.ds(c * rows, columns, stride=comps * rows), :]
            north = north * mask[c][top : top + 1, :]
            south = south * mask[c][0:1, :]
            rowa_ref[c * columns : (c + 1) * columns, :] = pick(even_row, north, south)
            rowb_ref[c * columns : (c + 1) * columns, :] = pick(even_row, south, north)
        north = [mask[c][top : top + 1, :] * rhs[c][top : top + 1, :] for c in range(comps)]
        south = [mask[c][0:1, :] * rhs[c][0:1, :] for c in range(comps)]
        north += [visc[top : top + 1, :], visc[top - 1 : top, :]]
        south += [visc[0:1, :], visc[1:2, :]]
        for i in range(comps + 2):
            at = comps * columns + i
            rowa_ref[at : at + 1, :] = pick(even_row, north[i], south[i])
            rowb_ref[at : at + 1, :] = pick(even_row, south[i], north[i])
        rest = comps * columns + comps + 2
        blank = jnp.zeros((rowa_ref.shape[0] - rest, cols), F32)
        rowa_ref[rest:, :] = blank
        rowb_ref[rest:, :] = blank
    if cola_ref is None:
        return

    for c in range(comps):
        east, west = (jnp.zeros((rows, cols), F32), jnp.zeros((rows, cols), F32))
        for k in range(columns):
            base = (k * comps + c) * rows
            tile = basis_ref[base : base + rows, :]
            tile = pltpu.roll(tile, k + 1, 1)
            east = jnp.where(lane == k, tile, east)
            west = jnp.where(lane == k + 1, tile, west)
        west = pltpu.roll(west, low, 1)
        east = jnp.where(lane == columns, rhs[c][:, low : low + 1], east)
        west = jnp.where(lane == columns, rhs[c][:, 0:1], west)
        east = east * mask[c][:, low : low + 1]
        west = west * mask[c][:, 0:1]
        cola_ref[c * rows : (c + 1) * rows, :] = pick(even_col, east, west)
        colb_ref[c * rows : (c + 1) * rows, :] = pick(even_col, west, east)
    east = jnp.where(lane == 0, visc[:, low : low + 1], visc[:, low - 1 : low])
    west = jnp.where(lane == 0, visc[:, 0:1], visc[:, 1:2])
    cola_ref[comps * rows :, :] = pick(even_col, east, west)
    colb_ref[comps * rows :, :] = pick(even_col, west, east)


def stencil(mask, faces, diagonal, tile, halo):
    masked = mask * tile
    near = shifts(masked, *halo)
    inner = diagonal * masked - (
        faces[0] * near[0] + faces[1] * near[1] + faces[2] * near[2] + faces[3] * near[3]
    )
    return mask * inner + (1.0 - mask) * tile


def split(values):
    high = values.astype(jnp.bfloat16)
    return jnp.concatenate([high, (values - high.astype(F32)).astype(jnp.bfloat16)], axis=0)


def product(lefts, rights):
    return lax.dot_general(
        jnp.concatenate([split(value) for value in lefts], axis=1),
        jnp.concatenate([split(value) for value in rights], axis=1),
        (((1,), (1,)), ((), ())),
        preferred_element_type=F32,
    )


def merge(blocks, columns):
    blocks = blocks + pltpu.roll(blocks, columns, 1)
    return blocks[:columns] + blocks[columns:]


def local_kernel(sizes, basis_ref, rhs_ref, mask_ref, visc_ref, inner_ref, dots_ref, acc_ref):
    columns, comps, rows, cols = sizes
    _, has_south, _, has_west = flags()
    top, low = (rows - 1, cols - 1)
    rhs = [rhs_ref[c * rows : (c + 1) * rows, :] for c in range(comps)]
    mask = [mask_ref[c * rows : (c + 1) * rows, :].astype(F32) for c in range(comps)]
    visc = visc_ref[...]
    sub, lane = (iota((rows, cols), 0), iota((rows, cols), 1))
    empty = (jnp.zeros((1, cols), F32),) * 2 + (jnp.zeros((rows, 1), F32),) * 2
    faces = [0.5 * (visc + v) for v in shifts(visc, *empty)]
    faces[0] = jnp.where(sub == top, 0.0, faces[0])
    faces[1] = jnp.where(sub == 0, faces[1] * (1.0 - has_south), faces[1])
    faces[2] = jnp.where(lane == low, 0.0, faces[2])
    faces[3] = jnp.where(lane == 0, faces[3] * (1.0 - has_west), faces[3])
    diagonal = 1.0 + faces[0] + faces[1] + faces[2] + faces[3]

    blocks = jnp.zeros((2 * columns, 2 * columns), F32)
    for c in range(comps):
        m = mask[c]
        own = m * diagonal + (1.0 - m)
        up, down = (m * faces[0], m * faces[1])
        right = m * faces[2]
        left = jnp.where(lane == 0, 0.0, m * faces[3])
        plain = [
            basis_ref[pl.ds(c * rows + i, columns, stride=comps * rows), :] for i in range(rows)
        ]
        free = [plain[i] * m[i : i + 1, :] for i in range(rows)]
        images = []
        for i in range(rows):
            here = slice(i, i + 1)
            value = own[here] * plain[i] - right[here] * pltpu.roll(free[i], low, 1)
            value = value - left[here] * pltpu.roll(free[i], 1, 1)
            if i < top:
                value = value - up[here] * free[i + 1]
            if i > 0:
                value = value - down[here] * free[i - 1]
            images.append(value)
        for i in range(0, rows, 2):
            blocks = blocks + product(plain[i : i + 2], images[i : i + 2])
    inner_ref[...] = merge(blocks, columns)
    dots = to_row(project(basis_ref, rhs, acc_ref, columns, comps, rows))
    dots_ref[...] = jnp.broadcast_to(dots, dots_ref.shape)


def border_kernel(sizes, inner_ref, dots_ref, basis_ref, mask_ref, visc_ref, gram_ref, rowa_ref,
                  rowb_ref, cola_ref, colb_ref, owna_ref, ownb_ref, send_ref, full_ref):
    columns, comps, rows, cols = sizes
    even_row = 1 - lax.rem(lax.axis_index("row"), 2)
    even_col = 1 - lax.rem(lax.axis_index("col"), 2)
    has_north, _, has_east, _ = flags()
    top, low, half = (rows - 1, cols - 1, cols // 2)
    field = comps * rows
    visc, lanes = (visc_ref[...], iota((1, cols), 1))
    at = comps * columns + comps
    v_north = pick(even_row, rowa_ref[at : at + 1, :], rowb_ref[at : at + 1, :]) * has_north
    east = pick(even_col, cola_ref[...], colb_ref[...]) * has_east
    own_east = pick(even_col, owna_ref[...], ownb_ref[...])
    north_face = 0.5 * (visc[top : top + 1, :] + v_north)
    east_face = 0.5 * (visc[:, low : low + 1] + east[field:, 0:1])
    tops = []
    for c in range(comps):
        span = slice(c * columns, (c + 1) * columns)
        own = basis_ref[pl.ds(c * rows + top, columns, stride=comps * rows), :]
        own = own * mask_ref[c * rows + top : c * rows + rows, :].astype(F32)
        tops.append(own - pick(even_row, rowa_ref[span, :], rowb_ref[span, :]) * has_north)
    full = inner_ref[...] + merge(product([value * north_face for value in tops], tops), columns)
    gap = own_east[:field] - east[:field]
    edge = lax.dot_general(
        gap * jnp.concatenate([east_face] * comps, axis=0), gap, (((0,), (0,)), ((), ())),
        preferred_element_type=F32, precision=lax.Precision.HIGHEST,
    )
    wide_lane = iota((columns, cols), 1)
    edge = jnp.where(wide_lane < half, edge[:columns], 0.0)
    full = full + edge + pltpu.roll(edge, half, 1)
    full_ref[...] = full
    spot = jnp.where(wide_lane >= half, wide_lane - half, wide_lane) == iota((columns, cols), 0)
    spine = jnp.sum(jnp.where(spot, full, 0.0), axis=0, keepdims=True)
    count = columns // 2
    chunk = jnp.where(
        iota((count, cols), 1) < half,
        full_ref[pl.ds(0, count, stride=2), :],
        full_ref[pl.ds(1, count, stride=2), :],
    )
    dots = dots_ref[0:1, :]
    corner_row = jnp.zeros((1, cols), F32)
    for i, corner in enumerate(corners_of(visc)):
        corner_row = jnp.where(lanes == i, corner, corner_row)
    at = 2 * lax.axis_index("row")
    piece = jnp.concatenate([gram_ref[pl.ds(at + t, 1), :] for t in range(2)], axis=1)
    head = jnp.concatenate([jnp.where(lanes < half, dots, spine), piece], axis=0)
    for d in range(count):
        send_ref[d] = jnp.concatenate([head, chunk[d : d + 1, :], corner_row], axis=0)


def first_kernel(sizes, whole_rows, two, got_ref, *refs):
    columns, comps, rows, cols, scale = sizes
    if whole_rows:
        gram_in_ref = None
    else:
        gram_in_ref, *refs = refs
    (basis_ref, rhs_ref, mask_ref, visc_ref, rowa_ref, rowb_ref, cola_ref, colb_ref,
     send_ref, state_ref, face_ref, small_ref, gram_ref, *refs) = refs
    edge_ref, side_ref = (None, None) if two else refs[:2]
    acc_ref, wide_ref = refs[-2:]
    at_row, at_col = (lax.axis_index("row"), lax.axis_index("col"))
    row_count, col_count = (lax.axis_size("row"), lax.axis_size("col"))
    even_row, even_col = (1 - lax.rem(at_row, 2), 1 - lax.rem(at_col, 2))
    me = at_row * col_count + at_col
    top, low = rows - 1, cols - 1
    rhs = [rhs_ref[c * rows : (c + 1) * rows, :] for c in range(comps)]
    mask = [mask_ref[c * rows : (c + 1) * rows, :].astype(F32) for c in range(comps)]
    visc = visc_ref[...]
    sub, lane = (iota((rows, cols), 0), iota((rows, cols), 1))
    lanes = iota((1, cols), 1)

    if whole_rows:
        per = cols // columns
        for r in range(row_count):
            for c in range(col_count):
                piece = got_ref[r * col_count + c, 1:2, :]
                for t in range(per):
                    at = (c * row_count + r) * per + t
                    moved = pltpu.roll(piece, cols - t * columns, 1) if t else piece
                    gram_ref[at : at + 1, :] = moved
    else:
        gram_ref[:, :columns] = gram_in_ref[...]
    all_sums = jnp.sum(got_ref[...], axis=0)
    sums = all_sums[0:1, :]
    dots = jnp.where(lanes < columns, sums, 0.0)
    gram = jnp.where(iota((columns, cols), 1) < columns, gram_ref[...], 0.0)
    coeffs = jnp.sum(gram * dots, axis=1, keepdims=True) * scale
    wide = jnp.broadcast_to(coeffs, (columns, cols))
    wide_ref[...] = wide
    coeff_row = to_row(coeffs)

    extra = comps * columns
    tail_a, tail_b = (rowa_ref[extra:, :], rowb_ref[extra:, :])
    has_north, has_south, has_east, has_west = flags()
    north_tail = pick(even_row, tail_a, tail_b) * has_north
    south_tail = pick(even_row, tail_b, tail_a) * has_south
    side_a, side_b = (cola_ref[...], colb_ref[...])
    east_side = pick(even_col, side_a, side_b) * has_east
    west_side = pick(even_col, side_b, side_a) * has_west
    v_north, v_south = (north_tail[comps : comps + 1, :], south_tail[comps : comps + 1, :])
    v_north2, v_south2 = (north_tail[comps + 1 : comps + 2, :], south_tail[comps + 1 : comps + 2, :])
    v_east, v_west = (east_side[comps * rows :, 0:1], west_side[comps * rows :, 0:1])
    v_east2, v_west2 = (east_side[comps * rows :, 1:2], west_side[comps * rows :, 1:2])
    faces = [0.5 * (visc + v) for v in shifts(visc, v_north, v_south, v_east, v_west)]
    diagonal = 1.0 + faces[0] + faces[1] + faces[2] + faces[3]
    face_ref[...] = jnp.concatenate(faces + [diagonal], axis=0)
    jacobi = [m / diagonal + (1.0 - m) for m in mask]

    def corner(step_row, step_col, which):
        r, c = (at_row + step_row, at_col + step_col)
        inside = (r >= 0) & (r < row_count) & (c >= 0) & (c < col_count)
        place = jnp.where(inside, r * col_count + c, me)
        line, first = (3, 0) if two else (0, columns)
        value = got_ref[place, line : line + 1, :]
        value = jnp.sum(jnp.where(lanes == first + which, value, 0.0), axis=1, keepdims=True)
        return value * jnp.where(inside, 1.0, 0.0)

    north_west, north_east = (corner(1, -1, 1), corner(1, 1, 0))
    south_west, south_east = (corner(-1, -1, 3), corner(-1, 1, 2))

    def row_inverse(own, inner, outer, west, east):
        right = jnp.where(lanes == low, east, pltpu.roll(own, low, 1))
        left = jnp.where(lanes == 0, west, pltpu.roll(own, 1, 1))
        return 1.0 / (1.0 + 0.5 * (4.0 * own + inner + outer + left + right))

    def side_inverse(own, inner, outer, south, north):
        own = jnp.broadcast_to(own, (rows, cols))
        up = jnp.where(sub == top, north, pltpu.roll(own, top, 0))
        down = jnp.where(sub == 0, south, pltpu.roll(own, 1, 0))
        return 1.0 / (1.0 + 0.5 * (4.0 * own + inner + outer + up + down))

    inv_north = row_inverse(v_north, visc[top : top + 1, :], v_north2, north_west, north_east)
    inv_south = row_inverse(v_south, visc[0:1, :], v_south2, south_west, south_east)
    inv_east = side_inverse(v_east, visc[:, low : low + 1], v_east2, south_east, north_east)
    inv_west = side_inverse(v_west, visc[:, 0:1], v_west2, south_west, north_west)

    corr = combine(basis_ref, wide_ref, columns, comps, rows)
    image, scaled, smooth, point = ([], [], [], [])
    scaled_image = []
    none = (jnp.zeros((1, cols), F32),) * 2 + (jnp.zeros((rows, 1), F32),) * 2
    for c in range(comps):
        span = slice(c * columns, (c + 1) * columns)
        sum_a = jnp.sum(wide * rowa_ref[span, :], axis=0, keepdims=True)
        sum_b = jnp.sum(wide * rowb_ref[span, :], axis=0, keepdims=True)
        u_north = inv_north * north_tail[c : c + 1, :]
        u_south = inv_south * south_tail[c : c + 1, :]
        p_north = u_north + has_north * pick(even_row, sum_a, sum_b)
        p_south = u_south + has_south * pick(even_row, sum_b, sum_a)
        here = slice(c * rows, (c + 1) * rows)
        east, west = (east_side[here, :], west_side[here, :])
        u_east = inv_east * east[:, columns : columns + 1]
        u_west = inv_west * west[:, columns : columns + 1]
        p_east = u_east + jnp.sum(coeff_row * east, axis=1, keepdims=True)
        p_west = u_west + jnp.sum(coeff_row * west, axis=1, keepdims=True)
        u = jacobi[c] * rhs[c]
        p = u + corr[c]
        q = stencil(mask[c], faces, diagonal, p, (p_north, p_south, p_east, p_west))
        if two:
            scaled_image.append(stencil(mask[c], faces, diagonal, jacobi[c] * q, none))
        smooth.append(u)
        point.append(p)
        image.append(q)
        scaled.append(jacobi[c] * q)
        if two:
            continue
        for i, value in enumerate((u_north, u_south, p_north, p_south)):
            edge_ref[i * 8 + c : i * 8 + c + 1, :] = value
        for i, value in enumerate((u_east, u_west, p_east, p_west)):
            side_ref[(i * comps + c) * rows : (i * comps + c + 1) * rows, :] = value
    fields = point + image + scaled
    state_ref[...] = jnp.concatenate(fields if two else smooth + fields, axis=0)

    row = to_row(project(basis_ref, image, acc_ref, columns, comps, rows))
    pairs = ((point, image), (smooth, image), (image, scaled), (rhs, smooth))
    if two:
        pairs += ((scaled, scaled_image),)
    for i, (left, right) in enumerate(pairs):
        value = left[0] * right[0]
        for c in range(1, comps):
            value = value + left[c] * right[c]
        row = jnp.where(lanes == (DOTS2 if two else DOTS) + i, total(value), row)
    masked = [mask[c] * scaled[c] for c in range(comps)]
    if two:
        norths = [m[top : top + 1, :] * faces[0][top : top + 1, :] * has_north for m in masked]
        easts = [m[:, low : low + 1] * faces[2][:, low : low + 1] * has_east for m in masked]
        souths, wests = ([m[0:1, :] for m in masked], [m[:, 0:1] for m in masked])
        row = row + to_row(jnp.concatenate(easts, axis=0), EAST2)
        row = row + to_row(jnp.concatenate(wests, axis=0), WEST2)
        reach = project(basis_ref, scaled_image, acc_ref, columns, comps, rows)
        beyond = jnp.zeros((columns, cols), F32)
        aside = jnp.zeros((rows, cols), F32)
        for c in range(comps):
            span, here = (slice(c * columns, (c + 1) * columns), slice(c * rows, (c + 1) * rows))
            halo_a, halo_b = (rowa_ref[span, :], rowb_ref[span, :])
            low_side = souths[c] * faces[1][0:1, :] * has_south
            beyond = beyond + norths[c] * pick(even_row, halo_a, halo_b)
            beyond = beyond + low_side * pick(even_row, halo_b, halo_a)
            aside = aside + easts[c] * east_side[here, :]
            aside = aside + wests[c] * faces[3][:, 0:1] * west_side[here, :]
        reach = to_row(reach - jnp.sum(beyond, axis=1, keepdims=True))
        reach = reach - jnp.where(lanes < columns, jnp.sum(aside, axis=0, keepdims=True), 0.0)
        half = cols // 2
        ours = jnp.broadcast_to(all_sums[2:3, :], (8, cols))
        other = pltpu.roll(ours, half, 1)
        wide_lane = iota((8, cols), 1)
        for t, (first, second) in enumerate(((ours, other), (other, ours))):
            value = jnp.where(wide_lane < half, first, second)
            turn = lax.rem(half + t * (half // 2) - (2 * me + t + 1) + 2 * cols, cols)
            value = pltpu.roll(value, turn, 1)[0:1, :]
            start = half + t * (half // 2)
            reach = jnp.where((lanes >= start) & (lanes < start + half // 2), value, reach)
        message = jnp.concatenate(norths + souths + [row, reach], axis=0)
        send_ref[...] = jnp.broadcast_to(message[None], send_ref.shape)
        spine = pltpu.roll(jnp.broadcast_to(sums, (8, cols)), half, 1)[0:1, :]
        spine = jnp.where(lanes < half, spine, 0.0)
        small_ref[...] = jnp.concatenate([dots, coeff_row, spine, jnp.zeros((5, cols), F32)], axis=0)
        return
    east = jnp.concatenate([m[:, low : low + 1] for m in masked], axis=0)
    west = jnp.concatenate([m[:, 0:1] for m in masked], axis=0)
    row = row + to_row(east, EAST) + to_row(west, WEST)
    message = jnp.concatenate([row] + [m[top : top + 1, :] for m in masked], axis=0)
    send_ref[...] = jnp.broadcast_to(message[None], send_ref.shape)
    message = jnp.concatenate([row] + [m[0:1, :] for m in masked], axis=0)
    send_ref[jnp.where(at_row > 0, me - col_count, me)] = message
    small_ref[...] = jnp.concatenate([dots, coeff_row, jnp.zeros((6, cols), F32)], axis=0)


def second_kernel(sizes, got_ref, basis_ref, rhs_ref, mask_ref, rowa_ref, rowb_ref, cola_ref,
                  colb_ref, state_ref, face_ref, small_ref, gram_ref, edge_ref, side_ref,
                  send_ref, out_ref, last_ref, wide_ref):
    columns, comps, rows, cols, scale = sizes
    at_row, at_col = (lax.axis_index("row"), lax.axis_index("col"))
    row_count, col_count = (lax.axis_size("row"), lax.axis_size("col"))
    even_row, even_col = (1 - lax.rem(at_row, 2), 1 - lax.rem(at_col, 2))
    me = at_row * col_count + at_col
    lanes = iota((1, cols), 1)
    mask = [mask_ref[c * rows : (c + 1) * rows, :].astype(F32) for c in range(comps)]

    sums = jnp.sum(got_ref[...], axis=0)[0:1, :]
    image_dots = jnp.where(lanes < columns, sums, 0.0)
    curve, cross, image_sq, rhs_sq = [
        jnp.sum(jnp.where(lanes == DOTS + i, sums, 0.0), axis=1, keepdims=True) for i in range(4)
    ]
    dots, coeff_row = (small_ref[0:1, :], small_ref[1:2, :])
    energy = rhs_sq + jnp.sum(dots * coeff_row, axis=1, keepdims=True)
    step = energy / curve
    gram = jnp.where(iota((columns, cols), 1) < columns, gram_ref[...], 0.0)
    dots = dots - step * image_dots
    coeffs = jnp.sum(gram * dots, axis=1, keepdims=True) * scale
    wide = jnp.broadcast_to(coeffs, (columns, cols))
    wide_ref[...] = wide
    coeff_row = to_row(coeffs)
    energy_new = rhs_sq - 2.0 * step * cross + step * step * image_sq
    energy_new = energy_new + jnp.sum(dots * coeff_row, axis=1, keepdims=True)
    ratio = energy_new / energy

    def beside(step_row, step_col):
        r, c = (at_row + step_row, at_col + step_col)
        inside = (r >= 0) & (r < row_count) & (c >= 0) & (c < col_count)
        message = got_ref[jnp.where(inside, r * col_count + c, me)]
        return message * jnp.where(inside, 1.0, 0.0)

    q_north, q_south = (beside(1, 0), beside(-1, 0))
    q_east = to_column(beside(0, 1)[0:1, :], comps * rows, WEST)
    q_west = to_column(beside(0, -1)[0:1, :], comps * rows, EAST)

    side_a, side_b = (cola_ref[...], colb_ref[...])
    has_north, has_south, has_east, has_west = flags()
    east_side = pick(even_col, side_a, side_b) * has_east
    west_side = pick(even_col, side_b, side_a) * has_west
    faces = [face_ref[i * rows : (i + 1) * rows, :] for i in range(4)]
    diagonal = face_ref[4 * rows : 5 * rows, :]
    corr = combine(basis_ref, wide_ref, columns, comps, rows)
    curve_part = jnp.zeros((rows, cols), F32)
    first, second, third, fourth = ([], [], [], [])
    for c in range(comps):
        span = slice(c * columns, (c + 1) * columns)
        here = slice(c * rows, (c + 1) * rows)
        sum_a = jnp.sum(wide * rowa_ref[span, :], axis=0, keepdims=True)
        sum_b = jnp.sum(wide * rowb_ref[span, :], axis=0, keepdims=True)
        old = [edge_ref[i * 8 + c : i * 8 + c + 1, :] for i in range(4)]
        p_north = old[0] - step * q_north[1 + c : 2 + c, :] + has_north * pick(even_row, sum_a, sum_b)
        p_south = old[1] - step * q_south[1 + c : 2 + c, :] + has_south * pick(even_row, sum_b, sum_a)
        p_north, p_south = (p_north + ratio * old[2], p_south + ratio * old[3])
        old = [side_ref[(i * comps + c) * rows : (i * comps + c + 1) * rows, :] for i in range(4)]
        p_east = old[0] - step * q_east[here] + ratio * old[2]
        p_west = old[1] - step * q_west[here] + ratio * old[3]
        p_east = p_east + jnp.sum(coeff_row * east_side[here, :], axis=1, keepdims=True)
        p_west = p_west + jnp.sum(coeff_row * west_side[here, :], axis=1, keepdims=True)
        u, p, q, jq = [
            state_ref[(i * comps + c) * rows : (i * comps + c + 1) * rows, :] for i in range(4)
        ]
        new = u - step * jq + corr[c] + ratio * p
        masked = mask[c] * new
        near = shifts(masked, p_north, p_south, p_east, p_west)
        stencil = diagonal * masked - (
            faces[0] * near[0] + faces[1] * near[1] + faces[2] * near[2] + faces[3] * near[3]
        )
        applied = mask[c] * stencil + (1.0 - mask[c]) * new
        curve_part = curve_part + new * applied
        first.append(step * p)
        second.append(new)
        third.append(rhs_ref[here, :] - step * q)
        fourth.append(applied)
    out_ref[...] = jnp.concatenate(first + second + third + fourth, axis=0)
    last_ref[...] = jnp.broadcast_to(energy_new, last_ref.shape)
    send_ref[...] = jnp.broadcast_to(total(curve_part)[None], send_ref.shape)


def close_kernel(sizes, got_ref, basis_ref, rhs_ref, mask_ref, rowa_ref, rowb_ref, cola_ref,
                 colb_ref, state_ref, face_ref, small_ref, gram_ref,
                 solution_ref, residual_ref, wide_ref):
    columns, comps, rows, cols, scale = sizes
    at_row, at_col = (lax.axis_index("row"), lax.axis_index("col"))
    row_count, col_count = (lax.axis_size("row"), lax.axis_size("col"))
    devices = row_count * col_count
    even_row, even_col = (1 - lax.rem(at_row, 2), 1 - lax.rem(at_col, 2))
    has_north, has_south, has_east, has_west = flags()
    me = at_row * col_count + at_col
    half, quarter = (cols // 2, cols // 4)
    lanes = iota((1, cols), 1)
    mask = [mask_ref[c * rows : (c + 1) * rows, :].astype(F32) for c in range(comps)]

    def along(left, right):
        return jnp.sum(left * right, axis=1, keepdims=True)

    sums = jnp.sum(got_ref[...], axis=0)
    line = sums[2 * comps : 2 * comps + 1, :]
    image_dots = jnp.where(lanes < columns, line, 0.0)
    reach_dots = jnp.where(lanes < columns, sums[2 * comps + 1 :, :], 0.0)
    gram = jnp.where(iota((columns, cols), 1) < columns, gram_ref[...], 0.0)
    turn = jnp.sum(gram * image_dots, axis=1, keepdims=True) * scale
    wide = jnp.broadcast_to(turn, (columns, cols))
    wide_ref[...] = wide
    turn_row = to_row(turn)

    def beside(step_row, step_col):
        r, c = (at_row + step_row, at_col + step_col)
        inside = (r >= 0) & (r < row_count) & (c >= 0) & (c < col_count)
        message = got_ref[jnp.where(inside, r * col_count + c, me)]
        return message * jnp.where(inside, 1.0, 0.0)

    faces = [face_ref[i * rows : (i + 1) * rows, :] for i in range(4)]
    diagonal = face_ref[4 * rows : 5 * rows, :]
    q_north, q_south = (beside(1, 0), beside(-1, 0))
    q_east = to_column(beside(0, 1)[2 * comps : 2 * comps + 1, :], comps * rows, WEST2)
    q_west = to_column(beside(0, -1)[2 * comps : 2 * comps + 1, :], comps * rows, EAST2)
    side_a, side_b = (cola_ref[...], colb_ref[...])
    east_side = pick(even_col, side_a, side_b) * has_east
    west_side = pick(even_col, side_b, side_a) * has_west
    corr = combine(basis_ref, wide_ref, columns, comps, rows)
    moved, moved_image = ([], [])
    for c in range(comps):
        span = slice(c * columns, (c + 1) * columns)
        here = slice(c * rows, (c + 1) * rows)
        sum_a = jnp.sum(wide * rowa_ref[span, :], axis=0, keepdims=True)
        sum_b = jnp.sum(wide * rowb_ref[span, :], axis=0, keepdims=True)
        north = q_north[comps + c : comps + c + 1, :] + has_north * pick(even_row, sum_a, sum_b)
        south = q_south[c : c + 1, :] / faces[1][0:1, :] + has_south * pick(even_row, sum_b, sum_a)
        east = q_east[here] + along(turn_row, east_side[here, :])
        west = q_west[here] / faces[3][:, 0:1] + along(turn_row, west_side[here, :])
        at = (2 * comps + c) * rows
        value = state_ref[at : at + rows, :] + corr[c]
        moved.append(value)
        moved_image.append(stencil(mask[c], faces, diagonal, value, (north, south, east, west)))

    parts = [jnp.zeros((2 * comps + 2, cols), F32) for _ in range(4)]
    for d in range(devices - col_count):
        value = got_ref[d] * pltpu.roll(got_ref[d + col_count], comps + 2, 0)
        parts[d % 4] = parts[d % 4] + value
    border = (parts[0] + parts[1]) + (parts[2] + parts[3])
    border = jnp.where(iota(border.shape, 0) < comps, border, 0.0)
    lines = got_ref[:, 2 * comps, :]
    later = pltpu.roll(pltpu.roll(lines, devices - 1, 0), cols - (WEST2 - EAST2), 1)
    line_lane = iota(lines.shape, 1)
    beside_it = jnp.where((line_lane >= EAST2) & (line_lane < WEST2), lines * later, 0.0)
    across = jnp.sum(border, axis=0, keepdims=True) + jnp.sum(beside_it, axis=0, keepdims=True)

    packed = pltpu.roll(got_ref[:, 2 * comps + 1, :], half, 1)
    sub = iota(packed.shape, 0)
    value = jnp.broadcast_to(turn_row, (8, cols))
    value = jnp.broadcast_to((value + pltpu.roll(value, half, 1))[0:1, :], packed.shape)
    bit = 1
    while bit < devices:
        value = jnp.where((sub & bit) != 0, pltpu.roll(value, cols - 2 * bit, 1), value)
        bit *= 2
    ahead = pltpu.roll(value, cols - 1, 1)
    ahead = jnp.where(line_lane < quarter, ahead, pltpu.roll(value, quarter - 2, 1))
    own = jnp.where(line_lane < quarter, value[:, 0:1], value[:, 1:2])
    weight = jnp.where((line_lane == quarter - 1) | (line_lane == half - 1), 1.0, 2.0)
    form = jnp.where(line_lane < half, packed * weight * own * ahead, 0.0)
    form = jnp.sum(form, axis=0, keepdims=True)

    curve, cross, image_sq, rhs_sq, scaled_sq = [
        along(jnp.where(lanes == DOTS2 + i, 1.0, 0.0), line) for i in range(5)
    ]
    dots, old_row, spine = (small_ref[0:1, :], small_ref[1:2, :], small_ref[2:3, :])
    energy = rhs_sq + along(dots, old_row)
    meet = image_sq + along(turn_row, image_dots)
    rest = form + spine * turn_row * turn_row + 2.0 * turn_row * reach_dots - 2.0 * across
    moved_sq = scaled_sq + jnp.sum(rest, axis=1, keepdims=True)
    step = energy / curve
    energy_new = rhs_sq - 2.0 * step * cross + step * step * image_sq
    energy_new = energy_new + along(dots - step * image_dots, old_row - step * turn_row)
    grow = 1.0 + energy_new / energy
    curve_new = grow * grow * curve - 2.0 * step * grow * meet + step * step * moved_sq
    step_new = energy_new / curve_new
    near, far = (step + step_new * grow, step_new * step)
    for c in range(comps):
        here = slice(c * rows, (c + 1) * rows)
        p = state_ref[here, :]
        q = state_ref[(comps + c) * rows : (comps + c + 1) * rows, :]
        solution_ref[here, :] = near * p - far * moved[c]
        residual_ref[here, :] = rhs_ref[here, :] - near * q + far * moved_image[c]


def last_kernel(count, got_ref, in_ref, last_ref, solution_ref, residual_ref):
    step = last_ref[0:1, :] / jnp.sum(got_ref[...], axis=0)
    solution_ref[...] = in_ref[:count, :] + step * in_ref[count : 2 * count, :]
    residual_ref[...] = in_ref[2 * count : 3 * count, :] - step * in_ref[3 * count :, :]


def on_device(right_side, viscosity, free_mask, coarse_basis, gram_inverse):
    comps, rows, cols = right_side.shape
    columns = coarse_basis.shape[0]
    row_count, col_count = (lax.axis_size("row"), lax.axis_size("col"))
    devices = row_count * col_count
    scale = 1.0 / (32.0 * math.sqrt(float(comps * rows * cols * devices * columns)))
    sizes = (columns, comps, rows, cols)

    def call(kernel, outs, scratch, *args, flops=None):
        cost = flops and pl.CostEstimate(flops=flops, bytes_accessed=4096, transcendentals=0)
        return pl.pallas_call(
            kernel,
            out_shape=[jax.ShapeDtypeStruct(s, F32) for s in outs],
            in_specs=[VMEM] * len(args),
            out_specs=[VMEM] * len(outs),
            scratch_shapes=[pltpu.VMEM(s, F32) for s in scratch],
            cost_estimate=cost,
            compiler_params=pltpu.CompilerParams(vmem_limit_bytes=16 * 1024 * 1024),
        )(*args)

    def share(message):
        return lax.all_to_all(message, ("row", "col"), 0, 0, tiled=True)

    def swap(packet, axis, first):
        pairs = []
        for r in range(row_count):
            for c in range(col_count):
                along, across = ((r, c) if axis == "row" else (c, r))
                length, width = (row_count, col_count)[:: 1 if axis == "row" else -1]
                other = along + 1 if (along - first) % 2 == 0 else along - 1
                if 0 <= other < length:
                    mate = (other, across)
                else:
                    mate = (along, across ^ 1 if (across ^ 1) < width else across)
                r2, c2 = mate if axis == "row" else mate[::-1]
                pairs.append((r * col_count + c, r2 * col_count + c2))
        return lax.ppermute(packet, ("row", "col"), pairs)

    basis = coarse_basis.reshape(columns * comps * rows, cols)
    rhs = right_side.reshape(comps * rows, cols)
    mask = free_mask.reshape(comps * rows, cols)

    block = gram_inverse.size
    piece = -(-block // row_count)
    two = columns * columns == devices * cols and cols == 2 * columns and rows == 8 and comps == 3
    if two:
        (first,) = call(open_kernel, [(8, cols)], [], flops=10**9)
        own = gram_inverse
    else:
        flat = jnp.pad(gram_inverse.reshape(-1), (0, piece * row_count - block))
        own = lax.dynamic_slice_in_dim(flat, lax.axis_index("row") * piece, piece)
        own = jnp.pad(own, (0, cols - piece)).reshape(1, cols)

    tall = -(-(comps * columns + comps + 2) // 8) * 8
    wide = (comps + 1) * rows
    field = comps * rows
    if two:
        row_a, row_b = call(
            functools.partial(rows_kernel, sizes),
            [(tall, cols), (tall, cols)],
            [],
            basis, rhs, mask, viscosity, first,
        )
        col_a, col_b = call(
            functools.partial(sides_kernel, sizes),
            [(wide, cols), (wide, cols)],
            [],
            basis, rhs, mask, viscosity,
        )
        packets = ((row_a, "row", 0), (row_b, "row", 1), (col_a, "col", 0), (col_b, "col", 1))
        halos = []
        for packet in packets:
            halos.append(swap(*packet))
        inner, dots = call(
            functools.partial(local_kernel, sizes),
            [(columns, cols), (8, cols)],
            [(columns * rows, cols)],
            basis, rhs, mask, viscosity, flops=10**8,
        )
        (send,) = call(
            functools.partial(border_kernel, sizes),
            [(devices, 4, cols)],
            [(columns, cols)],
            inner, dots, basis, mask, viscosity, own, *halos, col_a, col_b,
        )
        sizes = sizes + (scale,)
        send, *state = call(
            functools.partial(first_kernel, sizes, True, True),
            [(devices, 8, cols), (3 * field, cols), (5 * rows, cols), (8, cols), (columns, cols)],
            [(columns * rows, cols), (columns, cols)],
            share(send), basis, rhs, mask, viscosity, *halos,
        )
        solution, residual = call(
            functools.partial(close_kernel, sizes),
            [(field, cols), (field, cols)],
            [(columns, cols)],
            share(send), basis, rhs, mask, *halos, *state,
        )
        return (solution.reshape(right_side.shape), residual.reshape(right_side.shape))
    send, row_a, row_b, col_a, col_b = call(
        functools.partial(pack_kernel, sizes),
        [(devices, 2, cols), (tall, cols), (tall, cols), (wide, cols), (wide, cols)],
        [(columns * rows, cols)],
        basis, rhs, mask, viscosity, own,
    )
    halos = (swap(row_a, "row", 0), swap(row_b, "row", 1), swap(col_a, "col", 0), swap(col_b, "col", 1))
    got = share(send)
    whole_rows = piece == cols and cols % columns == 0 and block == piece * row_count
    gram = ()
    if not whole_rows:
        gram = got[:, 1, :piece].reshape(row_count, col_count, piece).transpose(1, 0, 2)
        gram = gram.reshape(col_count, row_count * piece)[:, :block].reshape(columns, columns)
        gram = (gram,)
    sizes = sizes + (scale,)
    send, *state = call(
        functools.partial(first_kernel, sizes, whole_rows, False),
        [(devices, 1 + comps, cols), (4 * field, cols), (5 * rows, cols), (8, cols),
         (columns, cols), (32, cols), (4 * field, cols)],
        [(columns * rows, cols), (columns, cols)],
        got, *gram, basis, rhs, mask, viscosity, *halos,
    )
    send, fields, last = call(
        functools.partial(second_kernel, sizes),
        [(devices, 1, cols), (4 * field, cols), (8, cols)],
        [(columns, cols)],
        share(send), basis, rhs, mask, *halos, *state,
    )
    solution, residual = call(
        functools.partial(last_kernel, field),
        [(field, cols), (field, cols)],
        [],
        share(send), fields, last,
    )
    return (solution.reshape(right_side.shape), residual.reshape(right_side.shape))


def solution(mesh):
    in_specs = (
        P(None, "row", "col"),
        P("row", "col"),
        P(None, "row", "col"),
        P(None, None, "row", "col"),
        P("col", None),
    )
    out_specs = (P(None, "row", "col"), P(None, "row", "col"))
    return jax.shard_map(
        on_device, mesh=mesh, in_specs=in_specs, out_specs=out_specs, check_vma=False
    )
```

```python
import functools
import math

import jax
import jax.numpy as jnp
from jax import lax
from jax.experimental import pallas as pl
from jax.experimental.pallas import tpu as pltpu
from jax.sharding import PartitionSpec as P


F32 = jnp.float32
VMEM = pl.BlockSpec(memory_space=pltpu.VMEM)
DOTS, EAST, WEST = 64, 72, 96
EAST2, WEST2, DOTS2 = 64, 88, 112


def flags():
    at_row, at_col = (lax.axis_index("row"), lax.axis_index("col"))
    tests = (
        at_row < lax.axis_size("row") - 1,
        at_row > 0,
        at_col < lax.axis_size("col") - 1,
        at_col > 0,
    )
    return [jnp.where(test, 1.0, 0.0) for test in tests]


def iota(shape, dim):
    return lax.broadcasted_iota(jnp.int32, shape, dim)


def pick(flag, yes, no):
    return jnp.where(jnp.full(yes.shape, flag, jnp.int32) == 1, yes, no)


def to_row(column, first=0):
    shape = (column.shape[0], 128)
    spread = jnp.where(iota(shape, 1) == iota(shape, 0) + first, column, 0.0)
    return jnp.sum(spread, axis=0, keepdims=True)


def to_column(row, count, first=0):
    shape = (count, 128)
    spread = jnp.where(iota(shape, 1) == iota(shape, 0) + first, row, 0.0)
    return jnp.sum(spread, axis=1, keepdims=True)


def total(values):
    return jnp.sum(jnp.sum(values, axis=0, keepdims=True), axis=1, keepdims=True)


def shifts(tile, north, south, east, west):
    rows, cols = tile.shape
    sub, lane = (iota(tile.shape, 0), iota(tile.shape, 1))
    return (
        jnp.where(sub == rows - 1, north, pltpu.roll(tile, rows - 1, 0)),
        jnp.where(sub == 0, south, pltpu.roll(tile, 1, 0)),
        jnp.where(lane == cols - 1, east, pltpu.roll(tile, cols - 1, 1)),
        jnp.where(lane == 0, west, pltpu.roll(tile, 1, 1)),
    )


def project(basis_ref, field, acc_ref, columns, comps, rows):
    for k in range(columns):
        base = k * comps * rows
        acc = basis_ref[base : base + rows, :] * field[0]
        for c in range(1, comps):
            acc = acc + basis_ref[base + c * rows : base + (c + 1) * rows, :] * field[c]
        acc_ref[k * rows : (k + 1) * rows, :] = acc
    sums = acc_ref[pl.ds(0, columns, stride=rows), :]
    for s in range(1, rows):
        sums = sums + acc_ref[pl.ds(s, columns, stride=rows), :]
    return jnp.sum(sums, axis=1, keepdims=True)


def combine(basis_ref, wide_ref, columns, comps, rows):
    out = [[None, None] for _ in range(comps)]
    for k in range(columns):
        weight = jnp.broadcast_to(wide_ref[k : k + 1, :], (rows, 128))
        for c in range(comps):
            base = (k * comps + c) * rows
            term = weight * basis_ref[base : base + rows, :]
            old = out[c][k % 2]
            out[c][k % 2] = term if old is None else old + term
    return [a + b for a, b in out]


def pack_kernel(sizes, basis_ref, rhs_ref, mask_ref, visc_ref, gram_ref,
                send_ref, rowa_ref, rowb_ref, cola_ref, colb_ref, acc_ref):
    columns, comps, rows, cols = sizes
    packet_kernel(sizes, basis_ref, rhs_ref, mask_ref, visc_ref, rowa_ref, rowb_ref, cola_ref, colb_ref)
    rhs = [rhs_ref[c * rows : (c + 1) * rows, :] for c in range(comps)]
    visc = visc_ref[...]

    row = to_row(project(basis_ref, rhs, acc_ref, columns, comps, rows))
    lanes = iota((1, cols), 1)
    for i, corner in enumerate(corners_of(visc)):
        row = jnp.where(lanes == columns + i, corner, row)
    both = jnp.concatenate([row, gram_ref[...]], axis=0)
    send_ref[...] = jnp.broadcast_to(both[None], send_ref.shape)


def open_kernel(out_ref):
    out_ref[...] = jnp.zeros_like(out_ref)


def rows_kernel(sizes, basis_ref, rhs_ref, mask_ref, visc_ref, first_ref, rowa_ref, rowb_ref):
    packet_kernel(sizes, basis_ref, rhs_ref, mask_ref, visc_ref, rowa_ref, rowb_ref, None, None)


def sides_kernel(sizes, basis_ref, rhs_ref, mask_ref, visc_ref, cola_ref, colb_ref):
    packet_kernel(sizes, basis_ref, rhs_ref, mask_ref, visc_ref, None, None, cola_ref, colb_ref)


def corners_of(visc):
    top, low = (visc.shape[0] - 1, visc.shape[1] - 1)
    return [visc[i : i + 1, j : j + 1] for i in (0, top) for j in (0, low)]


def packet_kernel(sizes, basis_ref, rhs_ref, mask_ref, visc_ref,
                  rowa_ref, rowb_ref, cola_ref, colb_ref):
    columns, comps, rows, cols = sizes
    even_row = 1 - lax.rem(lax.axis_index("row"), 2)
    even_col = 1 - lax.rem(lax.axis_index("col"), 2)
    rhs = [rhs_ref[c * rows : (c + 1) * rows, :] for c in range(comps)]
    mask = [mask_ref[c * rows : (c + 1) * rows, :].astype(F32) for c in range(comps)]
    visc = visc_ref[...]
    lane = iota((rows, cols), 1)
    top, low = rows - 1, cols - 1

    if rowa_ref is not None:
        for c in range(comps):
            north = basis_ref[pl.ds(c * rows + top, columns, stride=comps * rows), :]
            south = basis_ref[pl.ds(c * rows, columns, stride=comps * rows), :]
            north = north * mask[c][top : top + 1, :]
            south = south * mask[c][0:1, :]
            rowa_ref[c * columns : (c + 1) * columns, :] = pick(even_row, north, south)
            rowb_ref[c * columns : (c + 1) * columns, :] = pick(even_row, south, north)
        north = [mask[c][top : top + 1, :] * rhs[c][top : top + 1, :] for c in range(comps)]
        south = [mask[c][0:1, :] * rhs[c][0:1, :] for c in range(comps)]
        north += [visc[top : top + 1, :], visc[top - 1 : top, :]]
        south += [visc[0:1, :], visc[1:2, :]]
        for i in range(comps + 2):
            at = comps * columns + i
            rowa_ref[at : at + 1, :] = pick(even_row, north[i], south[i])
            rowb_ref[at : at + 1, :] = pick(even_row, south[i], north[i])
        rest = comps * columns + comps + 2
        blank = jnp.zeros((rowa_ref.shape[0] - rest, cols), F32)
        rowa_ref[rest:, :] = blank
        rowb_ref[rest:, :] = blank
    if cola_ref is None:
        return

    for c in range(comps):
        east, west = (jnp.zeros((rows, cols), F32), jnp.zeros((rows, cols), F32))
        for k in range(columns):
            base = (k * comps + c) * rows
            tile = basis_ref[base : base + rows, :]
            east = jnp.where(lane == k, pltpu.roll(tile, (k - low) % cols, 1), east)
            west = jnp.where(lane == k, tile if k == 0 else pltpu.roll(tile, k, 1), west)
        east = jnp.where(lane == columns, rhs[c][:, low : low + 1], east)
        west = jnp.where(lane == columns, rhs[c][:, 0:1], west)
        east = east * mask[c][:, low : low + 1]
        west = west * mask[c][:, 0:1]
        cola_ref[c * rows : (c + 1) * rows, :] = pick(even_col, east, west)
        colb_ref[c * rows : (c + 1) * rows, :] = pick(even_col, west, east)
    east = jnp.where(lane == 0, visc[:, low : low + 1], visc[:, low - 1 : low])
    west = jnp.where(lane == 0, visc[:, 0:1], visc[:, 1:2])
    cola_ref[comps * rows :, :] = pick(even_col, east, west)
    colb_ref[comps * rows :, :] = pick(even_col, west, east)


def stencil(mask, faces, diagonal, tile, halo):
    masked = mask * tile
    near = shifts(masked, *halo)
    inner = diagonal * masked - (
        faces[0] * near[0] + faces[1] * near[1] + faces[2] * near[2] + faces[3] * near[3]
    )
    return mask * inner + (1.0 - mask) * tile


def split(values):
    high = values.astype(jnp.bfloat16)
    return jnp.concatenate([high, (values - high.astype(F32)).astype(jnp.bfloat16)], axis=0)


def product(lefts, rights):
    return lax.dot_general(
        jnp.concatenate([split(value) for value in lefts], axis=1),
        jnp.concatenate([split(value) for value in rights], axis=1),
        (((1,), (1,)), ((), ())),
        preferred_element_type=F32,
    )


def merge(blocks, columns):
    blocks = blocks + pltpu.roll(blocks, columns, 1)
    return blocks[:columns] + blocks[columns:]


def local_kernel(sizes, basis_ref, rhs_ref, mask_ref, visc_ref, inner_ref, dots_ref, acc_ref):
    columns, comps, rows, cols = sizes
    _, has_south, _, has_west = flags()
    top, low = (rows - 1, cols - 1)
    rhs = [rhs_ref[c * rows : (c + 1) * rows, :] for c in range(comps)]
    mask = [mask_ref[c * rows : (c + 1) * rows, :].astype(F32) for c in range(comps)]
    visc = visc_ref[...]
    sub, lane = (iota((rows, cols), 0), iota((rows, cols), 1))
    empty = (jnp.zeros((1, cols), F32),) * 2 + (jnp.zeros((rows, 1), F32),) * 2
    faces = [0.5 * (visc + v) for v in shifts(visc, *empty)]
    faces[0] = jnp.where(sub == top, 0.0, faces[0])
    faces[1] = jnp.where(sub == 0, faces[1] * (1.0 - has_south), faces[1])
    faces[2] = jnp.where(lane == low, 0.0, faces[2])
    faces[3] = jnp.where(lane == 0, faces[3] * (1.0 - has_west), faces[3])
    diagonal = 1.0 + faces[0] + faces[1] + faces[2] + faces[3]

    blocks = jnp.zeros((2 * columns, 2 * columns), F32)
    for c in range(comps):
        m = mask[c]
        own = m * diagonal + (1.0 - m)
        up, down = (m * faces[0], m * faces[1])
        right = m * faces[2]
        left = jnp.where(lane == 0, 0.0, m * faces[3])
        plain = [
            basis_ref[pl.ds(c * rows + i, columns, stride=comps * rows), :] for i in range(rows)
        ]
        free = [plain[i] * m[i : i + 1, :] for i in range(rows)]
        images = []
        for i in range(rows):
            here = slice(i, i + 1)
            value = own[here] * plain[i] - right[here] * pltpu.roll(free[i], low, 1)
            value = value - left[here] * pltpu.roll(free[i], 1, 1)
            if i < top:
                value = value - up[here] * free[i + 1]
            if i > 0:
                value = value - down[here] * free[i - 1]
            images.append(value)
        for i in range(0, rows, 2):
            blocks = blocks + product(plain[i : i + 2], images[i : i + 2])
    inner_ref[...] = merge(blocks, columns)
    dots = to_row(project(basis_ref, rhs, acc_ref, columns, comps, rows))
    dots_ref[...] = jnp.broadcast_to(dots, dots_ref.shape)


def border_kernel(sizes, inner_ref, dots_ref, basis_ref, mask_ref, visc_ref, gram_ref, rowa_ref,
                  rowb_ref, cola_ref, colb_ref, owna_ref, ownb_ref, send_ref, full_ref):
    columns, comps, rows, cols = sizes
    even_row = 1 - lax.rem(lax.axis_index("row"), 2)
    even_col = 1 - lax.rem(lax.axis_index("col"), 2)
    has_north, _, has_east, _ = flags()
    top, low, half = (rows - 1, cols - 1, cols // 2)
    field = comps * rows
    visc, lanes = (visc_ref[...], iota((1, cols), 1))
    at = comps * columns + comps
    v_north = pick(even_row, rowa_ref[at : at + 1, :], rowb_ref[at : at + 1, :]) * has_north
    east = pick(even_col, cola_ref[...], colb_ref[...]) * has_east
    own_east = pick(even_col, owna_ref[...], ownb_ref[...])
    north_face = 0.5 * (visc[top : top + 1, :] + v_north)
    east_face = 0.5 * (visc[:, low : low + 1] + east[field:, 0:1])
    tops = []
    for c in range(comps):
        span = slice(c * columns, (c + 1) * columns)
        own = basis_ref[pl.ds(c * rows + top, columns, stride=comps * rows), :]
        own = own * mask_ref[c * rows + top : c * rows + rows, :].astype(F32)
        tops.append(own - pick(even_row, rowa_ref[span, :], rowb_ref[span, :]) * has_north)
    full = inner_ref[...] + merge(product([value * north_face for value in tops], tops), columns)
    gap = own_east[:field] - east[:field]
    edge = lax.dot_general(
        gap * jnp.concatenate([east_face] * comps, axis=0), gap, (((0,), (0,)), ((), ())),
        preferred_element_type=F32, precision=lax.Precision.HIGHEST,
    )
    wide_lane = iota((columns, cols), 1)
    edge = jnp.where(wide_lane < half, edge[:columns], 0.0)
    full = full + edge + pltpu.roll(edge, half, 1)
    full_ref[...] = full
    spot = jnp.where(wide_lane >= half, wide_lane - half, wide_lane) == iota((columns, cols), 0)
    spine = jnp.sum(jnp.where(spot, full, 0.0), axis=0, keepdims=True)
    count = columns // 2
    chunk = jnp.where(
        iota((count, cols), 1) < half,
        full_ref[pl.ds(0, count, stride=2), :],
        full_ref[pl.ds(1, count, stride=2), :],
    )
    dots = dots_ref[0:1, :]
    corner_row = jnp.zeros((1, cols), F32)
    for i, corner in enumerate(corners_of(visc)):
        corner_row = jnp.where(lanes == i, corner, corner_row)
    at = 2 * lax.axis_index("row")
    piece = jnp.concatenate([gram_ref[pl.ds(at + t, 1), :] for t in range(2)], axis=1)
    head = jnp.concatenate([jnp.where(lanes < half, dots, spine), piece], axis=0)
    for d in range(count):
        send_ref[d] = jnp.concatenate([head, chunk[d : d + 1, :], corner_row], axis=0)


def first_kernel(sizes, whole_rows, two, got_ref, *refs):
    columns, comps, rows, cols, scale = sizes
    if whole_rows:
        gram_in_ref = None
    else:
        gram_in_ref, *refs = refs
    (basis_ref, rhs_ref, mask_ref, visc_ref, rowa_ref, rowb_ref, cola_ref, colb_ref,
     send_ref, state_ref, face_ref, small_ref, gram_ref, *refs) = refs
    edge_ref, side_ref = (None, None) if two else refs[:2]
    acc_ref, wide_ref = refs[-2:]
    at_row, at_col = (lax.axis_index("row"), lax.axis_index("col"))
    row_count, col_count = (lax.axis_size("row"), lax.axis_size("col"))
    even_row, even_col = (1 - lax.rem(at_row, 2), 1 - lax.rem(at_col, 2))
    me = at_row * col_count + at_col
    top, low = rows - 1, cols - 1
    rhs = [rhs_ref[c * rows : (c + 1) * rows, :] for c in range(comps)]
    mask = [mask_ref[c * rows : (c + 1) * rows, :].astype(F32) for c in range(comps)]
    visc = visc_ref[...]
    sub, lane = (iota((rows, cols), 0), iota((rows, cols), 1))
    lanes = iota((1, cols), 1)

    if whole_rows:
        per = cols // columns
        pieces = got_ref[:, 1, :]
        for c in range(col_count):
            piece = jnp.concatenate(
                [pieces[r * col_count + c : r * col_count + c + 1] for r in range(row_count)], axis=0
            )
            for t in range(per):
                moved = pltpu.roll(piece, cols - t * columns, 1) if t else piece
                gram_ref[pl.ds(c * row_count * per + t, row_count, stride=per), :] = moved
    else:
        gram_ref[:, :columns] = gram_in_ref[...]
    all_sums = jnp.sum(got_ref[...], axis=0)
    sums = all_sums[0:1, :]
    dots = jnp.where(lanes < columns, sums, 0.0)
    gram = jnp.where(iota((columns, cols), 1) < columns, gram_ref[...], 0.0)
    coeffs = jnp.sum(gram * dots, axis=1, keepdims=True) * scale
    wide = jnp.broadcast_to(coeffs, (columns, cols))
    wide_ref[...] = wide
    coeff_row = to_row(coeffs)

    extra = comps * columns
    tail_a, tail_b = (rowa_ref[extra:, :], rowb_ref[extra:, :])
    has_north, has_south, has_east, has_west = flags()
    north_tail = pick(even_row, tail_a, tail_b) * has_north
    south_tail = pick(even_row, tail_b, tail_a) * has_south
    side_a, side_b = (cola_ref[...], colb_ref[...])
    east_side = pick(even_col, side_a, side_b) * has_east
    west_side = pick(even_col, side_b, side_a) * has_west
    v_north, v_south = (north_tail[comps : comps + 1, :], south_tail[comps : comps + 1, :])
    v_north2, v_south2 = (north_tail[comps + 1 : comps + 2, :], south_tail[comps + 1 : comps + 2, :])
    v_east, v_west = (east_side[comps * rows :, 0:1], west_side[comps * rows :, 0:1])
    v_east2, v_west2 = (east_side[comps * rows :, 1:2], west_side[comps * rows :, 1:2])
    faces = [0.5 * (visc + v) for v in shifts(visc, v_north, v_south, v_east, v_west)]
    diagonal = 1.0 + faces[0] + faces[1] + faces[2] + faces[3]
    face_ref[...] = jnp.concatenate(faces + [diagonal], axis=0)
    jacobi = [m / diagonal + (1.0 - m) for m in mask]

    def corner(step_row, step_col, which):
        r, c = (at_row + step_row, at_col + step_col)
        inside = (r >= 0) & (r < row_count) & (c >= 0) & (c < col_count)
        place = jnp.where(inside, r * col_count + c, me)
        line, first = (3, 0) if two else (0, columns)
        value = got_ref[place, line : line + 1, :]
        value = jnp.sum(jnp.where(lanes == first + which, value, 0.0), axis=1, keepdims=True)
        return value * jnp.where(inside, 1.0, 0.0)

    north_west, north_east = (corner(1, -1, 1), corner(1, 1, 0))
    south_west, south_east = (corner(-1, -1, 3), corner(-1, 1, 2))

    def row_inverse(own, inner, outer, west, east):
        right = jnp.where(lanes == low, east, pltpu.roll(own, low, 1))
        left = jnp.where(lanes == 0, west, pltpu.roll(own, 1, 1))
        return 1.0 / (1.0 + 0.5 * (4.0 * own + inner + outer + left + right))

    def side_inverse(own, inner, outer, south, north):
        own = jnp.broadcast_to(own, (rows, cols))
        up = jnp.where(sub == top, north, pltpu.roll(own, top, 0))
        down = jnp.where(sub == 0, south, pltpu.roll(own, 1, 0))
        return 1.0 / (1.0 + 0.5 * (4.0 * own + inner + outer + up + down))

    inv_north = row_inverse(v_north, visc[top : top + 1, :], v_north2, north_west, north_east)
    inv_south = row_inverse(v_south, visc[0:1, :], v_south2, south_west, south_east)
    inv_east = side_inverse(v_east, visc[:, low : low + 1], v_east2, south_east, north_east)
    inv_west = side_inverse(v_west, visc[:, 0:1], v_west2, south_west, north_west)

    corr = combine(basis_ref, wide_ref, columns, comps, rows)
    image, scaled, smooth, point = ([], [], [], [])
    scaled_image = []
    none = (jnp.zeros((1, cols), F32),) * 2 + (jnp.zeros((rows, 1), F32),) * 2
    for c in range(comps):
        span = slice(c * columns, (c + 1) * columns)
        sum_a = jnp.sum(wide * rowa_ref[span, :], axis=0, keepdims=True)
        sum_b = jnp.sum(wide * rowb_ref[span, :], axis=0, keepdims=True)
        u_north = inv_north * north_tail[c : c + 1, :]
        u_south = inv_south * south_tail[c : c + 1, :]
        p_north = u_north + has_north * pick(even_row, sum_a, sum_b)
        p_south = u_south + has_south * pick(even_row, sum_b, sum_a)
        here = slice(c * rows, (c + 1) * rows)
        east, west = (east_side[here, :], west_side[here, :])
        u_east = inv_east * east[:, columns : columns + 1]
        u_west = inv_west * west[:, columns : columns + 1]
        p_east = u_east + jnp.sum(coeff_row * east, axis=1, keepdims=True)
        p_west = u_west + jnp.sum(coeff_row * west, axis=1, keepdims=True)
        u = jacobi[c] * rhs[c]
        p = u + corr[c]
        q = stencil(mask[c], faces, diagonal, p, (p_north, p_south, p_east, p_west))
        if two:
            scaled_image.append(stencil(mask[c], faces, diagonal, jacobi[c] * q, none))
        smooth.append(u)
        point.append(p)
        image.append(q)
        scaled.append(jacobi[c] * q)
        if two:
            continue
        for i, value in enumerate((u_north, u_south, p_north, p_south)):
            edge_ref[i * 8 + c : i * 8 + c + 1, :] = value
        for i, value in enumerate((u_east, u_west, p_east, p_west)):
            side_ref[(i * comps + c) * rows : (i * comps + c + 1) * rows, :] = value
    fields = point + image + scaled
    state_ref[...] = jnp.concatenate(fields if two else smooth + fields, axis=0)

    row = to_row(project(basis_ref, image, acc_ref, columns, comps, rows))
    pairs = ((point, image), (smooth, image), (image, scaled), (rhs, smooth))
    if two:
        pairs += ((scaled, scaled_image),)
    for i, (left, right) in enumerate(pairs):
        value = left[0] * right[0]
        for c in range(1, comps):
            value = value + left[c] * right[c]
        row = jnp.where(lanes == (DOTS2 if two else DOTS) + i, total(value), row)
    masked = [mask[c] * scaled[c] for c in range(comps)]
    if two:
        norths = [m[top : top + 1, :] * faces[0][top : top + 1, :] * has_north for m in masked]
        easts = [m[:, low : low + 1] * faces[2][:, low : low + 1] * has_east for m in masked]
        souths, wests = ([m[0:1, :] for m in masked], [m[:, 0:1] for m in masked])
        row = row + to_row(jnp.concatenate(easts, axis=0), EAST2)
        row = row + to_row(jnp.concatenate(wests, axis=0), WEST2)
        reach = project(basis_ref, scaled_image, acc_ref, columns, comps, rows)
        beyond = jnp.zeros((columns, cols), F32)
        aside = jnp.zeros((rows, cols), F32)
        for c in range(comps):
            span, here = (slice(c * columns, (c + 1) * columns), slice(c * rows, (c + 1) * rows))
            halo_a, halo_b = (rowa_ref[span, :], rowb_ref[span, :])
            low_side = souths[c] * faces[1][0:1, :] * has_south
            beyond = beyond + norths[c] * pick(even_row, halo_a, halo_b)
            beyond = beyond + low_side * pick(even_row, halo_b, halo_a)
            aside = aside + easts[c] * east_side[here, :]
            aside = aside + wests[c] * faces[3][:, 0:1] * west_side[here, :]
        reach = to_row(reach - jnp.sum(beyond, axis=1, keepdims=True))
        reach = reach - jnp.where(lanes < columns, jnp.sum(aside, axis=0, keepdims=True), 0.0)
        half = cols // 2
        ours = jnp.broadcast_to(all_sums[2:3, :], (8, cols))
        other = pltpu.roll(ours, half, 1)
        wide_lane = iota((8, cols), 1)
        for t, (first, second) in enumerate(((ours, other), (other, ours))):
            value = jnp.where(wide_lane < half, first, second)
            turn = lax.rem(half + t * (half // 2) - (2 * me + t + 1) + 2 * cols, cols)
            value = pltpu.roll(value, turn, 1)[0:1, :]
            start = half + t * (half // 2)
            reach = jnp.where((lanes >= start) & (lanes < start + half // 2), value, reach)
        message = jnp.concatenate(norths + souths + [row, reach], axis=0)
        send_ref[...] = jnp.broadcast_to(message[None], send_ref.shape)
        spine = pltpu.roll(jnp.broadcast_to(sums, (8, cols)), half, 1)[0:1, :]
        spine = jnp.where(lanes < half, spine, 0.0)
        small_ref[...] = jnp.concatenate([dots, coeff_row, spine, jnp.zeros((5, cols), F32)], axis=0)
        return
    east = jnp.concatenate([m[:, low : low + 1] for m in masked], axis=0)
    west = jnp.concatenate([m[:, 0:1] for m in masked], axis=0)
    row = row + to_row(east, EAST) + to_row(west, WEST)
    message = jnp.concatenate([row] + [m[top : top + 1, :] for m in masked], axis=0)
    send_ref[...] = jnp.broadcast_to(message[None], send_ref.shape)
    message = jnp.concatenate([row] + [m[0:1, :] for m in masked], axis=0)
    send_ref[jnp.where(at_row > 0, me - col_count, me)] = message
    small_ref[...] = jnp.concatenate([dots, coeff_row, jnp.zeros((6, cols), F32)], axis=0)


def second_kernel(sizes, got_ref, basis_ref, rhs_ref, mask_ref, rowa_ref, rowb_ref, cola_ref,
                  colb_ref, state_ref, face_ref, small_ref, gram_ref, edge_ref, side_ref,
                  send_ref, out_ref, last_ref, wide_ref):
    columns, comps, rows, cols, scale = sizes
    at_row, at_col = (lax.axis_index("row"), lax.axis_index("col"))
    row_count, col_count = (lax.axis_size("row"), lax.axis_size("col"))
    even_row, even_col = (1 - lax.rem(at_row, 2), 1 - lax.rem(at_col, 2))
    me = at_row * col_count + at_col
    lanes = iota((1, cols), 1)
    mask = [mask_ref[c * rows : (c + 1) * rows, :].astype(F32) for c in range(comps)]

    sums = jnp.sum(got_ref[...], axis=0)[0:1, :]
    image_dots = jnp.where(lanes < columns, sums, 0.0)
    curve, cross, image_sq, rhs_sq = [
        jnp.sum(jnp.where(lanes == DOTS + i, sums, 0.0), axis=1, keepdims=True) for i in range(4)
    ]
    dots, coeff_row = (small_ref[0:1, :], small_ref[1:2, :])
    energy = rhs_sq + jnp.sum(dots * coeff_row, axis=1, keepdims=True)
    step = energy / curve
    gram = jnp.where(iota((columns, cols), 1) < columns, gram_ref[...], 0.0)
    dots = dots - step * image_dots
    coeffs = jnp.sum(gram * dots, axis=1, keepdims=True) * scale
    wide = jnp.broadcast_to(coeffs, (columns, cols))
    wide_ref[...] = wide
    coeff_row = to_row(coeffs)
    energy_new = rhs_sq - 2.0 * step * cross + step * step * image_sq
    energy_new = energy_new + jnp.sum(dots * coeff_row, axis=1, keepdims=True)
    ratio = energy_new / energy

    def beside(step_row, step_col):
        r, c = (at_row + step_row, at_col + step_col)
        inside = (r >= 0) & (r < row_count) & (c >= 0) & (c < col_count)
        message = got_ref[jnp.where(inside, r * col_count + c, me)]
        return message * jnp.where(inside, 1.0, 0.0)

    q_north, q_south = (beside(1, 0), beside(-1, 0))
    q_east = to_column(beside(0, 1)[0:1, :], comps * rows, WEST)
    q_west = to_column(beside(0, -1)[0:1, :], comps * rows, EAST)

    side_a, side_b = (cola_ref[...], colb_ref[...])
    has_north, has_south, has_east, has_west = flags()
    east_side = pick(even_col, side_a, side_b) * has_east
    west_side = pick(even_col, side_b, side_a) * has_west
    faces = [face_ref[i * rows : (i + 1) * rows, :] for i in range(4)]
    diagonal = face_ref[4 * rows : 5 * rows, :]
    corr = combine(basis_ref, wide_ref, columns, comps, rows)
    curve_part = jnp.zeros((rows, cols), F32)
    first, second, third, fourth = ([], [], [], [])
    for c in range(comps):
        span = slice(c * columns, (c + 1) * columns)
        here = slice(c * rows, (c + 1) * rows)
        sum_a = jnp.sum(wide * rowa_ref[span, :], axis=0, keepdims=True)
        sum_b = jnp.sum(wide * rowb_ref[span, :], axis=0, keepdims=True)
        old = [edge_ref[i * 8 + c : i * 8 + c + 1, :] for i in range(4)]
        p_north = old[0] - step * q_north[1 + c : 2 + c, :] + has_north * pick(even_row, sum_a, sum_b)
        p_south = old[1] - step * q_south[1 + c : 2 + c, :] + has_south * pick(even_row, sum_b, sum_a)
        p_north, p_south = (p_north + ratio * old[2], p_south + ratio * old[3])
        old = [side_ref[(i * comps + c) * rows : (i * comps + c + 1) * rows, :] for i in range(4)]
        p_east = old[0] - step * q_east[here] + ratio * old[2]
        p_west = old[1] - step * q_west[here] + ratio * old[3]
        p_east = p_east + jnp.sum(coeff_row * east_side[here, :], axis=1, keepdims=True)
        p_west = p_west + jnp.sum(coeff_row * west_side[here, :], axis=1, keepdims=True)
        u, p, q, jq = [
            state_ref[(i * comps + c) * rows : (i * comps + c + 1) * rows, :] for i in range(4)
        ]
        new = u - step * jq + corr[c] + ratio * p
        masked = mask[c] * new
        near = shifts(masked, p_north, p_south, p_east, p_west)
        stencil = diagonal * masked - (
            faces[0] * near[0] + faces[1] * near[1] + faces[2] * near[2] + faces[3] * near[3]
        )
        applied = mask[c] * stencil + (1.0 - mask[c]) * new
        curve_part = curve_part + new * applied
        first.append(step * p)
        second.append(new)
        third.append(rhs_ref[here, :] - step * q)
        fourth.append(applied)
    out_ref[...] = jnp.concatenate(first + second + third + fourth, axis=0)
    last_ref[...] = jnp.broadcast_to(energy_new, last_ref.shape)
    send_ref[...] = jnp.broadcast_to(total(curve_part)[None], send_ref.shape)


def close_kernel(sizes, got_ref, basis_ref, rhs_ref, mask_ref, rowa_ref, rowb_ref, cola_ref,
                 colb_ref, state_ref, face_ref, small_ref, gram_ref,
                 solution_ref, residual_ref, wide_ref):
    columns, comps, rows, cols, scale = sizes
    at_row, at_col = (lax.axis_index("row"), lax.axis_index("col"))
    row_count, col_count = (lax.axis_size("row"), lax.axis_size("col"))
    devices = row_count * col_count
    even_row, even_col = (1 - lax.rem(at_row, 2), 1 - lax.rem(at_col, 2))
    has_north, has_south, has_east, has_west = flags()
    me = at_row * col_count + at_col
    half, quarter = (cols // 2, cols // 4)
    lanes = iota((1, cols), 1)
    mask = [mask_ref[c * rows : (c + 1) * rows, :].astype(F32) for c in range(comps)]

    def along(left, right):
        return jnp.sum(left * right, axis=1, keepdims=True)

    sums = jnp.sum(got_ref[...], axis=0)
    line = sums[2 * comps : 2 * comps + 1, :]
    image_dots = jnp.where(lanes < columns, line, 0.0)
    reach_dots = jnp.where(lanes < columns, sums[2 * comps + 1 :, :], 0.0)
    gram = jnp.where(iota((columns, cols), 1) < columns, gram_ref[...], 0.0)
    turn = jnp.sum(gram * image_dots, axis=1, keepdims=True) * scale
    wide = jnp.broadcast_to(turn, (columns, cols))
    wide_ref[...] = wide
    turn_row = to_row(turn)

    def beside(step_row, step_col):
        r, c = (at_row + step_row, at_col + step_col)
        inside = (r >= 0) & (r < row_count) & (c >= 0) & (c < col_count)
        message = got_ref[jnp.where(inside, r * col_count + c, me)]
        return message * jnp.where(inside, 1.0, 0.0)

    faces = [face_ref[i * rows : (i + 1) * rows, :] for i in range(4)]
    diagonal = face_ref[4 * rows : 5 * rows, :]
    q_north, q_south = (beside(1, 0), beside(-1, 0))
    q_east = to_column(beside(0, 1)[2 * comps : 2 * comps + 1, :], comps * rows, WEST2)
    q_west = to_column(beside(0, -1)[2 * comps : 2 * comps + 1, :], comps * rows, EAST2)
    side_a, side_b = (cola_ref[...], colb_ref[...])
    east_side = pick(even_col, side_a, side_b) * has_east
    west_side = pick(even_col, side_b, side_a) * has_west
    corr = combine(basis_ref, wide_ref, columns, comps, rows)
    moved, moved_image = ([], [])
    for c in range(comps):
        span = slice(c * columns, (c + 1) * columns)
        here = slice(c * rows, (c + 1) * rows)
        sum_a = jnp.sum(wide * rowa_ref[span, :], axis=0, keepdims=True)
        sum_b = jnp.sum(wide * rowb_ref[span, :], axis=0, keepdims=True)
        north = q_north[comps + c : comps + c + 1, :] + has_north * pick(even_row, sum_a, sum_b)
        south = q_south[c : c + 1, :] / faces[1][0:1, :] + has_south * pick(even_row, sum_b, sum_a)
        east = q_east[here] + along(turn_row, east_side[here, :])
        west = q_west[here] / faces[3][:, 0:1] + along(turn_row, west_side[here, :])
        at = (2 * comps + c) * rows
        value = state_ref[at : at + rows, :] + corr[c]
        moved.append(value)
        moved_image.append(stencil(mask[c], faces, diagonal, value, (north, south, east, west)))

    border = jnp.zeros((2 * comps + 2, cols), F32)
    for d in range(devices - col_count):
        border = border + got_ref[d] * pltpu.roll(got_ref[d + col_count], comps + 2, 0)
    border = jnp.where(iota(border.shape, 0) < comps, border, 0.0)
    lines = got_ref[:, 2 * comps, :]
    later = pltpu.roll(pltpu.roll(lines, devices - 1, 0), cols - (WEST2 - EAST2), 1)
    line_lane = iota(lines.shape, 1)
    beside_it = jnp.where((line_lane >= EAST2) & (line_lane < WEST2), lines * later, 0.0)
    across = jnp.sum(border, axis=0, keepdims=True) + jnp.sum(beside_it, axis=0, keepdims=True)

    packed = pltpu.roll(got_ref[:, 2 * comps + 1, :], half, 1)
    sub = iota(packed.shape, 0)
    value = jnp.broadcast_to(turn_row, (8, cols))
    value = jnp.broadcast_to((value + pltpu.roll(value, half, 1))[0:1, :], packed.shape)
    bit = 1
    while bit < devices:
        value = jnp.where((sub & bit) != 0, pltpu.roll(value, cols - 2 * bit, 1), value)
        bit *= 2
    ahead = pltpu.roll(value, cols - 1, 1)
    ahead = jnp.where(line_lane < quarter, ahead, pltpu.roll(value, quarter - 2, 1))
    own = jnp.where(line_lane < quarter, value[:, 0:1], value[:, 1:2])
    weight = jnp.where((line_lane == quarter - 1) | (line_lane == half - 1), 1.0, 2.0)
    form = jnp.where(line_lane < half, packed * weight * own * ahead, 0.0)
    form = jnp.sum(form, axis=0, keepdims=True)

    curve, cross, image_sq, rhs_sq, scaled_sq = [
        along(jnp.where(lanes == DOTS2 + i, 1.0, 0.0), line) for i in range(5)
    ]
    dots, old_row, spine = (small_ref[0:1, :], small_ref[1:2, :], small_ref[2:3, :])
    energy = rhs_sq + along(dots, old_row)
    meet = image_sq + along(turn_row, image_dots)
    rest = form + spine * turn_row * turn_row + 2.0 * turn_row * reach_dots - 2.0 * across
    moved_sq = scaled_sq + jnp.sum(rest, axis=1, keepdims=True)
    step = energy / curve
    energy_new = rhs_sq - 2.0 * step * cross + step * step * image_sq
    energy_new = energy_new + along(dots - step * image_dots, old_row - step * turn_row)
    grow = 1.0 + energy_new / energy
    curve_new = grow * grow * curve - 2.0 * step * grow * meet + step * step * moved_sq
    step_new = energy_new / curve_new
    near, far = (step + step_new * grow, step_new * step)
    for c in range(comps):
        here = slice(c * rows, (c + 1) * rows)
        p = state_ref[here, :]
        q = state_ref[(comps + c) * rows : (comps + c + 1) * rows, :]
        solution_ref[here, :] = near * p - far * moved[c]
        residual_ref[here, :] = rhs_ref[here, :] - near * q + far * moved_image[c]


def last_kernel(count, got_ref, in_ref, last_ref, solution_ref, residual_ref):
    step = last_ref[0:1, :] / jnp.sum(got_ref[...], axis=0)
    solution_ref[...] = in_ref[:count, :] + step * in_ref[count : 2 * count, :]
    residual_ref[...] = in_ref[2 * count : 3 * count, :] - step * in_ref[3 * count :, :]


def on_device(right_side, viscosity, free_mask, coarse_basis, gram_inverse):
    comps, rows, cols = right_side.shape
    columns = coarse_basis.shape[0]
    row_count, col_count = (lax.axis_size("row"), lax.axis_size("col"))
    devices = row_count * col_count
    scale = 1.0 / (32.0 * math.sqrt(float(comps * rows * cols * devices * columns)))
    sizes = (columns, comps, rows, cols)

    def call(kernel, outs, scratch, *args, flops=None):
        cost = flops and pl.CostEstimate(flops=flops, bytes_accessed=4096, transcendentals=0)
        return pl.pallas_call(
            kernel,
            out_shape=[jax.ShapeDtypeStruct(s, F32) for s in outs],
            in_specs=[VMEM] * len(args),
            out_specs=[VMEM] * len(outs),
            scratch_shapes=[pltpu.VMEM(s, F32) for s in scratch],
            cost_estimate=cost,
            compiler_params=pltpu.CompilerParams(vmem_limit_bytes=16 * 1024 * 1024),
        )(*args)

    def share(message):
        return lax.all_to_all(message, ("row", "col"), 0, 0, tiled=True)

    def swap(packet, axis, first):
        pairs = []
        for r in range(row_count):
            for c in range(col_count):
                along, across = ((r, c) if axis == "row" else (c, r))
                length, width = (row_count, col_count)[:: 1 if axis == "row" else -1]
                other = along + 1 if (along - first) % 2 == 0 else along - 1
                if 0 <= other < length:
                    mate = (other, across)
                else:
                    mate = (along, across ^ 1 if (across ^ 1) < width else across)
                r2, c2 = mate if axis == "row" else mate[::-1]
                pairs.append((r * col_count + c, r2 * col_count + c2))
        return lax.ppermute(packet, ("row", "col"), pairs)

    basis = coarse_basis.reshape(columns * comps * rows, cols)
    rhs = right_side.reshape(comps * rows, cols)
    mask = free_mask.reshape(comps * rows, cols)

    block = gram_inverse.size
    piece = -(-block // row_count)
    two = columns * columns == devices * cols and cols == 2 * columns and rows == 8 and comps == 3
    if two:
        (first,) = call(open_kernel, [(8, cols)], [], flops=10**9)
        own = gram_inverse
    else:
        flat = jnp.pad(gram_inverse.reshape(-1), (0, piece * row_count - block))
        own = lax.dynamic_slice_in_dim(flat, lax.axis_index("row") * piece, piece)
        own = jnp.pad(own, (0, cols - piece)).reshape(1, cols)

    tall = -(-(comps * columns + comps + 2) // 8) * 8
    wide = (comps + 1) * rows
    field = comps * rows
    if two:
        row_a, row_b = call(
            functools.partial(rows_kernel, sizes),
            [(tall, cols), (tall, cols)],
            [],
            basis, rhs, mask, viscosity, first,
        )
        col_a, col_b = call(
            functools.partial(sides_kernel, sizes),
            [(wide, cols), (wide, cols)],
            [],
            basis, rhs, mask, viscosity,
        )
        packets = ((row_a, "row", 0), (row_b, "row", 1), (col_a, "col", 0), (col_b, "col", 1))
        halos = []
        for packet in packets:
            halos.append(swap(*packet))
        inner, dots = call(
            functools.partial(local_kernel, sizes),
            [(columns, cols), (8, cols)],
            [(columns * rows, cols)],
            basis, rhs, mask, viscosity, flops=10**8,
        )
        (send,) = call(
            functools.partial(border_kernel, sizes),
            [(devices, 4, cols)],
            [(columns, cols)],
            inner, dots, basis, mask, viscosity, own, *halos, col_a, col_b,
        )
        sizes = sizes + (scale,)
        send, *state = call(
            functools.partial(first_kernel, sizes, True, True),
            [(devices, 8, cols), (3 * field, cols), (5 * rows, cols), (8, cols), (columns, cols)],
            [(columns * rows, cols), (columns, cols)],
            share(send), basis, rhs, mask, viscosity, *halos,
        )
        solution, residual = call(
            functools.partial(close_kernel, sizes),
            [(field, cols), (field, cols)],
            [(columns, cols)],
            share(send), basis, rhs, mask, *halos, *state,
        )
        return (solution.reshape(right_side.shape), residual.reshape(right_side.shape))
    send, row_a, row_b, col_a, col_b = call(
        functools.partial(pack_kernel, sizes),
        [(devices, 2, cols), (tall, cols), (tall, cols), (wide, cols), (wide, cols)],
        [(columns * rows, cols)],
        basis, rhs, mask, viscosity, own,
    )
    halos = (swap(row_a, "row", 0), swap(row_b, "row", 1), swap(col_a, "col", 0), swap(col_b, "col", 1))
    got = share(send)
    whole_rows = piece == cols and cols % columns == 0 and block == piece * row_count
    gram = ()
    if not whole_rows:
        gram = got[:, 1, :piece].reshape(row_count, col_count, piece).transpose(1, 0, 2)
        gram = gram.reshape(col_count, row_count * piece)[:, :block].reshape(columns, columns)
        gram = (gram,)
    sizes = sizes + (scale,)
    send, *state = call(
        functools.partial(first_kernel, sizes, whole_rows, False),
        [(devices, 1 + comps, cols), (4 * field, cols), (5 * rows, cols), (8, cols),
         (columns, cols), (32, cols), (4 * field, cols)],
        [(columns * rows, cols), (columns, cols)],
        got, *gram, basis, rhs, mask, viscosity, *halos,
    )
    send, fields, last = call(
        functools.partial(second_kernel, sizes),
        [(devices, 1, cols), (4 * field, cols), (8, cols)],
        [(columns, cols)],
        share(send), basis, rhs, mask, *halos, *state,
    )
    solution, residual = call(
        functools.partial(last_kernel, field),
        [(field, cols), (field, cols)],
        [],
        share(send), fields, last,
    )
    return (solution.reshape(right_side.shape), residual.reshape(right_side.shape))


def solution(mesh):
    in_specs = (
        P(None, "row", "col"),
        P("row", "col"),
        P(None, "row", "col"),
        P(None, None, "row", "col"),
        P("col", None),
    )
    out_specs = (P(None, "row", "col"), P(None, "row", "col"))
    return jax.shard_map(
        on_device, mesh=mesh, in_specs=in_specs, out_specs=out_specs, check_vma=False
    )
```
